32 devices in a mesh: dp: 4 (over y, core), ctx: 4 (over z), tensor: 2 (over x).
Axes of the slice: x: 2, y: 2, z: 4, core: 2. Of those that a mesh axis runs over, the one named last changes fastest.
Arguments:
- layer_input: bfloat16 [12, 1024, 1536], P('dp', 'ctx'), may hold values from -6 to 6
- cotangent: float32 [12, 1024, 1536], P('dp', 'ctx', 'tensor'), may hold values from -6 to 6
- in_proj: float32 [1536, 2, 3072], P(('dp', 'ctx'), None, 'tensor'), may hold values from -0.15625 to 0.15625
- delta_proj: float32 [1536, 48], P(('dp', 'ctx'), 'tensor'), may hold values from -0.21875 to 0.21875
- out_proj: float32 [1536, 3072], P(('dp', 'ctx'), 'tensor'), may hold values from -0.109375 to 0.109375
- state_proj: float32 [1536, 2, 128], P(('dp', 'ctx', 'tensor')), may hold values from -0.15625 to 0.15625
- packed_params: float32 [21408], P(('dp', 'ctx', 'tensor')), may hold values from -6 to 6
- moment_in: float32 [1536, 2, 3072], P(('dp', 'ctx'), None, 'tensor'), may hold values from -18 to 18
- moment_delta: float32 [1536, 48], P(('dp', 'ctx'), 'tensor'), may hold values from -18 to 18
- moment_out: float32 [1536, 3072], P(('dp', 'ctx'), 'tensor'), may hold values from -18 to 18
- moment_state: float32 [1536, 2, 128], P(('dp', 'ctx', 'tensor')), may hold values from -18 to 18
- moment_packed: float32 [21408], P(('dp', 'ctx', 'tensor')), may hold values from -18 to 18
- square_in: float32 [1536, 2, 3072], P(('dp', 'ctx'), None, 'tensor'), may hold values from 1 to 30
- square_delta: float32 [1536, 48], P(('dp', 'ctx'), 'tensor'), may hold values from 1 to 30
- square_out: float32 [1536, 3072], P(('dp', 'ctx'), 'tensor'), may hold values from 1 to 30
- square_state: float32 [1536, 2, 128], P(('dp', 'ctx', 'tensor')), may hold values from 1 to 30
- square_packed: float32 [21408], P(('dp', 'ctx', 'tensor')), may hold values from 1 to 30
Outputs:
- layer_output: float32 [12, 1024, 1536], P('dp', 'ctx', 'tensor')
- input_grad: float32 [12, 1024, 1536], P('dp', 'ctx', 'tensor')
- grad_in: float32 [1536, 2, 3072], P(('dp', 'ctx'), None, 'tensor')
- grad_delta: float32 [1536, 48], P(('dp', 'ctx'), 'tensor')
- grad_out: float32 [1536, 3072], P(('dp', 'ctx'), 'tensor')
- grad_state: float32 [1536, 2, 128], P(('dp', 'ctx', 'tensor'))
- grad_packed: float32 [21408], P(('dp', 'ctx', 'tensor'))
- new_in: float32 [1536, 2, 3072], P(('dp', 'ctx'), None, 'tensor')
- new_delta: float32 [1536, 48], P(('dp', 'ctx'), 'tensor')
- new_out: float32 [1536, 3072], P(('dp', 'ctx'), 'tensor')
- new_state: float32 [1536, 2, 128], P(('dp', 'ctx', 'tensor'))
- new_packed: float32 [21408], P(('dp', 'ctx', 'tensor'))
- next_moment_in: float32 [1536, 2, 3072], P(('dp', 'ctx'), None, 'tensor')
- next_moment_delta: float32 [1536, 48], P(('dp', 'ctx'), 'tensor')
- next_moment_out: float32 [1536, 3072], P(('dp', 'ctx'), 'tensor')
- next_moment_state: float32 [1536, 2, 128], P(('dp', 'ctx', 'tensor'))
- next_moment_packed: float32 [21408], P(('dp', 'ctx', 'tensor'))
- next_square_in: float32 [1536, 2, 3072], P(('dp', 'ctx'), None, 'tensor')
- next_square_delta: float32 [1536, 48], P(('dp', 'ctx'), 'tensor')
- next_square_out: float32 [1536, 3072], P(('dp', 'ctx'), 'tensor')
- next_square_state: float32 [1536, 2, 128], P(('dp', 'ctx', 'tensor'))
- next_square_packed: float32 [21408], P(('dp', 'ctx', 'tensor'))
The draws below stay inside these ranges and needn't reach their ends.
All inputs are finite; a program needn't handle non-finite values.
Results may differ from the reference program's by a relative error of at most 0.00105.
The reference program's roundings to bfloat16 on the way count: a program that leaves them out, or rounds other values in their place, can miss the bound.
Values may be sent and summed in bfloat16 or wider, within the bound.
A program may use at most 256 MiB of HBM per device.

```python
import math
import jax
import jax.numpy as jnp
from jax import lax

D = 1536
HEADS = 48
HEAD_DIM = 64
STATE = 128
CONV = 4
BLOCK_LEN = 256
STEP = 3
INNER = 3072
SEQS = 12
SEQ_LEN = 1024
PACK = 21408


def draw_packed_params(key, part):
    subkeys = jax.random.split(key, 12)
    conv_kernel = 0.5 * jax.random.normal(subkeys[0], (CONV * INNER,))
    conv_bias = 0.5 * jax.random.normal(subkeys[1], (INNER,))
    gate_gain = 1.0 + 0.3 * jax.random.uniform(subkeys[2], (INNER,), minval=-1.0, maxval=1.0)
    state_kernel = 0.5 * jax.random.normal(subkeys[3], (2 * CONV * STATE,))
    state_bias = 0.5 * jax.random.normal(subkeys[4], (2 * STATE,))
    norm_gain = 1.0 + 0.3 * jax.random.uniform(subkeys[10], (D,), minval=-1.0, maxval=1.0)
    slow_share = 0.5
    delta_bias = jax.random.uniform(subkeys[5], (HEADS,), minval=-4.5, maxval=-3.5)
    slow_heads = jax.random.uniform(subkeys[6], (HEADS,)) < slow_share
    slow_logs = jax.random.uniform(subkeys[7], (HEADS,), minval=math.log(0.0025), maxval=math.log(0.01))
    fast_logs = jax.random.uniform(subkeys[8], (HEADS,), minval=math.log(0.5), maxval=math.log(2.0))
    log_rates = jnp.where(slow_heads, slow_logs, fast_logs)
    skip_gain = jax.random.uniform(subkeys[9], (HEADS,), minval=0.5, maxval=1.5)
    joined = jnp.concatenate([conv_kernel, conv_bias, gate_gain, state_kernel, state_bias, delta_bias, log_rates, skip_gain, norm_gain])
    filler = 0.1 * jax.random.normal(subkeys[11], (PACK - joined.shape[0],))
    return jnp.clip(jnp.concatenate([joined, filler]), -6.0, 6.0).astype(jnp.float32)


def level_of(own_key, dims, shards, least, top_value):
    def one(axis_at, blocks):
        draws = jax.random.uniform(jax.random.fold_in(jax.random.fold_in(own_key, 6), axis_at), (blocks,), jnp.float32, least / len(shards), top_value / len(shards))
        return jnp.repeat(jnp.exp(draws), dims[axis_at] // blocks).reshape((-1,) + (1,) * (len(dims) - axis_at - 1))

    gain = one(*shards[0])
    for cut in shards[1:]:
        gain = gain * one(*cut)
    return gain


def gaussian(rng, shape, scale, reach, cuts=(), held_as=jnp.bfloat16):
    array = scale * jax.random.normal(rng, shape, jnp.float32)
    if cuts:
        array = array * level_of(rng, shape, cuts, -0.22, 0.18)
    return jnp.clip(array, -reach, reach).astype(held_as)


def setup_inputs(seed: int = 0) -> dict:
    splits = jax.random.split(jax.random.key(seed), 18)
    return {
        "layer_input": gaussian(splits[0], (SEQS, SEQ_LEN, D), 1.0, 6.0, ((0, 4), (1, 4))),
        "cotangent": gaussian(splits[1], (SEQS, SEQ_LEN, D), 1.0, 6.0, ((0, 4), (1, 4), (2, 2)), jnp.float32),
        "in_proj": gaussian(splits[2], (D, 2, INNER), D ** -0.5, 0.15625, ((0, 16), (2, 2)), jnp.float32),
        "delta_proj": gaussian(splits[3], (D, HEADS), (D // 2) ** -0.5, 0.21875, ((0, 16), (1, 2)), jnp.float32),
        "out_proj": gaussian(splits[4], (D, INNER), INNER ** -0.5, 0.109375, ((0, 16), (1, 2)), jnp.float32),
        "state_proj": gaussian(splits[5], (D, 2, STATE), D ** -0.5, 0.15625, ((0, 32),), jnp.float32),
        "packed_params": draw_packed_params(jax.random.fold_in(splits[17], 71), 0),
        "moment_in": gaussian(splits[7], (D, 2, INNER), 3.0, 18.0, ((0, 16), (2, 2)), jnp.float32),
        "moment_delta": gaussian(splits[8], (D, HEADS), 3.0, 18.0, ((0, 16), (1, 2)), jnp.float32),
        "moment_out": gaussian(splits[9], (D, INNER), 3.0, 18.0, ((0, 16), (1, 2)), jnp.float32),
        "moment_state": gaussian(splits[10], (D, 2, STATE), 3.0, 18.0, ((0, 32),), jnp.float32),
        "moment_packed": gaussian(splits[11], (PACK,), 3.0, 18.0, ((0, 32),), jnp.float32),
        "square_in": jnp.clip(jnp.exp(math.log(30.0) - 3.4011974 * jax.random.uniform(splits[12], (D, 2, INNER), jnp.float32) ** level_of(splits[12], (D, 2, INNER), ((0, 16), (2, 2)), -0.2, 0.2)), 1.0, 30.0),
        "square_delta": jnp.clip(jnp.exp(math.log(30.0) - 3.4011974 * jax.random.uniform(splits[13], (D, HEADS), jnp.float32) ** level_of(splits[13], (D, HEADS), ((0, 16), (1, 2)), -0.2, 0.2)), 1.0, 30.0),
        "square_out": jnp.clip(jnp.exp(math.log(30.0) - 3.4011974 * jax.random.uniform(splits[14], (D, INNER), jnp.float32) ** level_of(splits[14], (D, INNER), ((0, 16), (1, 2)), -0.2, 0.2)), 1.0, 30.0),
        "square_state": jnp.clip(jnp.exp(math.log(30.0) - 3.4011974 * jax.random.uniform(splits[15], (D, 2, STATE), jnp.float32) ** level_of(splits[15], (D, 2, STATE), ((0, 32),), -0.2, 0.2)), 1.0, 30.0),
        "square_packed": jnp.clip(jnp.exp(math.log(30.0) - 3.4011974 * jax.random.uniform(splits[16], (PACK,), jnp.float32) ** level_of(splits[16], (PACK,), ((0, 32),), -0.2, 0.2)), 1.0, 30.0),
    }


NORM_EPS = 1e-05
BETA_ONE = 0.9
BETA_TWO = 0.999
ADAM_EPS = 1e-08
DECAY_RATE = 0.1
MATRIX_RATE = 0.01
PACKED_RATE = 0.1
HIGH = lax.Precision.HIGHEST

def segment_lengths():
    return [CONV * INNER, INNER, INNER, 2 * CONV * STATE, 2 * STATE, HEADS, HEADS, HEADS, D]

def unpack(flat):
    pieces = []
    offset = 0
    for length in segment_lengths():
        pieces.append(flat[offset:offset + length])
        offset += length
    return pieces

def silu_grad(value):
    sigma = jax.nn.sigmoid(value)
    return sigma * (1.0 + value * (1.0 - sigma))

def conv_forward(extended, kernel, offset_bias, length):
    total = jnp.zeros(extended[:, :length].shape, jnp.float32) + offset_bias
    for tap_index in range(CONV):
        total = total + kernel[tap_index] * extended[:, tap_index:tap_index + length]
    return total

def conv_backward(slope, follow, extended, kernel, length):
    padded = jnp.concatenate([slope, follow], axis=1)
    grad_input = jnp.zeros(slope.shape, jnp.float32)
    kernel_grads = []
    for tap_index in range(CONV):
        begin = CONV - 1 - tap_index
        grad_input = grad_input + kernel[tap_index] * padded[:, begin:begin + length]
        kernel_grads.append(lax.optimization_barrier(jnp.sum(slope * extended[:, tap_index:tap_index + length], axis=(0, 1))))
    return (grad_input, jnp.stack(kernel_grads), lax.optimization_barrier(jnp.sum(slope, axis=(0, 1))))

def ssd_scan(inputs, writer, reader, delta, decay_rates, skip_gain, entering):
    seq_count, token_count, head_count, head_width = inputs.shape
    block_count = token_count // BLOCK_LEN

    def blocked(values):
        shaped = values.reshape((seq_count, block_count, BLOCK_LEN) + values.shape[2:])
        return jnp.moveaxis(shaped, 1, 0)
    cumulative = jnp.cumsum(blocked(delta * decay_rates), axis=2)
    causal = (jnp.arange(BLOCK_LEN)[:, None] >= jnp.arange(BLOCK_LEN)[None, :])[None, None, :, :]

    def advance(carry_state, packed):
        block_in, block_writer, block_reader, block_cum, block_delta = packed
        scores = jnp.einsum('sln,smn->slm', block_reader, block_writer, precision=HIGH)
        cum_heads = jnp.swapaxes(block_cum, 1, 2)
        delta_heads = jnp.swapaxes(block_delta, 1, 2)
        differences = cum_heads[:, :, :, None] - cum_heads[:, :, None, :]
        decays = jnp.where(causal, jnp.exp(jnp.where(causal, differences, 0.0)), 0.0)
        mixing = decays * scores[:, None, :, :] * delta_heads[:, :, None, :]
        within = jnp.einsum('shlm,smhp->slhp', mixing, block_in, precision=HIGH)
        carried = jnp.einsum('sln,shpn->slhp', block_reader, carry_state, precision=HIGH) * jnp.exp(block_cum)[:, :, :, None]
        ending = block_cum[:, -1, :]
        fading = jnp.exp(ending[:, None, :] - block_cum) * block_delta
        additions = jnp.einsum('slh,slhp,sln->shpn', fading, block_in, block_writer, precision=HIGH)
        carry_state = carry_state * jnp.exp(ending)[:, :, None, None] + additions
        return (carry_state, within + carried)
    last_state, outputs = lax.scan(advance, entering, (blocked(inputs), blocked(writer), blocked(reader), cumulative, blocked(delta)))
    outputs = jnp.moveaxis(outputs, 0, 1).reshape(seq_count, token_count, head_count, head_width)
    return (outputs + skip_gain[None, None, :, None] * inputs, last_state)

def contract_cols(left, right, exact):
    if exact:
        return lax.dot_general(left, right, (((1,), (1,)), ((), ())), precision=HIGH, preferred_element_type=jnp.float32)
    return lax.dot_general(left, right, (((1,), (1,)), ((), ())), preferred_element_type=jnp.float32)

def contract_rows(left, right, exact):
    if exact:
        return lax.dot_general(left, right, (((0,), (0,)), ((), ())), precision=HIGH, preferred_element_type=jnp.float32)
    return lax.dot_general(left, right, (((0,), (0,)), ((), ())), preferred_element_type=jnp.float32)

def adam_update(weight, moment, second, gradient, rate):
    moment = BETA_ONE * moment + (1.0 - BETA_ONE) * gradient
    second = BETA_TWO * second + (1.0 - BETA_TWO) * gradient * gradient
    moment_hat = moment / (1.0 - BETA_ONE ** STEP)
    second_hat = second / (1.0 - BETA_TWO ** STEP)
    weight = weight - rate * (moment_hat / (jnp.sqrt(second_hat) + ADAM_EPS) + DECAY_RATE * weight)
    return (weight, moment, second)

def reference(layer_input, cotangent, in_proj, delta_proj, out_proj, state_proj, packed_params, moment_in, moment_delta, moment_out, moment_state, moment_packed, square_in, square_delta, square_out, square_state, square_packed):
    in_matrix = in_proj.astype(jnp.bfloat16).reshape(D, 2 * INNER)
    delta_half = delta_proj.astype(jnp.bfloat16)
    out_half = out_proj.astype(jnp.bfloat16)
    state_half = state_proj.astype(jnp.bfloat16).reshape(D, 2 * STATE)
    state_float = state_half.astype(jnp.float32)
    delta_float = delta_half.astype(jnp.float32)
    pieces = unpack(packed_params.astype(jnp.bfloat16).astype(jnp.float32))
    conv_kernel = pieces[0].reshape(CONV, INNER)
    conv_bias = pieces[1]
    gate_gain = pieces[2]
    state_kernel = pieces[3].reshape(CONV, 2 * STATE)
    state_bias = pieces[4]
    delta_bias = pieces[5]
    log_rates = pieces[6]
    skip_gain = pieces[7]
    norm_gain = pieces[8]
    decay_rates = -jnp.exp(log_rates)
    rim_rows = CONV - 1

    def one_sequence(totals, packed):
        tokens_in, upstream = packed
        input_float = tokens_in.astype(jnp.float32)[None]
        inverse = lax.rsqrt(lax.optimization_barrier(jnp.mean(input_float * input_float, axis=-1, keepdims=True)) + NORM_EPS)
        normed_rows = (input_float * inverse * norm_gain).astype(jnp.bfloat16).reshape(SEQ_LEN, D)
        projected = jnp.dot(normed_rows, in_matrix, preferred_element_type=jnp.float32).astype(jnp.bfloat16).reshape(1, SEQ_LEN, 2, INNER)
        gate_input = projected[:, :, 0].astype(jnp.float32)
        conv_input = projected[:, :, 1]
        state_input = jnp.dot(normed_rows, state_half, preferred_element_type=jnp.float32).astype(jnp.bfloat16).reshape(1, SEQ_LEN, 2 * STATE)
        delta_raw = jnp.dot(normed_rows, delta_half, preferred_element_type=jnp.float32).reshape(1, SEQ_LEN, HEADS)
        extended_conv = jnp.pad(conv_input.astype(jnp.float32), ((0, 0), (rim_rows, 0), (0, 0)))
        extended_state = jnp.pad(state_input.astype(jnp.float32), ((0, 0), (rim_rows, 0), (0, 0)))
        conv_out = conv_forward(extended_conv, conv_kernel, conv_bias, SEQ_LEN)
        state_out = conv_forward(extended_state, state_kernel, state_bias, SEQ_LEN)
        conv_act = jax.nn.silu(conv_out).astype(jnp.bfloat16)
        state_act = jax.nn.silu(state_out).astype(jnp.bfloat16)
        delta = jax.nn.softplus(delta_raw + delta_bias)
        inputs = conv_act.astype(jnp.float32).reshape(1, SEQ_LEN, HEADS, HEAD_DIM)
        writer = state_act[:, :, :STATE].astype(jnp.float32)
        reader = state_act[:, :, STATE:].astype(jnp.float32)
        entering = jnp.zeros((1, HEADS, HEAD_DIM, STATE), jnp.float32)
        (mixer_heads, last_state), mixer_back = jax.vjp(ssd_scan, inputs, writer, reader, delta, decay_rates, skip_gain, entering)
        mixer_flat = mixer_heads.reshape(1, SEQ_LEN, INNER)
        gate_act = jax.nn.silu(gate_input)
        mixed = mixer_flat * gate_act
        gate_inverse = lax.rsqrt(lax.optimization_barrier(jnp.mean(mixed * mixed, axis=-1, keepdims=True)) + NORM_EPS)
        gated_rows = (mixed * gate_inverse * gate_gain).astype(jnp.bfloat16).reshape(SEQ_LEN, INNER)
        branch = contract_cols(gated_rows, out_half, False)
        result = input_float[0] + branch
        up_rows = upstream.astype(jnp.bfloat16)
        gated_grad = jnp.dot(up_rows, out_half, preferred_element_type=jnp.float32).reshape(1, SEQ_LEN, INNER)
        grad_out_part = contract_rows(up_rows, gated_rows, False)
        scaled = gated_grad * gate_gain
        row_mean = lax.optimization_barrier(jnp.mean(scaled * mixed, axis=-1, keepdims=True))
        mixed_grad = gate_inverse * scaled - mixed * gate_inverse ** 3 * row_mean
        grad_gate_gain = lax.optimization_barrier(jnp.sum(gated_grad * mixed * gate_inverse, axis=(0, 1)))
        heads_grad = (mixed_grad * gate_act).reshape(1, SEQ_LEN, HEADS, HEAD_DIM)
        gate_grad = mixed_grad * mixer_flat * silu_grad(gate_input)
        grad_inputs, grad_writer, grad_reader, grad_deltas, grad_rates, grad_skip, unused = mixer_back((heads_grad, jnp.zeros_like(last_state)))
        grad_log_rates = grad_rates * decay_rates
        raw_grad = grad_deltas * jax.nn.sigmoid(delta_raw + delta_bias)
        grad_delta_bias = lax.optimization_barrier(jnp.sum(raw_grad, axis=(0, 1)))
        conv_slope = grad_inputs.reshape(1, SEQ_LEN, INNER) * silu_grad(conv_out)
        state_slope = jnp.concatenate([grad_writer, grad_reader], axis=-1) * silu_grad(state_out)
        conv_back, grad_conv_kernel, grad_conv_bias = conv_backward(conv_slope, jnp.zeros((1, rim_rows, INNER), jnp.float32), extended_conv, conv_kernel, SEQ_LEN)
        state_back, grad_state_kernel, grad_state_bias = conv_backward(state_slope, jnp.zeros((1, rim_rows, 2 * STATE), jnp.float32), extended_state, state_kernel, SEQ_LEN)
        proj_grad = jnp.stack([gate_grad, conv_back], axis=2).astype(jnp.bfloat16).reshape(SEQ_LEN, 2 * INNER)
        state_rows = state_back.reshape(SEQ_LEN, 2 * STATE)
        raw_rows = raw_grad.reshape(SEQ_LEN, HEADS)
        normed_grad = contract_cols(proj_grad, in_matrix, False) + contract_cols(state_rows, state_float, True) + contract_cols(raw_rows, delta_float, True)
        normed_grad = normed_grad.reshape(1, SEQ_LEN, D)
        normed_float = normed_rows.astype(jnp.float32)
        grad_in_part = contract_rows(normed_rows, proj_grad, False).reshape(D, 2, INNER)
        grad_state_part = contract_rows(normed_float, state_rows, True).reshape(D, 2, STATE)
        grad_delta_part = contract_rows(normed_float, raw_rows, True)
        grad_norm_gain = lax.optimization_barrier(jnp.sum(normed_grad * input_float * inverse, axis=(0, 1)))
        scaled_in = normed_grad * norm_gain
        in_mean = lax.optimization_barrier(jnp.mean(scaled_in * input_float, axis=-1, keepdims=True))
        input_part = upstream + (inverse * scaled_in - input_float * inverse ** 3 * in_mean)[0]
        joined = jnp.concatenate([grad_conv_kernel.reshape(-1), grad_conv_bias, grad_gate_gain, grad_state_kernel.reshape(-1), grad_state_bias, grad_delta_bias, grad_log_rates, grad_skip, grad_norm_gain])
        packed_part = jnp.pad(joined, (0, PACK - joined.shape[0]))
        totals = (totals[0] + grad_in_part, totals[1] + grad_delta_part, totals[2] + grad_out_part, totals[3] + grad_state_part, totals[4] + packed_part)
        return (totals, (result, input_part))
    start_totals = (jnp.zeros((D, 2, INNER), jnp.float32), jnp.zeros((D, HEADS), jnp.float32), jnp.zeros((D, INNER), jnp.float32), jnp.zeros((D, 2, STATE), jnp.float32), jnp.zeros((PACK,), jnp.float32))
    totals, (layer_output, input_grad) = lax.scan(one_sequence, start_totals, (layer_input, cotangent))
    grad_in, grad_delta, grad_out, grad_state, grad_packed = totals
    new_in, next_moment_in, next_square_in = adam_update(in_proj, moment_in, square_in, grad_in, MATRIX_RATE)
    new_delta, next_moment_delta, next_square_delta = adam_update(delta_proj, moment_delta, square_delta, grad_delta, MATRIX_RATE)
    new_out, next_moment_out, next_square_out = adam_update(out_proj, moment_out, square_out, grad_out, MATRIX_RATE)
    new_state, next_moment_state, next_square_state = adam_update(state_proj, moment_state, square_state, grad_state, MATRIX_RATE)
    new_packed, next_moment_packed, next_square_packed = adam_update(packed_params, moment_packed, square_packed, grad_packed, PACKED_RATE)
    return (layer_output, input_grad, grad_in, grad_delta, grad_out, grad_state, grad_packed, new_in, new_delta, new_out, new_state, new_packed, next_moment_in, next_moment_delta, next_moment_out, next_moment_state, next_moment_packed, next_square_in, next_square_delta, next_square_out, next_square_state, next_square_packed)
```

```python
import functools

import jax
import jax.numpy as jnp
from jax import lax
from jax.experimental import pallas as pl
from jax.experimental.pallas import tpu as pltpu
from jax.sharding import PartitionSpec as P

D = 1536
HEADS = 48
HEAD_DIM = 64
STATE = 128
CONV = 4
STEP = 3
INNER = 3072
LANES = 128

NORM_EPS = 1e-05
BETA_ONE = 0.9
BETA_TWO = 0.999
ADAM_EPS = 1e-08
DECAY_RATE = 0.1
MATRIX_RATE = 0.01
PACKED_RATE = 0.1
HIGH = lax.Precision.HIGHEST
MESH = pl.DeviceIdType.MESH
BF = jnp.bfloat16
F32 = jnp.float32


def cdiv(a, b):
    return -(-a // b)


def gather_kernel(sizes, in_ref, out_ref, local_sem, send_sem, recv_sem):
    n_dp, n_ctx, n_t = sizes
    d, c, t = lax.axis_index("dp"), lax.axis_index("ctx"), lax.axis_index("tensor")
    peers = []
    for k in range(1, n_ctx):
        peers.append((d, lax.rem(c + k, n_ctx), t))
    for k in range(1, n_t):
        peers.append((d, c, lax.rem(t + k, n_t)))
    for k in range(1, n_dp):
        peers.append((lax.rem(d + k, n_dp), c, t))
    barrier = pltpu.get_barrier_semaphore()
    for peer in peers:
        pl.semaphore_signal(barrier, inc=1, device_id=peer, device_id_type=MESH)
    pl.semaphore_wait(barrier, len(peers))
    own = pltpu.make_async_copy(in_ref, out_ref.at[d, c, t], local_sem)
    own.start()
    own.wait()
    number = 0

    def stage(copies):
        for copy in copies:
            copy.start()
        for copy in copies:
            copy.wait()

    copies = []
    for k in range(1, n_ctx):
        view = out_ref.at[d, c, t]
        copies.append(
            pltpu.make_async_remote_copy(
                src_ref=view,
                dst_ref=view,
                send_sem=send_sem.at[number],
                recv_sem=recv_sem.at[number],
                device_id=(d, lax.rem(c + k, n_ctx), t),
                device_id_type=MESH,
            )
        )
        number += 1
    stage(copies)
    copies = []
    for k in range(1, n_t):
        view = out_ref.at[d, :, t]
        copies.append(
            pltpu.make_async_remote_copy(
                src_ref=view,
                dst_ref=view,
                send_sem=send_sem.at[number],
                recv_sem=recv_sem.at[number],
                device_id=(d, c, lax.rem(t + k, n_t)),
                device_id_type=MESH,
            )
        )
        number += 1
    stage(copies)
    copies = []
    for k in range(1, n_dp):
        view = out_ref.at[d]
        copies.append(
            pltpu.make_async_remote_copy(
                src_ref=view,
                dst_ref=view,
                send_sem=send_sem.at[number],
                recv_sem=recv_sem.at[number],
                device_id=(lax.rem(d + k, n_dp), c, t),
                device_id_type=MESH,
            )
        )
        number += 1
    stage(copies)


def gather_small(block, sizes):
    count = sum(sizes) - 3
    return pl.pallas_call(
        functools.partial(gather_kernel, sizes),
        out_shape=jax.ShapeDtypeStruct(sizes + block.shape, block.dtype),
        in_specs=[pl.BlockSpec(memory_space=pltpu.VMEM)],
        out_specs=pl.BlockSpec(memory_space=pltpu.VMEM),
        scratch_shapes=[
            pltpu.SemaphoreType.DMA(()),
            pltpu.SemaphoreType.DMA((count,)),
            pltpu.SemaphoreType.DMA((count,)),
        ],
        compiler_params=pltpu.CompilerParams(collective_id=0, has_side_effects=True),
        name="gather_small",
    )(block)


PAIR = LANES // HEAD_DIM


def matmul(left, right, contract):
    return lax.dot_general(
        left, right, ((contract[:1], contract[1:]), ((), ())), preferred_element_type=F32
    )


def split(value):
    high = value.astype(BF)
    return high, (value - high.astype(F32)).astype(BF)


def dot_exact_right(left, right, contract):
    high, low = split(left)
    return matmul(high, right, contract) + matmul(low, right, contract)


def dot_exact_left(left, right, contract):
    high, low = split(right)
    return matmul(left, high, contract) + matmul(left, low, contract)


def dot_terms(left, right, contract):
    left_high, left_low = split(left)
    right_high, right_low = split(right)
    return (
        matmul(left_high, right_high, contract)
        + matmul(left_high, right_low, contract)
        + matmul(left_low, right_high, contract)
    )


def column(values, head):
    lanes = lax.broadcasted_iota(jnp.int32, values.shape, 1)
    return jnp.sum(jnp.where(lanes == head, values, 0.0), axis=1, keepdims=True)


def spread_heads(values, first):
    tokens = values.shape[0]
    lanes = lax.broadcasted_iota(jnp.int32, (tokens, LANES), 1)
    result = column(values, first)
    for k in range(1, PAIR):
        result = jnp.where(lanes < k * HEAD_DIM, result, column(values, first + k))
    return jnp.broadcast_to(result, (tokens, LANES))


def place_heads(values, first, heads):
    tokens = values.shape[0]
    lanes = lax.broadcasted_iota(jnp.int32, (tokens, LANES), 1)
    columns = lax.broadcasted_iota(jnp.int32, (tokens, heads), 1)
    total = jnp.zeros((tokens, heads), F32)
    for k in range(PAIR):
        mine = (lanes >= k * HEAD_DIM) & (lanes < (k + 1) * HEAD_DIM)
        summed = jnp.sum(jnp.where(mine, values, 0.0), axis=1, keepdims=True)
        total = jnp.where(columns == first + k, summed, total)
    return total


def within_kernel(x_ref, w_ref, r_ref, cum_ref, cum_t_ref, delta_t_ref, out_ref, score_ref):
    step = pl.program_id(1)
    tokens = x_ref.shape[1]
    edge = min(tokens, LANES)

    @pl.when(step == 0)
    def _():
        score_ref[...] = matmul(r_ref[0], w_ref[0], (1, 1))

    lanes = lax.broadcasted_iota(jnp.int32, (edge, LANES), 1)
    for top in range(0, tokens, edge):
        wide = top + edge
        rows_at = top + lax.broadcasted_iota(jnp.int32, (edge, wide), 0)
        causal = rows_at >= lax.broadcasted_iota(jnp.int32, (edge, wide), 1)
        x = x_ref[0, :wide, :]
        result = None
        for k in range(PAIR):
            head = step * PAIR + k
            down = column(cum_ref[0, top:wide, :], head)
            across = cum_t_ref[0, pl.ds(head, 1), :][:, :wide]
            scale = delta_t_ref[0, pl.ds(head, 1), :][:, :wide]
            decays = jnp.exp(jnp.where(causal, down - across, -1e30))
            mixing = decays * (score_ref[top:wide, :wide] * scale)
            part = dot_exact_right(mixing, x, (1, 0))
            result = part if k == 0 else jnp.where(lanes < k * HEAD_DIM, result, part)
        out_ref[0, top:wide, :] = result


def gate_kernel(
    within_ref, x_ref, z_ref, r_ref, growth_ref, enter_ref, skip_ref, plain_ref, mixed_ref, sum_ref
):
    step = pl.program_id(1)
    carried = dot_exact_left(r_ref[0], enter_ref[0], (1, 1))
    plain = within_ref[0] + carried * spread_heads(growth_ref[0], step * PAIR)
    plain_ref[0] = plain
    gate = z_ref[0].astype(F32)
    mixed = (plain + skip_ref[...] * x_ref[0].astype(F32)) * (gate * jax.nn.sigmoid(gate))
    mixed_ref[0] = mixed

    @pl.when(step == 0)
    def _():
        sum_ref[...] = jnp.zeros_like(sum_ref)

    sum_ref[0] += jnp.sum(mixed * mixed, axis=1, keepdims=True)


def within_back_kernel(
    dy_ref, x_ref, w_ref, r_ref, cum_ref, cum_t_ref, delta_ref, bare_ref, dw_ref, dr_ref,
    score_ref, total_ref,
):
    step = pl.program_id(1)
    tokens = x_ref.shape[1]
    edge = min(tokens, LANES)

    @pl.when(step == 0)
    def _():
        score_ref[...] = matmul(w_ref[0], r_ref[0], (1, 1))
        total_ref[...] = jnp.zeros_like(total_ref)

    for top in range(0, tokens, edge):
        wide = tokens - top
        rows_at = lax.broadcasted_iota(jnp.int32, (edge, wide), 0)
        causal = rows_at <= lax.broadcasted_iota(jnp.int32, (edge, wide), 1)
        x = x_ref[0, top : top + edge, :]
        dy = dy_ref[0, top:, :]
        lanes = lax.broadcasted_iota(jnp.int32, (wide, LANES), 1)
        near = lax.broadcasted_iota(jnp.int32, (edge, LANES), 1)
        dy_high, dy_low = split(dy)
        zero = jnp.zeros_like(dy_high)
        result = None
        added = None
        for k in range(PAIR):
            head = step * PAIR + k
            down = column(cum_ref[0, top : top + edge, :], head)
            across = cum_t_ref[0, pl.ds(head, 1), :][:, top:]
            decays = jnp.exp(jnp.where(causal, across - down, -1e30))
            mixing = decays * score_ref[top : top + edge, top:]
            high, low = split(mixing)
            part = matmul(high, dy_high, (1, 0)) + matmul(high, dy_low, (1, 0))
            part = part + matmul(low, dy_high, (1, 0))
            result = part if k == 0 else jnp.where(near < k * HEAD_DIM, result, part)
            mine = (lanes >= k * HEAD_DIM) & (lanes < (k + 1) * HEAD_DIM)
            pairs = matmul(x, jnp.where(mine, dy_high, zero), (1, 1))
            pairs = pairs + matmul(x, jnp.where(mine, dy_low, zero), (1, 1))
            term = pairs * decays * column(delta_ref[0, top : top + edge, :], head)
            added = term if k == 0 else added + term
        bare_ref[0, top : top + edge, :] = result
        total_ref[top : top + edge, top:] += added

    @pl.when(step == pl.num_programs(1) - 1)
    def _():
        high, low = split(total_ref[...])
        dw_ref[0] = matmul(high, r_ref[0], (1, 0)) + matmul(low, r_ref[0], (1, 0))
        dr_ref[0] = matmul(high, w_ref[0], (0, 0)) + matmul(low, w_ref[0], (0, 0))


def state_back_kernel(
    dy_ref, x_ref, plain_ref, bare_ref, w_ref, delta_ref, fading_ref, growth_ref, enter_ref,
    leave_ref, skip_ref, dw_in_ref, dr_in_ref, dx_ref, dw_ref, dr_ref, bare_dot_ref, fade_dot_ref,
    plain_dot_ref, skip_dot_ref,
):
    step = pl.program_id(1)
    first = step * PAIR
    heads = delta_ref.shape[2]

    @pl.when(step == 0)
    def _():
        dw_ref[...] = dw_in_ref[...]
        dr_ref[...] = dr_in_ref[...]
        bare_dot_ref[...] = jnp.zeros_like(bare_dot_ref)
        fade_dot_ref[...] = jnp.zeros_like(fade_dot_ref)
        plain_dot_ref[...] = jnp.zeros_like(plain_dot_ref)

    x = x_ref[0].astype(F32)
    dy = dy_ref[0]
    bare = bare_ref[0]
    fading = spread_heads(fading_ref[0], first)
    reach = dot_exact_left(w_ref[0], leave_ref[0], (1, 1))
    dx_ref[0] = (
        spread_heads(delta_ref[0], first) * bare + fading * reach + skip_ref[...] * dy
    )
    dr_ref[0] += dot_terms(dy * spread_heads(growth_ref[0], first), enter_ref[0], (1, 0))
    dw_ref[0] += dot_terms(x * fading, leave_ref[0], (1, 0))
    bare_dot_ref[0] += place_heads(x * bare, first, heads)
    fade_dot_ref[0] += place_heads(x * reach, first, heads)
    plain_dot_ref[0] += place_heads(dy * plain_ref[0], first, heads)
    skip_dot_ref[0] = jnp.sum(dy * x, axis=0, keepdims=True)


def scan_specs(seqs, tokens, inner, heads):
    tile = pl.BlockSpec((1, tokens, LANES), lambda s, j: (s, 0, j))
    state = pl.BlockSpec((1, tokens, STATE), lambda s, j: (s, 0, 0))
    per_head = pl.BlockSpec((1, tokens, heads), lambda s, j: (s, 0, 0))
    per_head_t = pl.BlockSpec((1, heads, tokens), lambda s, j: (s, 0, 0))
    carry = pl.BlockSpec((1, LANES, STATE), lambda s, j: (s, j, 0))
    lane = pl.BlockSpec((1, LANES), lambda s, j: (0, j))
    one = pl.BlockSpec((1, tokens, 1), lambda s, j: (s, 0, 0))
    lane_sum = pl.BlockSpec((1, 1, LANES), lambda s, j: (s, 0, j))
    return tile, state, per_head, per_head_t, carry, lane, one, lane_sum


def shaped(*shape):
    return jax.ShapeDtypeStruct(shape, F32)


def scan_call(kernel, name, grid, in_specs, out_specs, out_shape, scratch, flops, moved):
    return pl.pallas_call(
        kernel,
        grid=grid,
        in_specs=in_specs,
        out_specs=out_specs,
        out_shape=out_shape,
        scratch_shapes=scratch,
        name=name,
        cost_estimate=pl.CostEstimate(flops=flops, bytes_accessed=moved, transcendentals=0),
    )


def scan_within(x, w, r, cum, cum_t, delta_t):
    seqs, tokens, inner = x.shape
    heads = cum.shape[2]
    tile, state, per_head, per_head_t, _, _, _, _ = scan_specs(seqs, tokens, inner, heads)
    size = seqs * tokens * inner
    return scan_call(
        within_kernel, "scan_within", (seqs, inner // LANES),
        [tile, state, state, per_head, per_head_t, per_head_t], tile, shaped(seqs, tokens, inner),
        [pltpu.VMEM((tokens, tokens), F32)], 16 * size * tokens, 6 * size,
    )(x, w, r, cum, cum_t, delta_t)


def scan_gate(within, x, z, r, growth, enter, skip):
    seqs, tokens, inner = x.shape
    heads = growth.shape[2]
    tile, state, per_head, _, carry, lane, one, _ = scan_specs(seqs, tokens, inner, heads)
    size = seqs * tokens * inner
    return scan_call(
        gate_kernel, "scan_gate", (seqs, inner // LANES),
        [tile, tile, tile, state, per_head, carry, lane], [tile, tile, one],
        [shaped(seqs, tokens, inner), shaped(seqs, tokens, inner), shaped(seqs, tokens, 1)],
        [], 8 * size * STATE, 16 * size,
    )(within, x, z, r, growth, enter, skip)


def scan_within_back(dy, x, w, r, cum, cum_t, delta):
    seqs, tokens, inner = x.shape
    heads = cum.shape[2]
    tile, state, per_head, per_head_t, _, _, _, _ = scan_specs(seqs, tokens, inner, heads)
    size = seqs * tokens * inner
    square = pltpu.VMEM((tokens, tokens), F32)
    return scan_call(
        within_back_kernel, "scan_within_back", (seqs, inner // LANES),
        [tile, tile, state, state, per_head, per_head_t, per_head], [tile, state, state],
        [shaped(seqs, tokens, inner), shaped(seqs, tokens, STATE), shaped(seqs, tokens, STATE)],
        [square, square], 32 * size * tokens, 10 * size,
    )(dy, x, w, r, cum, cum_t, delta)


def scan_state_back(dy, x, plain, bare, w, delta, fading, growth, enter, leave, skip, dw, dr):
    seqs, tokens, inner = x.shape
    heads = delta.shape[2]
    tile, state, per_head, _, carry, lane, _, lane_sum = scan_specs(seqs, tokens, inner, heads)
    size = seqs * tokens * inner
    sums = shaped(seqs, tokens, heads)
    return scan_call(
        state_back_kernel, "scan_state_back", (seqs, inner // LANES),
        [tile] * 4 + [state] + [per_head] * 3 + [carry, carry, lane, state, state],
        [tile, state, state, per_head, per_head, per_head, lane_sum],
        [shaped(seqs, tokens, inner), shaped(seqs, tokens, STATE), shaped(seqs, tokens, STATE)]
        + [sums] * 3 + [shaped(seqs, 1, inner)],
        [], 24 * size * STATE, 22 * size,
    )(dy, x, plain, bare, w, delta, fading, growth, enter, leave, skip, dw, dr)


def from_behind(value, axis, steps):
    count = lax.axis_size(axis)
    initial, last = (max(0, -steps), min(count, count - steps))
    return lax.ppermute(value, axis, [(source, source + steps) for source in range(initial, last)])


def swap(value):
    return lax.ppermute(value, "tensor", [(0, 1), (1, 0)])


def sum_tensor(value):
    if lax.axis_size("tensor") == 2:
        return value + swap(value)
    return lax.psum(value, "tensor")


def scatter_tensor(make, width, rank):
    if lax.axis_size("tensor") == 2:
        away = swap(make((1 - rank) * width))
        return make(rank * width), away
    whole = jnp.concatenate([make(k * width) for k in range(lax.axis_size("tensor"))], axis=-1)
    return lax.psum_scatter(whole, "tensor", scatter_dimension=whole.ndim - 1, tiled=True), 0.0


def scatter_rows(left, right):
    n_dp, n_ctx = lax.axis_size("dp"), lax.axis_size("ctx")
    if n_dp != 4:
        part = dot(left, right, (0, 0))
        return lax.psum_scatter(part, ("dp", "ctx"), scatter_dimension=0, tiled=True)
    d, c = lax.axis_index("dp"), lax.axis_index("ctx")
    low, high = lax.rem(d, 2), d // 2
    rows = left.shape[1] // n_dp

    def part(high_at, low_at):
        cut = lax.dynamic_slice_in_dim(left, (2 * high_at + low_at) * rows, rows, 1)
        return dot(cut, right, (0, 0))

    def over(value, flip):
        return lax.ppermute(value, "dp", [(k, k ^ flip) for k in range(n_dp)])

    away = part(1 - high, 1 - low), part(high, 1 - low)
    near = over(away[0], 1), over(away[1], 1)
    far = over(part(1 - high, low) + near[0], 2)
    held = part(high, low) + near[1] + far
    block = rows // n_ctx
    total = lax.dynamic_slice_in_dim(held, c * block, block, 0)
    for k in range(1, n_ctx):
        give = lax.dynamic_slice_in_dim(held, lax.rem(c + k, n_ctx) * block, block, 0)
        total = total + lax.ppermute(give, "ctx", [(m, (m + k) % n_ctx) for m in range(n_ctx)])
    return total


def chain(own, totals, backward):
    count = lax.axis_size("ctx")
    received, entering = None, None
    for hop in range(count - 1):
        leaving = own if hop == 0 else totals * received + own
        pair = (count - 1 - hop, count - 2 - hop) if backward else (hop, hop + 1)
        received = lax.ppermute(leaving, "ctx", [pair])
        entering = received if hop == 0 else entering + received
    return jnp.zeros_like(own) if entering is None else entering


def segment_lengths():
    return [CONV * INNER, INNER, INNER, 2 * CONV * STATE, 2 * STATE, HEADS, HEADS, HEADS, D]


def unpack(flat):
    pieces = []
    offset = 0
    for length in segment_lengths():
        pieces.append(flat[offset : offset + length])
        offset += length
    return pieces


def silu_grad(value):
    sigma = jax.nn.sigmoid(value)
    return sigma * (1.0 + value * (1.0 - sigma))


def conv_forward(extended, kernel, offset_bias, length):
    total = jnp.zeros(extended[:, :length].shape, F32) + offset_bias
    for tap_index in range(CONV):
        total = total + kernel[tap_index] * extended[:, tap_index : tap_index + length]
    return total


def conv_backward(slope, follow, extended, kernel, length):
    padded = jnp.concatenate([slope, follow], axis=1)
    grad_input = jnp.zeros(slope.shape, F32)
    kernel_grads = []
    for tap_index in range(CONV):
        begin = CONV - 1 - tap_index
        grad_input = grad_input + kernel[tap_index] * padded[:, begin : begin + length]
        kernel_grads.append(
            jnp.sum(slope * extended[:, tap_index : tap_index + length], axis=(0, 1))
        )
    return (grad_input, jnp.stack(kernel_grads), jnp.sum(slope, axis=(0, 1)))


def dot(left, right, contract, exact=False):
    return lax.dot_general(
        left,
        right,
        ((contract[:1], contract[1:]), ((), ())),
        precision=HIGH if exact else None,
        preferred_element_type=F32,
    )


def adam_update(weight, moment, second, gradient, rate):
    moment = BETA_ONE * moment + (1.0 - BETA_ONE) * gradient
    second = BETA_TWO * second + (1.0 - BETA_TWO) * gradient * gradient
    moment_hat = moment / (1.0 - BETA_ONE**STEP)
    second_hat = second / (1.0 - BETA_TWO**STEP)
    weight = weight - rate * (moment_hat / (jnp.sqrt(second_hat) + ADAM_EPS) + DECAY_RATE * weight)
    return (weight, moment, second)


def einsum(spec, *parts):
    return jnp.einsum(spec, *parts, precision=HIGH, preferred_element_type=F32)


def on_device(
    layer_input,
    cotangent,
    in_proj,
    delta_proj,
    out_proj,
    state_proj,
    packed_params,
    moment_in,
    moment_delta,
    moment_out,
    moment_state,
    moment_packed,
    square_in,
    square_delta,
    square_out,
    square_state,
    square_packed,
):
    sizes = (lax.axis_size("dp"), lax.axis_size("ctx"), lax.axis_size("tensor"))
    n_dp, n_ctx, n_t = sizes
    groups = n_dp * n_ctx
    rank = lax.axis_index("tensor")
    seqs, tokens, width = layer_input.shape
    rows = seqs * tokens
    local_inner = in_proj.shape[2]
    local_heads = delta_proj.shape[1]
    own_width = width // n_t
    rim = CONV - 1

    state_rows_own = state_proj.shape[0]
    pack_own = packed_params.shape[0]
    state_piece = jnp.concatenate(
        [state_proj[:, 0].astype(BF), state_proj[:, 1].astype(BF)], axis=0
    )
    state_pad = cdiv(2 * state_rows_own, 16) * 16
    delta_pad = cdiv(local_heads, 16) * 16
    pack_rows = cdiv(pack_own, LANES)
    pack_pad = cdiv(pack_rows, 16) * 16
    proj_rows = delta_proj.shape[0]
    block = jnp.concatenate(
        [
            jnp.pad(state_piece, ((0, state_pad - 2 * state_rows_own), (0, 0))),
            jnp.pad(
                delta_proj.astype(BF).T, ((0, delta_pad - local_heads), (0, LANES - proj_rows))
            ),
            jnp.pad(
                jnp.pad(packed_params.astype(BF), (0, pack_rows * LANES - pack_own)).reshape(
                    pack_rows, LANES
                ),
                ((0, pack_pad - pack_rows), (0, 0)),
            ),
        ],
        axis=0,
    )
    small = gather_small(block, sizes)
    wx = lax.all_gather(in_proj[:, 1].astype(BF), ("dp", "ctx"), axis=0, tiled=True)
    wz = lax.all_gather(in_proj[:, 0].astype(BF), ("dp", "ctx"), axis=0, tiled=True)
    wo = lax.all_gather(out_proj.astype(BF), ("dp", "ctx"), axis=0, tiled=True)
    up_own = cotangent.astype(BF)
    if n_t == 2:
        up_away = swap(up_own)
        first = rank == 0
        up_full = jnp.concatenate(
            [jnp.where(first, up_own, up_away), jnp.where(first, up_away, up_own)], axis=2
        )
    else:
        up_full = lax.all_gather(up_own, "tensor", axis=2, tiled=True)
    up_rows = up_full.reshape(rows, width)

    state_slots = small[..., : 2 * state_rows_own, :].reshape(-1, 2, state_rows_own, STATE)
    ws = jnp.concatenate(
        [state_slots[:, 0].reshape(width, STATE), state_slots[:, 1].reshape(width, STATE)], axis=1
    )
    delta_slots = lax.dynamic_index_in_dim(small, rank, 2, False)
    delta_slots = delta_slots[..., state_pad : state_pad + local_heads, :proj_rows]
    wd = delta_slots.reshape(groups, local_heads, proj_rows).transpose(0, 2, 1)
    wd = wd.reshape(width, local_heads)
    pack_slots = small[..., state_pad + delta_pad : state_pad + delta_pad + pack_rows, :]
    packed = pack_slots.reshape(groups * n_t, pack_rows * LANES)[:, :pack_own].reshape(-1)
    pieces = unpack(packed.astype(F32))
    conv_kernel = lax.dynamic_slice_in_dim(
        pieces[0].reshape(CONV, INNER), rank * local_inner, local_inner, 1
    )
    conv_bias = lax.dynamic_slice_in_dim(pieces[1], rank * local_inner, local_inner, 0)
    gate_gain = lax.dynamic_slice_in_dim(pieces[2], rank * local_inner, local_inner, 0)
    state_kernel = pieces[3].reshape(CONV, 2 * STATE)
    state_bias = pieces[4]
    delta_bias = lax.dynamic_slice_in_dim(pieces[5], rank * local_heads, local_heads, 0)
    log_rates = lax.dynamic_slice_in_dim(pieces[6], rank * local_heads, local_heads, 0)
    skip_gain = lax.dynamic_slice_in_dim(pieces[7], rank * local_heads, local_heads, 0)
    norm_gain = pieces[8]
    rates = -jnp.exp(log_rates)

    input_float = layer_input.astype(F32)
    inverse = lax.rsqrt(jnp.mean(input_float * input_float, axis=-1, keepdims=True) + NORM_EPS)
    normed = (input_float * inverse * norm_gain).astype(BF).reshape(rows, width)
    sproj = dot(normed, ws, (1, 0)).astype(BF).reshape(seqs, tokens, 2 * STATE)
    raw = dot(normed, wd, (1, 0)).reshape(seqs, tokens, local_heads)
    xproj = dot(normed, wx, (1, 0)).astype(BF).reshape(seqs, tokens, local_inner)
    tails = from_behind(
        jnp.concatenate([xproj[:, tokens - rim :], sproj[:, tokens - rim :]], axis=2), "ctx", 1
    )
    ext_x = jnp.concatenate([tails[:, :, :local_inner], xproj], axis=1).astype(F32)
    ext_s = jnp.concatenate([tails[:, :, local_inner:], sproj], axis=1).astype(F32)
    conv_x = conv_forward(ext_x, conv_kernel, conv_bias, tokens)
    conv_s = conv_forward(ext_s, state_kernel, state_bias, tokens)
    act_x = jax.nn.silu(conv_x).astype(BF)
    act_s = jax.nn.silu(conv_s).astype(BF)
    delta = jax.nn.softplus(raw + delta_bias)
    xs = act_x.astype(F32).reshape(seqs, tokens, local_heads, HEAD_DIM)
    wv = act_s[:, :, :STATE]
    rv = act_s[:, :, STATE:]
    wv32, rv32 = wv.astype(F32), rv.astype(F32)
    cum = jnp.cumsum(delta * rates, axis=1)
    totals = jnp.exp(cum[:, -1])
    fade_decay = jnp.exp(cum[:, -1:] - cum)
    fading = fade_decay * delta
    growth = jnp.exp(cum)
    own_state = einsum("sth,sthp,stn->shpn", fading, xs, wv32)
    spread = totals[:, :, None, None]
    entering = jnp.stack(
        [chain(own_state[s], spread[s], False) for s in range(seqs)], axis=0
    )

    cum_t = jnp.swapaxes(cum, 1, 2)
    skip_lanes = jnp.repeat(skip_gain, HEAD_DIM)[None, :]
    entering = entering.reshape(seqs, local_inner, STATE)
    within = scan_within(act_x, wv, rv, cum, cum_t, jnp.swapaxes(delta, 1, 2))

    zproj = dot(normed, wz, (1, 0)).astype(BF).reshape(seqs, tokens, local_inner)
    plain, mixed, square_sums = scan_gate(within, act_x, zproj, rv, growth, entering, skip_lanes)
    gate_input = zproj.astype(F32)
    gate_act = jax.nn.silu(gate_input)
    mixer = plain + skip_lanes * act_x.astype(F32)
    square_sums = sum_tensor(square_sums[:, :, 0])
    gate_inverse = lax.rsqrt(square_sums / INNER + NORM_EPS)[:, :, None]
    gated = (mixed * gate_inverse * gate_gain).astype(BF).reshape(rows, local_inner)

    def out_columns(start):
        return dot(gated, lax.dynamic_slice_in_dim(wo, start, own_width, 0), (1, 1))

    branch, branch_away = scatter_tensor(out_columns, own_width, rank)
    own_input = lax.dynamic_slice_in_dim(layer_input, rank * own_width, own_width, 2).astype(F32)

    gated_grad = dot(up_rows, wo, (1, 0)).reshape(seqs, tokens, local_inner)
    gated_late, wo = lax.optimization_barrier((gated, wo))
    grad_out_part = dot(up_rows, gated_late, (0, 0))
    grad_out = lax.psum_scatter(grad_out_part, ("dp", "ctx"), scatter_dimension=0, tiled=True)
    scaled = gated_grad * gate_gain
    row_sums = sum_tensor(jnp.sum(scaled * mixed, axis=-1))
    mixed_grad = gate_inverse * scaled - mixed * gate_inverse**3 * (row_sums / INNER)[:, :, None]
    grad_gate_gain = jnp.sum(gated_grad * mixed * gate_inverse, axis=(0, 1))
    mixer_grad = mixed_grad * gate_act
    z_grad = (mixed_grad * mixer * silu_grad(gate_input)).astype(BF).reshape(rows, local_inner)
    grad_z_part = dot(normed, z_grad, (0, 0))

    dy = mixer_grad.reshape(seqs, tokens, local_heads, HEAD_DIM)
    pulled = einsum("sth,sthp,stn->shpn", growth, dy, rv32)
    leaving = jnp.stack([chain(pulled[s], spread[s], True) for s in range(seqs)], axis=0)
    dy, grad_z_part = lax.optimization_barrier((dy, grad_z_part))
    grad_z = lax.psum_scatter(grad_z_part, ("dp", "ctx"), scatter_dimension=0, tiled=True)
    dy = dy.reshape(seqs, tokens, local_inner)
    leaving = leaving.reshape(seqs, local_inner, STATE)
    dx_bare, dw, dr = scan_within_back(dy, act_x, wv, rv, cum, cum_t, delta)
    dx, dw, dr, bare_dot, fade_dot, plain_dot, skip_dot = scan_state_back(
        dy, act_x, plain, dx_bare, wv, delta, fading, growth, entering, leaving, skip_lanes, dw, dr
    )
    cum_grad = plain_dot - delta * bare_dot - fading * fade_dot
    end_grad = jnp.sum(fading * fade_dot, axis=1) + totals * jnp.sum(
        (leaving * entering).reshape(seqs, local_heads, HEAD_DIM, STATE), axis=(2, 3)
    )
    step_grad = (
        lax.cumsum(cum_grad, axis=1, reverse=True) + end_grad[:, None, :]
    )
    delta_grad = bare_dot + fade_decay * fade_dot + rates * step_grad
    grad_rates = jnp.sum(delta * step_grad, axis=(0, 1))
    grad_skip = jnp.sum(skip_dot.reshape(seqs, local_heads, HEAD_DIM), axis=(0, 2))
    grad_log_rates = grad_rates * rates
    raw_grad = delta_grad * jax.nn.sigmoid(raw + delta_bias)
    grad_delta_bias = jnp.sum(raw_grad, axis=(0, 1))

    slope_x = dx.reshape(seqs, tokens, local_inner) * silu_grad(conv_x)
    slope_s = jnp.concatenate([dw, dr], axis=-1) * silu_grad(conv_s)
    follow = from_behind(
        jnp.concatenate([slope_x[:, :rim], slope_s[:, :rim]], axis=2), "ctx", -1
    )
    back_x, grad_conv_kernel, grad_conv_bias = conv_backward(
        slope_x, follow[:, :, :local_inner], ext_x, conv_kernel, tokens
    )
    back_s, grad_state_kernel, grad_state_bias = conv_backward(
        slope_s, follow[:, :, local_inner:], ext_s, state_kernel, tokens
    )
    x_grad = back_x.astype(BF).reshape(rows, local_inner)
    state_rows = back_s.reshape(rows, 2 * STATE)
    raw_rows = raw_grad.reshape(rows, local_heads)

    def normed_columns(start):
        def cut(weight):
            return lax.dynamic_slice_in_dim(weight, start, own_width, 0)

        return (
            dot(x_grad, cut(wx), (1, 1))
            + dot(z_grad, cut(wz), (1, 1))
            + dot(state_rows, cut(ws).astype(F32), (1, 1), True)
            + dot(raw_rows, cut(wd).astype(F32), (1, 1), True)
        )

    x_grad, branch_away, grad_out = lax.optimization_barrier((x_grad, branch_away, grad_out))
    layer_output = own_input + (branch + branch_away).reshape(seqs, tokens, own_width)
    normed_grad, normed_away = scatter_tensor(normed_columns, own_width, rank)
    normed_grad = (normed_grad + normed_away).reshape(seqs, tokens, own_width)
    own_gain = lax.dynamic_slice_in_dim(norm_gain, rank * own_width, own_width, 0)
    grad_norm_gain = jnp.sum(normed_grad * own_input * inverse, axis=(0, 1))
    scaled_in = normed_grad * own_gain
    in_mean = sum_tensor(jnp.sum(scaled_in * own_input, axis=-1, keepdims=True)) / width
    input_grad = cotangent + inverse * scaled_in - own_input * inverse**3 * in_mean

    normed_float = normed.astype(F32)
    pieces_x = 3 if local_inner % (3 * LANES) == 0 else 1
    piece = local_inner // pieces_x
    grad_x = jnp.concatenate(
        [
            scatter_rows(normed, x_grad[:, k * piece : (k + 1) * piece])
            for k in range(pieces_x)
        ],
        axis=1,
    )
    grad_state_part = dot(normed_float, state_rows, (0, 0), True)
    grad_delta_part = dot(normed_float, raw_rows, (0, 0), True)

    def widen(local_values, full_length):
        return lax.dynamic_update_slice_in_dim(
            jnp.zeros((full_length,), F32), local_values, rank * local_values.shape[0], 0
        )

    conv_wide = lax.dynamic_update_slice_in_dim(
        jnp.zeros((CONV, INNER), F32), grad_conv_kernel, rank * local_inner, 1
    ).reshape(-1)
    joined = jnp.concatenate(
        [
            conv_wide,
            widen(grad_conv_bias, INNER),
            widen(grad_gate_gain, INNER),
            grad_state_kernel.reshape(-1),
            grad_state_bias,
            widen(grad_delta_bias, HEADS),
            widen(grad_log_rates, HEADS),
            widen(grad_skip, HEADS),
            widen(grad_norm_gain, D),
        ]
    )
    pack_group = n_t * pack_own
    packed_part = jnp.pad(joined, (0, groups * pack_group - joined.shape[0]))
    pack_cols = cdiv(pack_group, proj_rows)
    packed_part = jnp.pad(
        packed_part.reshape(groups, pack_group), ((0, 0), (0, pack_cols * proj_rows - pack_group))
    ).reshape(width, pack_cols)
    extra_pad = cdiv(local_heads + pack_cols, LANES) * LANES - local_heads - pack_cols
    tail_part = jnp.concatenate(
        [
            grad_state_part,
            grad_delta_part,
            packed_part,
            jnp.zeros((width, extra_pad), F32),
        ],
        axis=1,
    )
    tail_part, grad_z = lax.optimization_barrier((tail_part, grad_z))
    tail = lax.psum_scatter(tail_part, ("dp", "ctx"), scatter_dimension=0, tiled=True)
    at = 2 * STATE
    grad_delta = tail[:, at : at + local_heads]
    state_group = tail[:, :at]
    packed_group = tail[:, at + local_heads : at + local_heads + pack_cols]
    packed_group = packed_group.reshape(-1)[:pack_group]
    if n_t == 2:
        away = swap(
            (
                lax.dynamic_slice_in_dim(
                    state_group, (1 - rank) * state_rows_own, state_rows_own, 0
                ),
                lax.dynamic_slice_in_dim(packed_group, (1 - rank) * pack_own, pack_own, 0),
            )
        )
        grad_state = (
            lax.dynamic_slice_in_dim(state_group, rank * state_rows_own, state_rows_own, 0)
            + away[0]
        )
        grad_packed = (
            lax.dynamic_slice_in_dim(packed_group, rank * pack_own, pack_own, 0) + away[1]
        )
    else:
        grad_state = lax.psum_scatter(state_group, "tensor", scatter_dimension=0, tiled=True)
        grad_packed = lax.psum_scatter(packed_group, "tensor", scatter_dimension=0, tiled=True)
    grad_state = grad_state.reshape(state_rows_own, 2, STATE)
    grad_in = jnp.stack([grad_z, grad_x], axis=1)

    new_in, next_moment_in, next_square_in = adam_update(
        in_proj, moment_in, square_in, grad_in, MATRIX_RATE
    )
    new_delta, next_moment_delta, next_square_delta = adam_update(
        delta_proj, moment_delta, square_delta, grad_delta, MATRIX_RATE
    )
    new_out, next_moment_out, next_square_out = adam_update(
        out_proj, moment_out, square_out, grad_out, MATRIX_RATE
    )
    new_state, next_moment_state, next_square_state = adam_update(
        state_proj, moment_state, square_state, grad_state, MATRIX_RATE
    )
    new_packed, next_moment_packed, next_square_packed = adam_update(
        packed_params, moment_packed, square_packed, grad_packed, PACKED_RATE
    )
    return (
        layer_output,
        input_grad,
        grad_in,
        grad_delta,
        grad_out,
        grad_state,
        grad_packed,
        new_in,
        new_delta,
        new_out,
        new_state,
        new_packed,
        next_moment_in,
        next_moment_delta,
        next_moment_out,
        next_moment_state,
        next_moment_packed,
        next_square_in,
        next_square_delta,
        next_square_out,
        next_square_state,
        next_square_packed,
    )


def solution(mesh):
    matrix = P(("dp", "ctx"), "tensor")
    projection = P(("dp", "ctx"), None, "tensor")
    state = P(("dp", "ctx", "tensor"), None, None)
    flat = P(("dp", "ctx", "tensor"))
    tokens = P("dp", "ctx", "tensor")
    weights = (projection, matrix, matrix, state, flat)
    return jax.shard_map(
        on_device,
        mesh=mesh,
        in_specs=(P("dp", "ctx", None), tokens) + weights * 3,
        out_specs=(tokens, tokens) + weights * 4,
        check_vma=False,
    )
```

```python
import functools

import jax
import jax.numpy as jnp
from jax import lax
from jax.experimental import pallas as pl
from jax.experimental.pallas import tpu as pltpu
from jax.sharding import PartitionSpec as P


D = 1536
HEADS = 48
HEAD_DIM = 64
STATE = 128
CONV = 4
STEP = 3
INNER = 3072
LANES = 128

NORM_EPS = 1e-05
BETA_ONE = 0.9
BETA_TWO = 0.999
ADAM_EPS = 1e-08
DECAY_RATE = 0.1
MATRIX_RATE = 0.01
PACKED_RATE = 0.1
HIGH = lax.Precision.HIGHEST
MESH = pl.DeviceIdType.MESH
BF = jnp.bfloat16
F32 = jnp.float32


def cdiv(a, b):
    return -(-a // b)


def gather_kernel(sizes, in_ref, out_ref, local_sem, send_sem, recv_sem):
    n_dp, n_ctx, n_t = sizes
    d, c, t = lax.axis_index("dp"), lax.axis_index("ctx"), lax.axis_index("tensor")
    peers = []
    for k in range(1, n_ctx):
        peers.append((d, lax.rem(c + k, n_ctx), t))
    for k in range(1, n_t):
        peers.append((d, c, lax.rem(t + k, n_t)))
    for k in range(1, n_dp):
        peers.append((lax.rem(d + k, n_dp), c, t))
    barrier = pltpu.get_barrier_semaphore()
    for peer in peers:
        pl.semaphore_signal(barrier, inc=1, device_id=peer, device_id_type=MESH)
    pl.semaphore_wait(barrier, len(peers))
    own = pltpu.make_async_copy(in_ref, out_ref.at[d, c, t], local_sem)
    own.start()
    own.wait()
    number = 0

    def stage(copies):
        for copy in copies:
            copy.start()
        for copy in copies:
            copy.wait()

    copies = []
    for k in range(1, n_ctx):
        view = out_ref.at[d, c, t]
        copies.append(
            pltpu.make_async_remote_copy(
                src_ref=view,
                dst_ref=view,
                send_sem=send_sem.at[number],
                recv_sem=recv_sem.at[number],
                device_id=(d, lax.rem(c + k, n_ctx), t),
                device_id_type=MESH,
            )
        )
        number += 1
    stage(copies)
    copies = []
    for k in range(1, n_t):
        view = out_ref.at[d, :, t]
        copies.append(
            pltpu.make_async_remote_copy(
                src_ref=view,
                dst_ref=view,
                send_sem=send_sem.at[number],
                recv_sem=recv_sem.at[number],
                device_id=(d, c, lax.rem(t + k, n_t)),
                device_id_type=MESH,
            )
        )
        number += 1
    stage(copies)
    copies = []
    for k in range(1, n_dp):
        view = out_ref.at[d]
        copies.append(
            pltpu.make_async_remote_copy(
                src_ref=view,
                dst_ref=view,
                send_sem=send_sem.at[number],
                recv_sem=recv_sem.at[number],
                device_id=(lax.rem(d + k, n_dp), c, t),
                device_id_type=MESH,
            )
        )
        number += 1
    stage(copies)


def gather_small(block, sizes):
    count = sum(sizes) - 3
    return pl.pallas_call(
        functools.partial(gather_kernel, sizes),
        out_shape=jax.ShapeDtypeStruct(sizes + block.shape, block.dtype),
        in_specs=[pl.BlockSpec(memory_space=pltpu.VMEM)],
        out_specs=pl.BlockSpec(memory_space=pltpu.VMEM),
        scratch_shapes=[
            pltpu.SemaphoreType.DMA(()),
            pltpu.SemaphoreType.DMA((count,)),
            pltpu.SemaphoreType.DMA((count,)),
        ],
        compiler_params=pltpu.CompilerParams(collective_id=0, has_side_effects=True),
        name="gather_small",
    )(block)


PAIR = LANES // HEAD_DIM


def step_width(inner):
    return 3 * LANES if inner % (3 * LANES) == 0 else LANES


def matmul(left, right, contract):
    return lax.dot_general(
        left, right, ((contract[:1], contract[1:]), ((), ())), preferred_element_type=F32
    )


def split(value):
    high = value.astype(BF)
    return high, (value - high.astype(F32)).astype(BF)


def dot_exact_right(left, right, contract):
    high, low = split(left)
    return matmul(high, right, contract) + matmul(low, right, contract)


def dot_exact_left(left, right, contract):
    high, low = split(right)
    return matmul(left, high, contract) + matmul(left, low, contract)


def dot_terms(left, right, contract):
    left_high, left_low = split(left)
    right_high, right_low = split(right)
    return (
        matmul(left_high, right_high, contract)
        + matmul(left_high, right_low, contract)
        + matmul(left_low, right_high, contract)
    )


def picker(heads, first, width, each):
    row = lax.broadcasted_iota(jnp.int32, (heads, width), 0)
    lane = lax.broadcasted_iota(jnp.int32, (heads, width), 1)
    return jnp.where(row == first + lane // each, 1.0, 0.0).astype(BF)


def spread_exact(values, first, width, each):
    pick = picker(values.shape[1], first, width, each)
    high = values.astype(BF)
    rest = values - high.astype(F32)
    middle = rest.astype(BF)
    low = (rest - middle.astype(F32)).astype(BF)
    return matmul(high, pick, (1, 0)) + (matmul(middle, pick, (1, 0)) + matmul(low, pick, (1, 0)))


def place_heads(values, first, heads):
    width = values.shape[1]
    lane = lax.broadcasted_iota(jnp.int32, (width, heads), 0)
    column = lax.broadcasted_iota(jnp.int32, (width, heads), 1)
    pick = jnp.where(column == first + lane // HEAD_DIM, 1.0, 0.0).astype(BF)
    return dot_exact_right(values, pick, (1, 0))


def twice(value, wide):
    count = wide // LANES
    return value if count <= 1 else jnp.concatenate([value] * count, axis=1)


def state_kernel(v_ref, u_ref, scale_ref, out_ref):
    width = v_ref.shape[2]
    first = pl.program_id(0) * (width // HEAD_DIM)
    scaled = v_ref[0].astype(F32) * spread_exact(scale_ref[0], first, width, HEAD_DIM)
    out_ref[...] = dot_exact_right(scaled, u_ref[0], (0, 0))


def within_kernel(x_ref, w_ref, r_ref, cum_ref, cum_t_ref, delta_t_ref, out_ref, score_ref, down_ref):
    step = pl.program_id(1)
    tokens, width = x_ref.shape[1:]
    edge = min(tokens, LANES)
    count = width // HEAD_DIM
    first = step * count

    @pl.when(step == 0)
    def _():
        score_ref[...] = matmul(r_ref[0], w_ref[0], (1, 1))

    down_ref[...] = spread_exact(cum_ref[0], first, count * LANES, LANES)
    lanes = lax.broadcasted_iota(jnp.int32, (edge, LANES), 1)
    for top in range(0, tokens, edge):
        wide = top + edge
        rows_at = top + lax.broadcasted_iota(jnp.int32, (edge, wide), 0)
        causal = rows_at >= lax.broadcasted_iota(jnp.int32, (edge, wide), 1)
        score = score_ref[top:wide, :wide]
        for tile in range(width // LANES):
            channels = slice(tile * LANES, (tile + 1) * LANES)
            x = x_ref[0, :wide, channels]
            result = None
            for k in range(PAIR):
                at = tile * PAIR + k
                down = twice(down_ref[top:wide, at * LANES : (at + 1) * LANES], wide)
                across = cum_t_ref[0, pl.ds(first + at, 1), :][:, :wide]
                scale = delta_t_ref[0, pl.ds(first + at, 1), :][:, :wide]
                decays = jnp.exp(jnp.where(causal, down - across, -1e30))
                part = dot_exact_right(decays * (score * scale), x, (1, 0))
                result = part if k == 0 else jnp.where(lanes < k * HEAD_DIM, result, part)
            out_ref[0, top:wide, channels] = result


def gate_kernel(
    within_ref, x_ref, z_ref, r_ref, growth_ref, enter_ref, skip_ref, plain_ref, mixed_ref, sum_ref
):
    step = pl.program_id(1)
    width = x_ref.shape[2]
    first = step * (width // HEAD_DIM)
    carried = dot_exact_left(r_ref[0], enter_ref[0], (1, 1))
    plain = within_ref[0] + carried * spread_exact(growth_ref[0], first, width, HEAD_DIM)
    plain_ref[0] = plain
    gate = z_ref[0].astype(F32)
    mixed = (plain + skip_ref[...] * x_ref[0].astype(F32)) * (gate * jax.nn.sigmoid(gate))
    mixed_ref[0] = mixed

    @pl.when(step == 0)
    def _():
        sum_ref[...] = jnp.zeros_like(sum_ref)

    sum_ref[0] += jnp.sum(mixed * mixed, axis=1, keepdims=True)


def within_back_kernel(
    dy_ref, x_ref, w_ref, r_ref, cum_ref, cum_t_ref, delta_ref, bare_ref, dw_ref, dr_ref,
    score_ref, total_ref, down_ref, scale_ref,
):
    step = pl.program_id(1)
    tokens, width = x_ref.shape[1:]
    edge = min(tokens, LANES)
    count = width // HEAD_DIM
    first = step * count

    @pl.when(step == 0)
    def _():
        score_ref[...] = matmul(w_ref[0], r_ref[0], (1, 1))
        total_ref[...] = jnp.zeros_like(total_ref)

    down_ref[...] = spread_exact(cum_ref[0], first, count * LANES, LANES)
    scale_ref[...] = spread_exact(delta_ref[0], first, count * LANES, LANES)
    for top in range(0, tokens, edge):
        wide = tokens - top
        rows_at = lax.broadcasted_iota(jnp.int32, (edge, wide), 0)
        causal = rows_at <= lax.broadcasted_iota(jnp.int32, (edge, wide), 1)
        lanes = lax.broadcasted_iota(jnp.int32, (wide, LANES), 1)
        near = lax.broadcasted_iota(jnp.int32, (edge, LANES), 1)
        score = score_ref[top : top + edge, top:]
        added = None
        for tile in range(width // LANES):
            channels = slice(tile * LANES, (tile + 1) * LANES)
            x = x_ref[0, top : top + edge, channels]
            dy_high, dy_low = split(dy_ref[0, top:, channels])
            zero = jnp.zeros_like(dy_high)
            result = None
            for k in range(PAIR):
                at = tile * PAIR + k
                down = twice(down_ref[top : top + edge, at * LANES : (at + 1) * LANES], wide)
                scale = twice(scale_ref[top : top + edge, at * LANES : (at + 1) * LANES], wide)
                across = cum_t_ref[0, pl.ds(first + at, 1), :][:, top:]
                decays = jnp.exp(jnp.where(causal, across - down, -1e30))
                high, low = split(decays * score)
                part = matmul(high, dy_high, (1, 0)) + matmul(high, dy_low, (1, 0))
                part = part + matmul(low, dy_high, (1, 0))
                result = part if k == 0 else jnp.where(near < k * HEAD_DIM, result, part)
                mine = (lanes >= k * HEAD_DIM) & (lanes < (k + 1) * HEAD_DIM)
                pairs = matmul(x, jnp.where(mine, dy_high, zero), (1, 1))
                pairs = pairs + matmul(x, jnp.where(mine, dy_low, zero), (1, 1))
                term = pairs * decays * scale
                added = term if added is None else added + term
            bare_ref[0, top : top + edge, channels] = result
        total_ref[top : top + edge, top:] += added

    @pl.when(step == pl.num_programs(1) - 1)
    def _():
        high, low = split(total_ref[...])
        dw_ref[0] = matmul(high, r_ref[0], (1, 0)) + matmul(low, r_ref[0], (1, 0))
        dr_ref[0] = matmul(high, w_ref[0], (0, 0)) + matmul(low, w_ref[0], (0, 0))


def state_back_kernel(
    dy_ref, x_ref, plain_ref, bare_ref, w_ref, delta_ref, fading_ref, growth_ref, enter_ref,
    leave_ref, skip_ref, dw_in_ref, dr_in_ref, dx_ref, dw_ref, dr_ref, bare_dot_ref, fade_dot_ref,
    plain_dot_ref, skip_dot_ref,
):
    step = pl.program_id(1)
    width = x_ref.shape[2]
    first = step * (width // HEAD_DIM)
    heads = delta_ref.shape[2]

    @pl.when(step == 0)
    def _():
        dw_ref[...] = dw_in_ref[...]
        dr_ref[...] = dr_in_ref[...]
        bare_dot_ref[...] = jnp.zeros_like(bare_dot_ref)
        fade_dot_ref[...] = jnp.zeros_like(fade_dot_ref)
        plain_dot_ref[...] = jnp.zeros_like(plain_dot_ref)

    x = x_ref[0].astype(F32)
    dy = dy_ref[0]
    bare = bare_ref[0]
    fading = spread_exact(fading_ref[0], first, width, HEAD_DIM)
    reach = dot_exact_left(w_ref[0], leave_ref[0], (1, 1))
    dx_ref[0] = (
        spread_exact(delta_ref[0], first, width, HEAD_DIM) * bare
        + fading * reach
        + skip_ref[...] * dy
    )
    growth = spread_exact(growth_ref[0], first, width, HEAD_DIM)
    dr_ref[0] += dot_terms(dy * growth, enter_ref[0], (1, 0))
    dw_ref[0] += dot_terms(x * fading, leave_ref[0], (1, 0))
    bare_dot_ref[0] += place_heads(x * bare, first, heads)
    fade_dot_ref[0] += place_heads(x * reach, first, heads)
    plain_dot_ref[0] += place_heads(dy * plain_ref[0], first, heads)
    skip_dot_ref[0] = jnp.sum(dy * x, axis=0, keepdims=True)


def scan_specs(tokens, inner, heads):
    width = step_width(inner)
    tile = pl.BlockSpec((1, tokens, width), lambda s, j: (s, 0, j))
    state = pl.BlockSpec((1, tokens, STATE), lambda s, j: (s, 0, 0))
    per_head = pl.BlockSpec((1, tokens, heads), lambda s, j: (s, 0, 0))
    per_head_t = pl.BlockSpec((1, heads, tokens), lambda s, j: (s, 0, 0))
    carry = pl.BlockSpec((1, width, STATE), lambda s, j: (s, j, 0))
    lane = pl.BlockSpec((1, width), lambda s, j: (0, j))
    one = pl.BlockSpec((1, tokens, 1), lambda s, j: (s, 0, 0))
    lane_sum = pl.BlockSpec((1, 1, width), lambda s, j: (s, 0, j))
    return tile, state, per_head, per_head_t, carry, lane, one, lane_sum


def shaped(*shape):
    return jax.ShapeDtypeStruct(shape, F32)


def scan_call(kernel, grid, in_specs, out_specs, out_shape, scratch, flops, moved):
    return pl.pallas_call(
        kernel,
        grid=grid,
        in_specs=in_specs,
        out_specs=out_specs,
        out_shape=out_shape,
        scratch_shapes=scratch,
        cost_estimate=pl.CostEstimate(flops=flops, bytes_accessed=moved, transcendentals=0),
    )


def scan_state(v, u, scale, s):
    _, tokens, inner = v.shape
    heads = scale.shape[2]
    width = step_width(inner)
    return scan_call(
        state_kernel, (inner // width,),
        [
            pl.BlockSpec((1, tokens, width), lambda j: (s, 0, j)),
            pl.BlockSpec((1, tokens, STATE), lambda j: (s, 0, 0)),
            pl.BlockSpec((1, tokens, heads), lambda j: (s, 0, 0)),
        ],
        pl.BlockSpec((width, STATE), lambda j: (j, 0)), shaped(inner, STATE),
        [], 4 * tokens * inner * STATE, 8 * tokens * inner,
    )(v, u, scale)


def scan_within(x, w, r, cum, cum_t, delta_t):
    seqs, tokens, inner = x.shape
    width = step_width(inner)
    tile, state, per_head, per_head_t, _, _, _, _ = scan_specs(tokens, inner, cum.shape[2])
    size = seqs * tokens * inner
    return scan_call(
        within_kernel, (seqs, inner // width),
        [tile, state, state, per_head, per_head_t, per_head_t], tile, shaped(seqs, tokens, inner),
        [pltpu.VMEM((tokens, tokens), F32), pltpu.VMEM((tokens, PAIR * width), F32)],
        16 * size * tokens, 6 * size,
    )(x, w, r, cum, cum_t, delta_t)


def scan_gate(within, x, z, r, growth, enter, skip):
    seqs, tokens, inner = x.shape
    tile, state, per_head, _, carry, lane, one, _ = scan_specs(tokens, inner, growth.shape[2])
    size = seqs * tokens * inner
    return scan_call(
        gate_kernel, (seqs, inner // step_width(inner)),
        [tile, tile, tile, state, per_head, carry, lane], [tile, tile, one],
        [shaped(seqs, tokens, inner), shaped(seqs, tokens, inner), shaped(seqs, tokens, 1)],
        [], 8 * size * STATE, 16 * size,
    )(within, x, z, r, growth, enter, skip)


def scan_within_back(dy, x, w, r, cum, cum_t, delta):
    seqs, tokens, inner = x.shape
    width = step_width(inner)
    tile, state, per_head, per_head_t, _, _, _, _ = scan_specs(tokens, inner, cum.shape[2])
    size = seqs * tokens * inner
    square = pltpu.VMEM((tokens, tokens), F32)
    wide = pltpu.VMEM((tokens, PAIR * width), F32)
    return scan_call(
        within_back_kernel, (seqs, inner // width),
        [tile, tile, state, state, per_head, per_head_t, per_head], [tile, state, state],
        [shaped(seqs, tokens, inner), shaped(seqs, tokens, STATE), shaped(seqs, tokens, STATE)],
        [square, square, wide, wide], 32 * size * tokens, 10 * size,
    )(dy, x, w, r, cum, cum_t, delta)


def scan_state_back(dy, x, plain, bare, w, delta, fading, growth, enter, leave, skip, dw, dr):
    seqs, tokens, inner = x.shape
    heads = delta.shape[2]
    tile, state, per_head, _, carry, lane, _, lane_sum = scan_specs(tokens, inner, heads)
    size = seqs * tokens * inner
    sums = shaped(seqs, tokens, heads)
    return scan_call(
        state_back_kernel, (seqs, inner // step_width(inner)),
        [tile] * 4 + [state] + [per_head] * 3 + [carry, carry, lane, state, state],
        [tile, state, state, per_head, per_head, per_head, lane_sum],
        [shaped(seqs, tokens, inner), shaped(seqs, tokens, STATE), shaped(seqs, tokens, STATE)]
        + [sums] * 3 + [shaped(seqs, 1, inner)],
        [], 24 * size * STATE, 22 * size,
    )(dy, x, plain, bare, w, delta, fading, growth, enter, leave, skip, dw, dr)


def from_behind(value, axis, steps):
    count = lax.axis_size(axis)
    initial, last = (max(0, -steps), min(count, count - steps))
    return lax.ppermute(value, axis, [(source, source + steps) for source in range(initial, last)])


def swap(value):
    return lax.ppermute(value, "tensor", [(0, 1), (1, 0)])


def sum_tensor(value):
    if lax.axis_size("tensor") == 2:
        return value + swap(value)
    return lax.psum(value, "tensor")


def scatter_tensor(make, width, rank):
    if lax.axis_size("tensor") == 2:
        away = swap(make((1 - rank) * width))
        return make(rank * width), away
    whole = jnp.concatenate([make(k * width) for k in range(lax.axis_size("tensor"))], axis=-1)
    return lax.psum_scatter(whole, "tensor", scatter_dimension=whole.ndim - 1, tiled=True), 0.0


def over_dp(value, flip):
    return lax.ppermute(value, "dp", [(k, k ^ flip) for k in range(lax.axis_size("dp"))])


def row_blocks(width):
    d = lax.axis_index("dp")
    return lax.rem(d, 2), d // 2, width // lax.axis_size("dp")


def staged():
    return lax.axis_size("dp") == 4


def cut_dot(left, right):
    def part(start, rows):
        return dot(lax.dynamic_slice_in_dim(left, start, rows, 1), right, (0, 0))

    return part


def scatter_start(part, width):
    if not staged():
        return ()
    low, high, rows = row_blocks(width)
    first = part((2 * (1 - high) + 1 - low) * rows, rows)
    second = part((2 * high + 1 - low) * rows, rows)
    return over_dp(first, 1), over_dp(second, 1)


def scatter_high(part, width, near):
    if not staged():
        return ()
    low, high, rows = row_blocks(width)
    return over_dp(part((2 * (1 - high) + low) * rows, rows) + near[0], 2)


def scatter_end(part, width, near, far):
    if not staged():
        return lax.psum_scatter(
            part(0, width), ("dp", "ctx"), scatter_dimension=0, tiled=True
        )
    low, high, rows = row_blocks(width)
    n_ctx, c = lax.axis_size("ctx"), lax.axis_index("ctx")
    held = part((2 * high + low) * rows, rows) + near[1] + far
    block = rows // n_ctx
    total = lax.dynamic_slice_in_dim(held, c * block, block, 0)
    for k in range(1, n_ctx):
        give = lax.dynamic_slice_in_dim(held, lax.rem(c + k, n_ctx) * block, block, 0)
        total = total + lax.ppermute(give, "ctx", [(m, (m + k) % n_ctx) for m in range(n_ctx)])
    return total


def tie(first, second):
    return lax.optimization_barrier((first, second))


def chain(own, totals, backward):
    count = lax.axis_size("ctx")
    if count == 1:
        return [jnp.zeros_like(part) for part in own]
    received = entering = list(own)
    for hop in range(count - 1):
        pair = (count - 1 - hop, count - 2 - hop) if backward else (hop, hop + 1)
        leaving = own if hop == 0 else [t * r + o for t, r, o in zip(totals, received, own)]
        received = []
        for part in leaving:
            received.append(lax.ppermute(part, "ctx", [pair]))
        entering = received if hop == 0 else [e + r for e, r in zip(entering, received)]
    return entering


def segment_lengths():
    return [CONV * INNER, INNER, INNER, 2 * CONV * STATE, 2 * STATE, HEADS, HEADS, HEADS, D]


def unpack(flat):
    pieces = []
    offset = 0
    for length in segment_lengths():
        pieces.append(flat[offset : offset + length])
        offset += length
    return pieces


def silu_grad(value):
    sigma = jax.nn.sigmoid(value)
    return sigma * (1.0 + value * (1.0 - sigma))


def conv_forward(extended, kernel, offset_bias, length):
    total = jnp.zeros(extended[:, :length].shape, F32) + offset_bias
    for tap_index in range(CONV):
        total = total + kernel[tap_index] * extended[:, tap_index : tap_index + length]
    return total


def conv_backward(slope, follow, extended, kernel, length):
    padded = jnp.concatenate([slope, follow], axis=1)
    grad_input = jnp.zeros(slope.shape, F32)
    kernel_grads = []
    for tap_index in range(CONV):
        begin = CONV - 1 - tap_index
        grad_input = grad_input + kernel[tap_index] * padded[:, begin : begin + length]
        kernel_grads.append(
            jnp.sum(slope * extended[:, tap_index : tap_index + length], axis=(0, 1))
        )
    return (grad_input, jnp.stack(kernel_grads), jnp.sum(slope, axis=(0, 1)))


def dot(left, right, contract, exact=False):
    return lax.dot_general(
        left,
        right,
        ((contract[:1], contract[1:]), ((), ())),
        precision=HIGH if exact else None,
        preferred_element_type=F32,
    )


def adam_update(weight, moment, second, gradient, rate):
    moment = BETA_ONE * moment + (1.0 - BETA_ONE) * gradient
    second = BETA_TWO * second + (1.0 - BETA_TWO) * gradient * gradient
    moment_hat = moment / (1.0 - BETA_ONE**STEP)
    second_hat = second / (1.0 - BETA_TWO**STEP)
    weight = weight - rate * (moment_hat / (jnp.sqrt(second_hat) + ADAM_EPS) + DECAY_RATE * weight)
    return (weight, moment, second)


def einsum(spec, *parts):
    return jnp.einsum(spec, *parts, precision=HIGH, preferred_element_type=F32)


def on_device(
    layer_input,
    cotangent,
    in_proj,
    delta_proj,
    out_proj,
    state_proj,
    packed_params,
    moment_in,
    moment_delta,
    moment_out,
    moment_state,
    moment_packed,
    square_in,
    square_delta,
    square_out,
    square_state,
    square_packed,
):
    sizes = (lax.axis_size("dp"), lax.axis_size("ctx"), lax.axis_size("tensor"))
    n_dp, n_ctx, n_t = sizes
    groups = n_dp * n_ctx
    rank = lax.axis_index("tensor")
    seqs, tokens, width = layer_input.shape
    rows = seqs * tokens
    local_inner = in_proj.shape[2]
    local_heads = delta_proj.shape[1]
    own_width = width // n_t
    rim = CONV - 1

    state_rows_own = state_proj.shape[0]
    pack_own = packed_params.shape[0]
    state_piece = jnp.concatenate(
        [state_proj[:, 0].astype(BF), state_proj[:, 1].astype(BF)], axis=0
    )
    state_pad = cdiv(2 * state_rows_own, 16) * 16
    delta_pad = cdiv(local_heads, 16) * 16
    pack_rows = cdiv(pack_own, LANES)
    pack_pad = cdiv(pack_rows, 16) * 16
    proj_rows = delta_proj.shape[0]
    block = jnp.concatenate(
        [
            jnp.pad(state_piece, ((0, state_pad - 2 * state_rows_own), (0, 0))),
            jnp.pad(
                delta_proj.astype(BF).T, ((0, delta_pad - local_heads), (0, LANES - proj_rows))
            ),
            jnp.pad(
                jnp.pad(packed_params.astype(BF), (0, pack_rows * LANES - pack_own)).reshape(
                    pack_rows, LANES
                ),
                ((0, pack_pad - pack_rows), (0, 0)),
            ),
        ],
        axis=0,
    )
    small = gather_small(block, sizes)
    wx = lax.all_gather(in_proj[:, 1].astype(BF), ("dp", "ctx"), axis=0, tiled=True)
    wz = lax.all_gather(in_proj[:, 0].astype(BF), ("dp", "ctx"), axis=0, tiled=True)
    wo = lax.all_gather(out_proj.astype(BF), ("dp", "ctx"), axis=0, tiled=True)
    up_own = cotangent.astype(BF)
    if n_t == 2:
        up_away = swap(up_own)
        first = rank == 0
        up_full = jnp.concatenate(
            [jnp.where(first, up_own, up_away), jnp.where(first, up_away, up_own)], axis=2
        )
    else:
        up_full = lax.all_gather(up_own, "tensor", axis=2, tiled=True)
    up_rows = up_full.reshape(rows, width)

    state_slots = small[..., : 2 * state_rows_own, :].reshape(-1, 2, state_rows_own, STATE)
    ws = jnp.concatenate(
        [state_slots[:, 0].reshape(width, STATE), state_slots[:, 1].reshape(width, STATE)], axis=1
    )
    delta_slots = lax.dynamic_index_in_dim(small, rank, 2, False)
    delta_slots = delta_slots[..., state_pad : state_pad + local_heads, :proj_rows]
    wd = delta_slots.reshape(groups, local_heads, proj_rows).transpose(0, 2, 1)
    wd = wd.reshape(width, local_heads)
    pack_slots = small[..., state_pad + delta_pad : state_pad + delta_pad + pack_rows, :]
    packed = pack_slots.reshape(groups * n_t, pack_rows * LANES)[:, :pack_own].reshape(-1)
    pieces = unpack(packed.astype(F32))
    conv_kernel = lax.dynamic_slice_in_dim(
        pieces[0].reshape(CONV, INNER), rank * local_inner, local_inner, 1
    )
    conv_bias = lax.dynamic_slice_in_dim(pieces[1], rank * local_inner, local_inner, 0)
    gate_gain = lax.dynamic_slice_in_dim(pieces[2], rank * local_inner, local_inner, 0)
    state_kernel = pieces[3].reshape(CONV, 2 * STATE)
    state_bias = pieces[4]
    delta_bias = lax.dynamic_slice_in_dim(pieces[5], rank * local_heads, local_heads, 0)
    log_rates = lax.dynamic_slice_in_dim(pieces[6], rank * local_heads, local_heads, 0)
    skip_gain = lax.dynamic_slice_in_dim(pieces[7], rank * local_heads, local_heads, 0)
    norm_gain = pieces[8]
    rates = -jnp.exp(log_rates)

    input_float = layer_input.astype(F32)
    inverse = lax.rsqrt(jnp.mean(input_float * input_float, axis=-1, keepdims=True) + NORM_EPS)
    normed = (input_float * inverse * norm_gain).astype(BF).reshape(rows, width)
    sproj = dot(normed, ws, (1, 0)).astype(BF).reshape(seqs, tokens, 2 * STATE)
    raw = dot(normed, wd, (1, 0)).reshape(seqs, tokens, local_heads)
    xproj = dot(normed, wx, (1, 0)).astype(BF).reshape(seqs, tokens, local_inner)
    tails = from_behind(
        jnp.concatenate([xproj[:, tokens - rim :], sproj[:, tokens - rim :]], axis=2), "ctx", 1
    )
    ext_x = jnp.concatenate([tails[:, :, :local_inner], xproj], axis=1).astype(F32)
    ext_s = jnp.concatenate([tails[:, :, local_inner:], sproj], axis=1).astype(F32)
    conv_x = conv_forward(ext_x, conv_kernel, conv_bias, tokens)
    conv_s = conv_forward(ext_s, state_kernel, state_bias, tokens)
    act_x = jax.nn.silu(conv_x).astype(BF)
    act_s = jax.nn.silu(conv_s).astype(BF)
    delta = jax.nn.softplus(raw + delta_bias)
    wv = act_s[:, :, :STATE]
    rv = act_s[:, :, STATE:]
    past = (jnp.arange(tokens)[:, None] >= jnp.arange(tokens)[None, :]).astype(F32)
    cum = einsum("tm,smh->sth", past, delta * rates)
    totals = jnp.exp(cum[:, -1])
    fade_decay = jnp.exp(cum[:, -1:] - cum)
    fading = fade_decay * delta
    growth = jnp.exp(cum)
    spread = [
        jnp.broadcast_to(
            jnp.repeat(totals[k], HEAD_DIM)[:, None], (local_inner, STATE)
        )
        for k in range(seqs)
    ]
    cum_t = jnp.swapaxes(cum, 1, 2)
    skip_lanes = jnp.repeat(skip_gain, HEAD_DIM)[None, :]
    own_state = [scan_state(act_x, wv, fading, k) for k in range(seqs)]
    within = scan_within(act_x, wv, rv, cum, cum_t, jnp.swapaxes(delta, 1, 2))
    own_state, normed_late = tie(own_state, normed)
    zproj = dot(normed_late, wz, (1, 0)).astype(BF).reshape(seqs, tokens, local_inner)
    entering = chain(own_state, spread, False)
    entering = jnp.stack(entering, axis=0)

    plain, mixed, square_sums = scan_gate(within, act_x, zproj, rv, growth, entering, skip_lanes)
    gate_input = zproj.astype(F32)
    gate_act = jax.nn.silu(gate_input)
    mixer = plain + skip_lanes * act_x.astype(F32)
    square_sums = sum_tensor(square_sums[:, :, 0])
    gate_inverse = lax.rsqrt(square_sums / INNER + NORM_EPS)[:, :, None]
    gated = (mixed * gate_inverse * gate_gain).astype(BF).reshape(rows, local_inner)

    def out_columns(start):
        return dot(gated, lax.dynamic_slice_in_dim(wo, start, own_width, 0), (1, 1))

    branch, branch_away = scatter_tensor(out_columns, own_width, rank)
    own_input = lax.dynamic_slice_in_dim(layer_input, rank * own_width, own_width, 2).astype(F32)

    gated_grad = dot(up_rows, wo, (1, 0)).reshape(seqs, tokens, local_inner)
    part_out = cut_dot(up_rows, gated)
    near_out = scatter_start(part_out, width)
    scaled = gated_grad * gate_gain
    row_sums = sum_tensor(jnp.sum(scaled * mixed, axis=-1))
    mixed_grad = gate_inverse * scaled - mixed * gate_inverse**3 * (row_sums / INNER)[:, :, None]
    grad_gate_gain = jnp.sum(gated_grad * mixed * gate_inverse, axis=(0, 1))
    mixer_grad = mixed_grad * gate_act
    z_grad = (mixed_grad * mixer * silu_grad(gate_input)).astype(BF).reshape(rows, local_inner)
    part_z = cut_dot(normed, z_grad)

    pulled = [scan_state(mixer_grad, rv, growth, k) for k in range(seqs)]
    dy = mixer_grad
    dx_bare, dw, dr = scan_within_back(dy, act_x, wv, rv, cum, cum_t, delta)
    dx_bare, near_out = tie(dx_bare, near_out)
    far_out = scatter_high(part_out, width, near_out)
    near_z = scatter_start(part_z, width)
    leaving = jnp.stack(chain(pulled, spread, True), axis=0)
    leaving, (far_out, near_z) = tie(leaving, (far_out, near_z))
    far_z = scatter_high(part_z, width, near_z)
    grad_out = scatter_end(part_out, width, near_out, far_out)
    dx, dw, dr, bare_dot, fade_dot, plain_dot, skip_dot = scan_state_back(
        dy, act_x, plain, dx_bare, wv, delta, fading, growth, entering, leaving, skip_lanes, dw, dr
    )
    cum_grad = plain_dot - delta * bare_dot - fading * fade_dot
    end_grad = jnp.sum(fading * fade_dot, axis=1) + totals * jnp.sum(
        (leaving * entering).reshape(seqs, local_heads, HEAD_DIM, STATE), axis=(2, 3)
    )
    step_grad = (
        einsum("tm,sth->smh", past, cum_grad) + end_grad[:, None, :]
    )
    delta_grad = bare_dot + fade_decay * fade_dot + rates * step_grad
    grad_rates = jnp.sum(delta * step_grad, axis=(0, 1))
    grad_skip = jnp.sum(skip_dot.reshape(seqs, local_heads, HEAD_DIM), axis=(0, 2))
    grad_log_rates = grad_rates * rates
    raw_grad = delta_grad * jax.nn.sigmoid(raw + delta_bias)
    grad_delta_bias = jnp.sum(raw_grad, axis=(0, 1))

    slope_x = dx.reshape(seqs, tokens, local_inner) * silu_grad(conv_x)
    slope_s = jnp.concatenate([dw, dr], axis=-1) * silu_grad(conv_s)
    follow = from_behind(
        jnp.concatenate([slope_x[:, :rim], slope_s[:, :rim]], axis=2), "ctx", -1
    )
    back_x, grad_conv_kernel, grad_conv_bias = conv_backward(
        slope_x, follow[:, :, :local_inner], ext_x, conv_kernel, tokens
    )
    back_s, grad_state_kernel, grad_state_bias = conv_backward(
        slope_s, follow[:, :, local_inner:], ext_s, state_kernel, tokens
    )
    x_grad = back_x.astype(BF).reshape(rows, local_inner)
    state_rows = back_s.reshape(rows, 2 * STATE)
    raw_rows = raw_grad.reshape(rows, local_heads)

    def normed_columns(start):
        def cut(weight):
            return lax.dynamic_slice_in_dim(weight, start, own_width, 0)

        product = dot(x_grad, cut(wx), (1, 1))
        return (
            product
            + dot(z_grad, cut(wz), (1, 1))
            + dot(state_rows, cut(ws).astype(F32), (1, 1), True)
            + dot(raw_rows, cut(wd).astype(F32), (1, 1), True)
        )

    x_grad, (branch_away, far_z, grad_out) = tie(x_grad, (branch_away, far_z, grad_out))
    layer_output = own_input + (branch + branch_away).reshape(seqs, tokens, own_width)
    grad_z = scatter_end(part_z, width, near_z, far_z)
    pieces_x = 3 if local_inner % (3 * LANES) == 0 else 1
    piece = local_inner // pieces_x
    parts_x = [
        cut_dot(normed, x_grad[:, k * piece : (k + 1) * piece]) for k in range(pieces_x)
    ]
    near_x = []
    for part in parts_x:
        near_x.append(scatter_start(part, width))

    starts = [(1 - rank) * own_width, rank * own_width]
    if n_t != 2:
        starts = [k * own_width for k in range(n_t)]
    columns = [normed_columns(start) for start in starts]
    if n_t == 2:
        normed_grad = columns[1] + swap(columns[0])
    else:
        normed_grad = lax.psum_scatter(
            jnp.concatenate(columns, axis=1), "tensor", scatter_dimension=1, tiled=True
        )
    normed_grad = normed_grad.reshape(seqs, tokens, own_width)
    own_gain = lax.dynamic_slice_in_dim(norm_gain, rank * own_width, own_width, 0)
    grad_norm_gain = jnp.zeros((D,), F32)
    in_sums = 0.0
    for start, part in zip(starts, columns):
        inputs = lax.dynamic_slice_in_dim(layer_input, start, own_width, 2).astype(F32)
        gain = lax.dynamic_slice_in_dim(norm_gain, start, own_width, 0)
        product = part.reshape(seqs, tokens, own_width) * inputs
        in_sums = in_sums + jnp.sum(product * gain, axis=-1)
        grad_norm_gain = lax.dynamic_update_slice_in_dim(
            grad_norm_gain, jnp.sum(product * inverse, axis=(0, 1)), start, 0
        )
    in_mean = sum_tensor(in_sums)[:, :, None] / width
    scaled_in = normed_grad * own_gain
    input_grad = cotangent + inverse * scaled_in - own_input * inverse**3 * in_mean

    normed_float = normed.astype(F32)
    grad_state_part = dot(normed_float, state_rows, (0, 0), True)
    grad_delta_part = dot(normed_float, raw_rows, (0, 0), True)

    def widen(local_values, full_length):
        return lax.dynamic_update_slice_in_dim(
            jnp.zeros((full_length,), F32), local_values, rank * local_values.shape[0], 0
        )

    conv_wide = lax.dynamic_update_slice_in_dim(
        jnp.zeros((CONV, INNER), F32), grad_conv_kernel, rank * local_inner, 1
    ).reshape(-1)
    joined = jnp.concatenate(
        [
            conv_wide,
            widen(grad_conv_bias, INNER),
            widen(grad_gate_gain, INNER),
            grad_state_kernel.reshape(-1),
            grad_state_bias,
            widen(grad_delta_bias, HEADS),
            widen(grad_log_rates, HEADS),
            widen(grad_skip, HEADS),
            grad_norm_gain,
        ]
    )
    pack_group = n_t * pack_own
    packed_part = jnp.pad(joined, (0, groups * pack_group - joined.shape[0]))
    pack_cols = cdiv(pack_group, proj_rows)
    packed_part = jnp.pad(
        packed_part.reshape(groups, pack_group), ((0, 0), (0, pack_cols * proj_rows - pack_group))
    ).reshape(width, pack_cols)
    extra_pad = cdiv(local_heads + pack_cols, LANES) * LANES - local_heads - pack_cols
    tail_part = jnp.concatenate(
        [
            grad_state_part,
            grad_delta_part,
            packed_part,
            jnp.zeros((width, extra_pad), F32),
        ],
        axis=1,
    )
    far_x = [scatter_high(part, width, near) for part, near in zip(parts_x, near_x)]
    grad_x = jnp.concatenate(
        [
            scatter_end(part, width, near, far)
            for part, near, far in zip(parts_x, near_x, far_x)
        ],
        axis=1,
    )

    def part_tail(start, rows):
        return lax.dynamic_slice_in_dim(tail_part, start, rows, 0)

    near_tail = scatter_start(part_tail, width)
    far_tail = scatter_high(part_tail, width, near_tail)
    tail = scatter_end(part_tail, width, near_tail, far_tail)
    at = 2 * STATE
    grad_delta = tail[:, at : at + local_heads]
    state_group = tail[:, :at]
    packed_group = tail[:, at + local_heads : at + local_heads + pack_cols]
    packed_group = packed_group.reshape(-1)[:pack_group]
    if n_t == 2:
        away = swap(
            (
                lax.dynamic_slice_in_dim(
                    state_group, (1 - rank) * state_rows_own, state_rows_own, 0
                ),
                lax.dynamic_slice_in_dim(packed_group, (1 - rank) * pack_own, pack_own, 0),
            )
        )
        grad_state = (
            lax.dynamic_slice_in_dim(state_group, rank * state_rows_own, state_rows_own, 0)
            + away[0]
        )
        grad_packed = (
            lax.dynamic_slice_in_dim(packed_group, rank * pack_own, pack_own, 0) + away[1]
        )
    else:
        grad_state = lax.psum_scatter(state_group, "tensor", scatter_dimension=0, tiled=True)
        grad_packed = lax.psum_scatter(packed_group, "tensor", scatter_dimension=0, tiled=True)
    grad_state = grad_state.reshape(state_rows_own, 2, STATE)
    grad_in = jnp.stack([grad_z, grad_x], axis=1)

    new_in, next_moment_in, next_square_in = adam_update(
        in_proj, moment_in, square_in, grad_in, MATRIX_RATE
    )
    new_delta, next_moment_delta, next_square_delta = adam_update(
        delta_proj, moment_delta, square_delta, grad_delta, MATRIX_RATE
    )
    new_out, next_moment_out, next_square_out = adam_update(
        out_proj, moment_out, square_out, grad_out, MATRIX_RATE
    )
    new_state, next_moment_state, next_square_state = adam_update(
        state_proj, moment_state, square_state, grad_state, MATRIX_RATE
    )
    new_packed, next_moment_packed, next_square_packed = adam_update(
        packed_params, moment_packed, square_packed, grad_packed, PACKED_RATE
    )
    return (
        layer_output,
        input_grad,
        grad_in,
        grad_delta,
        grad_out,
        grad_state,
        grad_packed,
        new_in,
        new_delta,
        new_out,
        new_state,
        new_packed,
        next_moment_in,
        next_moment_delta,
        next_moment_out,
        next_moment_state,
        next_moment_packed,
        next_square_in,
        next_square_delta,
        next_square_out,
        next_square_state,
        next_square_packed,
    )


def solution(mesh):
    matrix = P(("dp", "ctx"), "tensor")
    projection = P(("dp", "ctx"), None, "tensor")
    state = P(("dp", "ctx", "tensor"), None, None)
    flat = P(("dp", "ctx", "tensor"))
    tokens = P("dp", "ctx", "tensor")
    weights = (projection, matrix, matrix, state, flat)

    return jax.shard_map(
        on_device,
        mesh=mesh,
        in_specs=(P("dp", "ctx", None), tokens) + weights * 3,
        out_specs=(tokens, tokens) + weights * 4,
        check_vma=False,
    )
```

```python
import functools

import jax
import jax.numpy as jnp
from jax import lax
from jax.experimental import pallas as pl
from jax.experimental.pallas import tpu as pltpu
from jax.sharding import PartitionSpec as P


D = 1536
HEADS = 48
HEAD_DIM = 64
STATE = 128
CONV = 4
STEP = 3
INNER = 3072
LANES = 128

NORM_EPS = 1e-05
BETA_ONE = 0.9
BETA_TWO = 0.999
ADAM_EPS = 1e-08
DECAY_RATE = 0.1
MATRIX_RATE = 0.01
PACKED_RATE = 0.1
HIGH = lax.Precision.HIGHEST
MESH = pl.DeviceIdType.MESH
BF = jnp.bfloat16
F32 = jnp.float32


def cdiv(a, b):
    return -(-a // b)


def gather_kernel(sizes, in_ref, out_ref, local_sem, send_sem, recv_sem):
    n_dp, n_ctx, n_t = sizes
    d, c, t = lax.axis_index("dp"), lax.axis_index("ctx"), lax.axis_index("tensor")
    peers = []
    for k in range(1, n_ctx):
        peers.append((d, lax.rem(c + k, n_ctx), t))
    for k in range(1, n_t):
        peers.append((d, c, lax.rem(t + k, n_t)))
    for k in range(1, n_dp):
        peers.append((lax.rem(d + k, n_dp), c, t))
    barrier = pltpu.get_barrier_semaphore()
    for peer in peers:
        pl.semaphore_signal(barrier, inc=1, device_id=peer, device_id_type=MESH)
    pl.semaphore_wait(barrier, len(peers))
    own = pltpu.make_async_copy(in_ref, out_ref.at[d, c, t], local_sem)
    own.start()
    own.wait()
    number = 0

    def stage(copies):
        for copy in copies:
            copy.start()
        for copy in copies:
            copy.wait()

    copies = []
    for k in range(1, n_ctx):
        view = out_ref.at[d, c, t]
        copies.append(
            pltpu.make_async_remote_copy(
                src_ref=view,
                dst_ref=view,
                send_sem=send_sem.at[number],
                recv_sem=recv_sem.at[number],
                device_id=(d, lax.rem(c + k, n_ctx), t),
                device_id_type=MESH,
            )
        )
        number += 1
    stage(copies)
    copies = []
    for k in range(1, n_t):
        view = out_ref.at[d, :, t]
        copies.append(
            pltpu.make_async_remote_copy(
                src_ref=view,
                dst_ref=view,
                send_sem=send_sem.at[number],
                recv_sem=recv_sem.at[number],
                device_id=(d, c, lax.rem(t + k, n_t)),
                device_id_type=MESH,
            )
        )
        number += 1
    stage(copies)
    copies = []
    for k in range(1, n_dp):
        view = out_ref.at[d]
        copies.append(
            pltpu.make_async_remote_copy(
                src_ref=view,
                dst_ref=view,
                send_sem=send_sem.at[number],
                recv_sem=recv_sem.at[number],
                device_id=(lax.rem(d + k, n_dp), c, t),
                device_id_type=MESH,
            )
        )
        number += 1
    stage(copies)


def gather_small(block, sizes):
    count = sum(sizes) - 3
    return pl.pallas_call(
        functools.partial(gather_kernel, sizes),
        out_shape=jax.ShapeDtypeStruct(sizes + block.shape, block.dtype),
        in_specs=[pl.BlockSpec(memory_space=pltpu.VMEM)],
        out_specs=pl.BlockSpec(memory_space=pltpu.VMEM),
        scratch_shapes=[
            pltpu.SemaphoreType.DMA(()),
            pltpu.SemaphoreType.DMA((count,)),
            pltpu.SemaphoreType.DMA((count,)),
        ],
        compiler_params=pltpu.CompilerParams(collective_id=0, has_side_effects=True),
        name="gather_small",
    )(block)


PAIR = LANES // HEAD_DIM


def step_width(inner):
    return 3 * LANES if inner % (3 * LANES) == 0 else LANES


def matmul(left, right, contract):
    return lax.dot_general(
        left, right, ((contract[:1], contract[1:]), ((), ())), preferred_element_type=F32
    )


def split(value):
    high = value.astype(BF)
    return high, (value - high.astype(F32)).astype(BF)


def dot_exact_right(left, right, contract):
    high, low = split(left)
    return matmul(high, right, contract) + matmul(low, right, contract)


def dot_exact_left(left, right, contract):
    high, low = split(right)
    return matmul(left, high, contract) + matmul(left, low, contract)


def dot_terms(left, right, contract):
    left_high, left_low = split(left)
    right_high, right_low = split(right)
    return (
        matmul(left_high, right_high, contract)
        + matmul(left_high, right_low, contract)
        + matmul(left_low, right_high, contract)
    )


def picker(heads, first, width, each):
    row = lax.broadcasted_iota(jnp.int32, (heads, width), 0)
    lane = lax.broadcasted_iota(jnp.int32, (heads, width), 1)
    return jnp.where(row == first + lane // each, 1.0, 0.0).astype(BF)


def spread_exact(values, first, width, each):
    pick = picker(values.shape[1], first, width, each)
    high = values.astype(BF)
    rest = values - high.astype(F32)
    middle = rest.astype(BF)
    low = (rest - middle.astype(F32)).astype(BF)
    return matmul(high, pick, (1, 0)) + (matmul(middle, pick, (1, 0)) + matmul(low, pick, (1, 0)))


def place_heads(values, first, heads):
    width = values.shape[1]
    lane = lax.broadcasted_iota(jnp.int32, (width, heads), 0)
    column = lax.broadcasted_iota(jnp.int32, (width, heads), 1)
    pick = jnp.where(column == first + lane // HEAD_DIM, 1.0, 0.0).astype(BF)
    return dot_exact_right(values, pick, (1, 0))


def twice(value, wide):
    count = wide // LANES
    return value if count <= 1 else jnp.concatenate([value] * count, axis=1)


def state_kernel(v_ref, u_ref, scale_ref, out_ref):
    width = v_ref.shape[2]
    first = pl.program_id(0) * (width // HEAD_DIM)
    scaled = v_ref[0].astype(F32) * spread_exact(scale_ref[0], first, width, HEAD_DIM)
    out_ref[...] = dot_exact_right(scaled, u_ref[0], (0, 0))


def within_kernel(x_ref, w_ref, r_ref, cum_ref, cum_t_ref, delta_t_ref, out_ref, score_ref, down_ref):
    step = pl.program_id(1)
    tokens, width = x_ref.shape[1:]
    edge = min(tokens, LANES)
    count = width // HEAD_DIM
    first = step * count

    @pl.when(step == 0)
    def _():
        score_ref[...] = matmul(r_ref[0], w_ref[0], (1, 1))

    down_ref[...] = spread_exact(cum_ref[0], first, count * LANES, LANES)
    lanes = lax.broadcasted_iota(jnp.int32, (edge, LANES), 1)
    for top in range(0, tokens, edge):
        wide = top + edge
        rows_at = top + lax.broadcasted_iota(jnp.int32, (edge, wide), 0)
        causal = rows_at >= lax.broadcasted_iota(jnp.int32, (edge, wide), 1)
        score = score_ref[top:wide, :wide]
        for tile in range(width // LANES):
            channels = slice(tile * LANES, (tile + 1) * LANES)
            x = x_ref[0, :wide, channels]
            result = None
            for k in range(PAIR):
                at = tile * PAIR + k
                down = twice(down_ref[top:wide, at * LANES : (at + 1) * LANES], wide)
                across = cum_t_ref[0, pl.ds(first + at, 1), :][:, :wide]
                scale = delta_t_ref[0, pl.ds(first + at, 1), :][:, :wide]
                decays = jnp.exp(jnp.where(causal, down - across, -1e30))
                part = dot_exact_right(decays * (score * scale), x, (1, 0))
                result = part if k == 0 else jnp.where(lanes < k * HEAD_DIM, result, part)
            out_ref[0, top:wide, channels] = result


def gate_kernel(
    within_ref, x_ref, z_ref, r_ref, growth_ref, enter_ref, skip_ref, plain_ref, mixed_ref, sum_ref
):
    step = pl.program_id(1)
    width = x_ref.shape[2]
    first = step * (width // HEAD_DIM)
    carried = dot_exact_left(r_ref[0], enter_ref[0], (1, 1))
    plain = within_ref[0] + carried * spread_exact(growth_ref[0], first, width, HEAD_DIM)
    plain_ref[0] = plain
    gate = z_ref[0].astype(F32)
    mixed = (plain + skip_ref[...] * x_ref[0].astype(F32)) * (gate * jax.nn.sigmoid(gate))
    mixed_ref[0] = mixed

    @pl.when(step == 0)
    def _():
        sum_ref[...] = jnp.zeros_like(sum_ref)

    sum_ref[0] += jnp.sum(mixed * mixed, axis=1, keepdims=True)


def within_back_kernel(
    dy_ref, x_ref, w_ref, r_ref, cum_ref, cum_t_ref, delta_ref, bare_ref, dw_ref, dr_ref,
    score_ref, total_ref, down_ref, scale_ref,
):
    step = pl.program_id(1)
    tokens, width = x_ref.shape[1:]
    edge = min(tokens, LANES)
    count = width // HEAD_DIM
    first = step * count

    @pl.when(step == 0)
    def _():
        score_ref[...] = matmul(w_ref[0], r_ref[0], (1, 1))
        total_ref[...] = jnp.zeros_like(total_ref)

    down_ref[...] = spread_exact(cum_ref[0], first, count * LANES, LANES)
    scale_ref[...] = spread_exact(delta_ref[0], first, count * LANES, LANES)
    for top in range(0, tokens, edge):
        wide = tokens - top
        rows_at = lax.broadcasted_iota(jnp.int32, (edge, wide), 0)
        causal = rows_at <= lax.broadcasted_iota(jnp.int32, (edge, wide), 1)
        lanes = lax.broadcasted_iota(jnp.int32, (wide, LANES), 1)
        near = lax.broadcasted_iota(jnp.int32, (edge, LANES), 1)
        score = score_ref[top : top + edge, top:]
        added = None
        for tile in range(width // LANES):
            channels = slice(tile * LANES, (tile + 1) * LANES)
            x = x_ref[0, top : top + edge, channels]
            dy_high, dy_low = split(dy_ref[0, top:, channels])
            zero = jnp.zeros_like(dy_high)
            result = None
            for k in range(PAIR):
                at = tile * PAIR + k
                down = twice(down_ref[top : top + edge, at * LANES : (at + 1) * LANES], wide)
                scale = twice(scale_ref[top : top + edge, at * LANES : (at + 1) * LANES], wide)
                across = cum_t_ref[0, pl.ds(first + at, 1), :][:, top:]
                decays = jnp.exp(jnp.where(causal, across - down, -1e30))
                high, low = split(decays * score)
                part = matmul(high, dy_high, (1, 0)) + matmul(high, dy_low, (1, 0))
                part = part + matmul(low, dy_high, (1, 0))
                result = part if k == 0 else jnp.where(near < k * HEAD_DIM, result, part)
                mine = (lanes >= k * HEAD_DIM) & (lanes < (k + 1) * HEAD_DIM)
                pairs = matmul(x, jnp.where(mine, dy_high, zero), (1, 1))
                pairs = pairs + matmul(x, jnp.where(mine, dy_low, zero), (1, 1))
                term = pairs * decays * scale
                added = term if added is None else added + term
            bare_ref[0, top : top + edge, channels] = result
        total_ref[top : top + edge, top:] += added

    @pl.when(step == pl.num_programs(1) - 1)
    def _():
        high, low = split(total_ref[...])
        dw_ref[0] = matmul(high, r_ref[0], (1, 0)) + matmul(low, r_ref[0], (1, 0))
        dr_ref[0] = matmul(high, w_ref[0], (0, 0)) + matmul(low, w_ref[0], (0, 0))


def state_back_kernel(
    dy_ref, x_ref, plain_ref, bare_ref, w_ref, delta_ref, fading_ref, growth_ref, enter_ref,
    leave_ref, skip_ref, dw_in_ref, dr_in_ref, dx_ref, dw_ref, dr_ref, bare_dot_ref, fade_dot_ref,
    plain_dot_ref, skip_dot_ref,
):
    step = pl.program_id(1)
    width = x_ref.shape[2]
    first = step * (width // HEAD_DIM)
    heads = delta_ref.shape[2]

    @pl.when(step == 0)
    def _():
        dw_ref[...] = dw_in_ref[...]
        dr_ref[...] = dr_in_ref[...]
        bare_dot_ref[...] = jnp.zeros_like(bare_dot_ref)
        fade_dot_ref[...] = jnp.zeros_like(fade_dot_ref)
        plain_dot_ref[...] = jnp.zeros_like(plain_dot_ref)

    x = x_ref[0].astype(F32)
    dy = dy_ref[0]
    bare = bare_ref[0]
    fading = spread_exact(fading_ref[0], first, width, HEAD_DIM)
    reach = dot_exact_left(w_ref[0], leave_ref[0], (1, 1))
    dx_ref[0] = (
        spread_exact(delta_ref[0], first, width, HEAD_DIM) * bare
        + fading * reach
        + skip_ref[...] * dy
    )
    growth = spread_exact(growth_ref[0], first, width, HEAD_DIM)
    dr_ref[0] += dot_terms(dy * growth, enter_ref[0], (1, 0))
    dw_ref[0] += dot_terms(x * fading, leave_ref[0], (1, 0))
    bare_dot_ref[0] += place_heads(x * bare, first, heads)
    fade_dot_ref[0] += place_heads(x * reach, first, heads)
    plain_dot_ref[0] += place_heads(dy * plain_ref[0], first, heads)
    skip_dot_ref[0] = jnp.sum(dy * x, axis=0, keepdims=True)


def scan_specs(tokens, inner, heads):
    width = step_width(inner)
    tile = pl.BlockSpec((1, tokens, width), lambda s, j: (s, 0, j))
    state = pl.BlockSpec((1, tokens, STATE), lambda s, j: (s, 0, 0))
    per_head = pl.BlockSpec((1, tokens, heads), lambda s, j: (s, 0, 0))
    per_head_t = pl.BlockSpec((1, heads, tokens), lambda s, j: (s, 0, 0))
    carry = pl.BlockSpec((1, width, STATE), lambda s, j: (s, j, 0))
    lane = pl.BlockSpec((1, width), lambda s, j: (0, j))
    one = pl.BlockSpec((1, tokens, 1), lambda s, j: (s, 0, 0))
    lane_sum = pl.BlockSpec((1, 1, width), lambda s, j: (s, 0, j))
    return tile, state, per_head, per_head_t, carry, lane, one, lane_sum


def shaped(*shape):
    return jax.ShapeDtypeStruct(shape, F32)


def scan_call(kernel, grid, in_specs, out_specs, out_shape, scratch, flops, moved):
    return pl.pallas_call(
        kernel,
        grid=grid,
        in_specs=in_specs,
        out_specs=out_specs,
        out_shape=out_shape,
        scratch_shapes=scratch,
        cost_estimate=pl.CostEstimate(flops=flops, bytes_accessed=moved, transcendentals=0),
    )


def scan_state(v, u, scale, s):
    _, tokens, inner = v.shape
    heads = scale.shape[2]
    width = step_width(inner)
    return scan_call(
        state_kernel, (inner // width,),
        [
            pl.BlockSpec((1, tokens, width), lambda j: (s, 0, j)),
            pl.BlockSpec((1, tokens, STATE), lambda j: (s, 0, 0)),
            pl.BlockSpec((1, tokens, heads), lambda j: (s, 0, 0)),
        ],
        pl.BlockSpec((width, STATE), lambda j: (j, 0)), shaped(inner, STATE),
        [], 4 * tokens * inner * STATE, 8 * tokens * inner,
    )(v, u, scale)


def scan_within(x, w, r, cum, cum_t, delta_t):
    seqs, tokens, inner = x.shape
    width = step_width(inner)
    tile, state, per_head, per_head_t, _, _, _, _ = scan_specs(tokens, inner, cum.shape[2])
    size = seqs * tokens * inner
    return scan_call(
        within_kernel, (seqs, inner // width),
        [tile, state, state, per_head, per_head_t, per_head_t], tile, shaped(seqs, tokens, inner),
        [pltpu.VMEM((tokens, tokens), F32), pltpu.VMEM((tokens, PAIR * width), F32)],
        16 * size * tokens, 6 * size,
    )(x, w, r, cum, cum_t, delta_t)


def scan_gate(within, x, z, r, growth, enter, skip):
    seqs, tokens, inner = x.shape
    tile, state, per_head, _, carry, lane, one, _ = scan_specs(tokens, inner, growth.shape[2])
    size = seqs * tokens * inner
    return scan_call(
        gate_kernel, (seqs, inner // step_width(inner)),
        [tile, tile, tile, state, per_head, carry, lane], [tile, tile, one],
        [shaped(seqs, tokens, inner), shaped(seqs, tokens, inner), shaped(seqs, tokens, 1)],
        [], 8 * size * STATE, 16 * size,
    )(within, x, z, r, growth, enter, skip)


def scan_within_back(dy, x, w, r, cum, cum_t, delta):
    seqs, tokens, inner = x.shape
    width = step_width(inner)
    tile, state, per_head, per_head_t, _, _, _, _ = scan_specs(tokens, inner, cum.shape[2])
    size = seqs * tokens * inner
    square = pltpu.VMEM((tokens, tokens), F32)
    wide = pltpu.VMEM((tokens, PAIR * width), F32)
    return scan_call(
        within_back_kernel, (seqs, inner // width),
        [tile, tile, state, state, per_head, per_head_t, per_head], [tile, state, state],
        [shaped(seqs, tokens, inner), shaped(seqs, tokens, STATE), shaped(seqs, tokens, STATE)],
        [square, square, wide, wide], 32 * size * tokens, 10 * size,
    )(dy, x, w, r, cum, cum_t, delta)


def scan_state_back(dy, x, plain, bare, w, delta, fading, growth, enter, leave, skip, dw, dr):
    seqs, tokens, inner = x.shape
    heads = delta.shape[2]
    tile, state, per_head, _, carry, lane, _, lane_sum = scan_specs(tokens, inner, heads)
    size = seqs * tokens * inner
    sums = shaped(seqs, tokens, heads)
    return scan_call(
        state_back_kernel, (seqs, inner // step_width(inner)),
        [tile] * 4 + [state] + [per_head] * 3 + [carry, carry, lane, state, state],
        [tile, state, state, per_head, per_head, per_head, lane_sum],
        [shaped(seqs, tokens, inner), shaped(seqs, tokens, STATE), shaped(seqs, tokens, STATE)]
        + [sums] * 3 + [shaped(seqs, 1, inner)],
        [], 24 * size * STATE, 22 * size,
    )(dy, x, plain, bare, w, delta, fading, growth, enter, leave, skip, dw, dr)


def from_behind(value, axis, steps):
    count = lax.axis_size(axis)
    initial, last = (max(0, -steps), min(count, count - steps))
    return lax.ppermute(value, axis, [(source, source + steps) for source in range(initial, last)])


def swap(value):
    return lax.ppermute(value, "tensor", [(0, 1), (1, 0)])


def sum_tensor(value):
    if lax.axis_size("tensor") == 2:
        return value + swap(value)
    return lax.psum(value, "tensor")


def scatter_tensor(make, width, rank):
    if lax.axis_size("tensor") == 2:
        away = swap(make((1 - rank) * width))
        return make(rank * width), away
    whole = jnp.concatenate([make(k * width) for k in range(lax.axis_size("tensor"))], axis=-1)
    return lax.psum_scatter(whole, "tensor", scatter_dimension=whole.ndim - 1, tiled=True), 0.0


def over_dp(value, flip):
    return lax.ppermute(value, "dp", [(k, k ^ flip) for k in range(lax.axis_size("dp"))])


def row_blocks(width):
    d = lax.axis_index("dp")
    return lax.rem(d, 2), d // 2, width // lax.axis_size("dp")


def staged():
    return lax.axis_size("dp") == 4


def cut_dot(left, right):
    def part(start, rows):
        return dot(lax.dynamic_slice_in_dim(left, start, rows, 1), right, (0, 0))

    return part


def scatter_start(part, width):
    if not staged():
        return ()
    low, high, rows = row_blocks(width)
    first = part((2 * (1 - high) + 1 - low) * rows, rows)
    second = part((2 * high + 1 - low) * rows, rows)
    return over_dp(first, 1), over_dp(second, 1)


def scatter_high(part, width, near):
    if not staged():
        return ()
    low, high, rows = row_blocks(width)
    return over_dp(part((2 * (1 - high) + low) * rows, rows) + near[0], 2)


def scatter_end(part, width, near, far):
    if not staged():
        return lax.psum_scatter(
            part(0, width), ("dp", "ctx"), scatter_dimension=0, tiled=True
        )
    low, high, rows = row_blocks(width)
    n_ctx, c = lax.axis_size("ctx"), lax.axis_index("ctx")
    held = part((2 * high + low) * rows, rows) + near[1] + far
    block = rows // n_ctx
    total = lax.dynamic_slice_in_dim(held, c * block, block, 0)
    for k in range(1, n_ctx):
        give = lax.dynamic_slice_in_dim(held, lax.rem(c + k, n_ctx) * block, block, 0)
        total = total + lax.ppermute(give, "ctx", [(m, (m + k) % n_ctx) for m in range(n_ctx)])
    return total


def tie(first, second):
    return lax.optimization_barrier((first, second))


def chain(own, totals, backward):
    count = lax.axis_size("ctx")
    if count == 1:
        return [jnp.zeros_like(part) for part in own]
    entering = [None] * len(own)
    leaving = list(own)
    for hop in range(count - 1):
        pair = (count - 1 - hop, count - 2 - hop) if backward else (hop, hop + 1)
        received = []
        for k, part in enumerate(leaving):
            if k:
                part, received[k - 1] = tie(part, received[k - 1])
            received.append(lax.ppermute(part, "ctx", [pair]))
        entering = received if hop == 0 else [e + r for e, r in zip(entering, received)]
        leaving = [t * r + o for t, r, o in zip(totals, received, own)]
    return entering


def segment_lengths():
    return [CONV * INNER, INNER, INNER, 2 * CONV * STATE, 2 * STATE, HEADS, HEADS, HEADS, D]


def unpack(flat):
    pieces = []
    offset = 0
    for length in segment_lengths():
        pieces.append(flat[offset : offset + length])
        offset += length
    return pieces


def silu_grad(value):
    sigma = jax.nn.sigmoid(value)
    return sigma * (1.0 + value * (1.0 - sigma))


def conv_forward(extended, kernel, offset_bias, length):
    total = jnp.zeros(extended[:, :length].shape, F32) + offset_bias
    for tap_index in range(CONV):
        total = total + kernel[tap_index] * extended[:, tap_index : tap_index + length]
    return total


def conv_backward(slope, follow, extended, kernel, length):
    padded = jnp.concatenate([slope, follow], axis=1)
    grad_input = jnp.zeros(slope.shape, F32)
    kernel_grads = []
    for tap_index in range(CONV):
        begin = CONV - 1 - tap_index
        grad_input = grad_input + kernel[tap_index] * padded[:, begin : begin + length]
        kernel_grads.append(
            jnp.sum(slope * extended[:, tap_index : tap_index + length], axis=(0, 1))
        )
    return (grad_input, jnp.stack(kernel_grads), jnp.sum(slope, axis=(0, 1)))


def dot(left, right, contract, exact=False):
    return lax.dot_general(
        left,
        right,
        ((contract[:1], contract[1:]), ((), ())),
        precision=HIGH if exact else None,
        preferred_element_type=F32,
    )


def adam_update(weight, moment, second, gradient, rate):
    moment = BETA_ONE * moment + (1.0 - BETA_ONE) * gradient
    second = BETA_TWO * second + (1.0 - BETA_TWO) * gradient * gradient
    moment_hat = moment / (1.0 - BETA_ONE**STEP)
    second_hat = second / (1.0 - BETA_TWO**STEP)
    weight = weight - rate * (moment_hat / (jnp.sqrt(second_hat) + ADAM_EPS) + DECAY_RATE * weight)
    return (weight, moment, second)


def einsum(spec, *parts):
    return jnp.einsum(spec, *parts, precision=HIGH, preferred_element_type=F32)


def on_device(
    layer_input,
    cotangent,
    in_proj,
    delta_proj,
    out_proj,
    state_proj,
    packed_params,
    moment_in,
    moment_delta,
    moment_out,
    moment_state,
    moment_packed,
    square_in,
    square_delta,
    square_out,
    square_state,
    square_packed,
):
    sizes = (lax.axis_size("dp"), lax.axis_size("ctx"), lax.axis_size("tensor"))
    n_dp, n_ctx, n_t = sizes
    groups = n_dp * n_ctx
    rank = lax.axis_index("tensor")
    seqs, tokens, width = layer_input.shape
    rows = seqs * tokens
    local_inner = in_proj.shape[2]
    local_heads = delta_proj.shape[1]
    own_width = width // n_t
    rim = CONV - 1

    state_rows_own = state_proj.shape[0]
    pack_own = packed_params.shape[0]
    state_piece = jnp.concatenate(
        [state_proj[:, 0].astype(BF), state_proj[:, 1].astype(BF)], axis=0
    )
    state_pad = cdiv(2 * state_rows_own, 16) * 16
    delta_pad = cdiv(local_heads, 16) * 16
    pack_rows = cdiv(pack_own, LANES)
    pack_pad = cdiv(pack_rows, 16) * 16
    proj_rows = delta_proj.shape[0]
    block = jnp.concatenate(
        [
            jnp.pad(state_piece, ((0, state_pad - 2 * state_rows_own), (0, 0))),
            jnp.pad(
                delta_proj.astype(BF).T, ((0, delta_pad - local_heads), (0, LANES - proj_rows))
            ),
            jnp.pad(
                jnp.pad(packed_params.astype(BF), (0, pack_rows * LANES - pack_own)).reshape(
                    pack_rows, LANES
                ),
                ((0, pack_pad - pack_rows), (0, 0)),
            ),
        ],
        axis=0,
    )
    small = gather_small(block, sizes)
    wx = lax.all_gather(in_proj[:, 1].astype(BF), ("dp", "ctx"), axis=0, tiled=True)
    wz = lax.all_gather(in_proj[:, 0].astype(BF), ("dp", "ctx"), axis=0, tiled=True)
    wo = lax.all_gather(out_proj.astype(BF), ("dp", "ctx"), axis=0, tiled=True)
    small, late_cotangent = tie(small, cotangent)
    up_own = late_cotangent.astype(BF)
    if n_t == 2:
        up_away = swap(up_own)
        first = rank == 0
        up_full = jnp.concatenate(
            [jnp.where(first, up_own, up_away), jnp.where(first, up_away, up_own)], axis=2
        )
    else:
        up_full = lax.all_gather(up_own, "tensor", axis=2, tiled=True)
    up_rows = up_full.reshape(rows, width)

    state_slots = small[..., : 2 * state_rows_own, :].reshape(-1, 2, state_rows_own, STATE)
    ws = jnp.concatenate(
        [state_slots[:, 0].reshape(width, STATE), state_slots[:, 1].reshape(width, STATE)], axis=1
    )
    delta_slots = lax.dynamic_index_in_dim(small, rank, 2, False)
    delta_slots = delta_slots[..., state_pad : state_pad + local_heads, :proj_rows]
    wd = delta_slots.reshape(groups, local_heads, proj_rows).transpose(0, 2, 1)
    wd = wd.reshape(width, local_heads)
    pack_slots = small[..., state_pad + delta_pad : state_pad + delta_pad + pack_rows, :]
    packed = pack_slots.reshape(groups * n_t, pack_rows * LANES)[:, :pack_own].reshape(-1)
    pieces = unpack(packed.astype(F32))
    conv_kernel = lax.dynamic_slice_in_dim(
        pieces[0].reshape(CONV, INNER), rank * local_inner, local_inner, 1
    )
    conv_bias = lax.dynamic_slice_in_dim(pieces[1], rank * local_inner, local_inner, 0)
    gate_gain = lax.dynamic_slice_in_dim(pieces[2], rank * local_inner, local_inner, 0)
    state_kernel = pieces[3].reshape(CONV, 2 * STATE)
    state_bias = pieces[4]
    delta_bias = lax.dynamic_slice_in_dim(pieces[5], rank * local_heads, local_heads, 0)
    log_rates = lax.dynamic_slice_in_dim(pieces[6], rank * local_heads, local_heads, 0)
    skip_gain = lax.dynamic_slice_in_dim(pieces[7], rank * local_heads, local_heads, 0)
    norm_gain = pieces[8]
    rates = -jnp.exp(log_rates)

    input_float = layer_input.astype(F32)
    inverse = lax.rsqrt(jnp.mean(input_float * input_float, axis=-1, keepdims=True) + NORM_EPS)
    normed = (input_float * inverse * norm_gain).astype(BF).reshape(rows, width)
    sproj = dot(normed, ws, (1, 0)).astype(BF).reshape(seqs, tokens, 2 * STATE)
    raw = dot(normed, wd, (1, 0)).reshape(seqs, tokens, local_heads)
    xproj = dot(normed, wx, (1, 0)).astype(BF).reshape(seqs, tokens, local_inner)
    tails = from_behind(
        jnp.concatenate([xproj[:, tokens - rim :], sproj[:, tokens - rim :]], axis=2), "ctx", 1
    )
    ext_x = jnp.concatenate([tails[:, :, :local_inner], xproj], axis=1).astype(F32)
    ext_s = jnp.concatenate([tails[:, :, local_inner:], sproj], axis=1).astype(F32)
    conv_x = conv_forward(ext_x, conv_kernel, conv_bias, tokens)
    conv_s = conv_forward(ext_s, state_kernel, state_bias, tokens)
    act_x = jax.nn.silu(conv_x).astype(BF)
    act_s = jax.nn.silu(conv_s).astype(BF)
    delta = jax.nn.softplus(raw + delta_bias)
    wv = act_s[:, :, :STATE]
    rv = act_s[:, :, STATE:]
    past = (jnp.arange(tokens)[:, None] >= jnp.arange(tokens)[None, :]).astype(F32)
    cum = einsum("tm,smh->sth", past, delta * rates)
    totals = jnp.exp(cum[:, -1])
    fade_decay = jnp.exp(cum[:, -1:] - cum)
    fading = fade_decay * delta
    growth = jnp.exp(cum)
    spread = [
        jnp.broadcast_to(
            jnp.repeat(totals[k], HEAD_DIM)[:, None], (local_inner, STATE)
        )
        for k in range(seqs)
    ]
    cum_t = jnp.swapaxes(cum, 1, 2)
    skip_lanes = jnp.repeat(skip_gain, HEAD_DIM)[None, :]
    own_state = [scan_state(act_x, wv, fading, k) for k in range(seqs)]
    within = scan_within(act_x, wv, rv, cum, cum_t, jnp.swapaxes(delta, 1, 2))
    own_state, normed_late = tie(own_state, normed)
    zproj = dot(normed_late, wz, (1, 0)).astype(BF).reshape(seqs, tokens, local_inner)
    entering = chain(own_state, spread, False)
    entering = jnp.stack(entering, axis=0)

    plain, mixed, square_sums = scan_gate(within, act_x, zproj, rv, growth, entering, skip_lanes)
    gate_input = zproj.astype(F32)
    gate_act = jax.nn.silu(gate_input)
    mixer = plain + skip_lanes * act_x.astype(F32)
    square_sums = sum_tensor(square_sums[:, :, 0])
    gate_inverse = lax.rsqrt(square_sums / INNER + NORM_EPS)[:, :, None]
    gated = (mixed * gate_inverse * gate_gain).astype(BF).reshape(rows, local_inner)

    def out_columns(start):
        return dot(gated, lax.dynamic_slice_in_dim(wo, start, own_width, 0), (1, 1))

    branch, branch_away = scatter_tensor(out_columns, own_width, rank)
    own_input = lax.dynamic_slice_in_dim(layer_input, rank * own_width, own_width, 2).astype(F32)

    gated_grad = dot(up_rows, wo, (1, 0)).reshape(seqs, tokens, local_inner)
    part_out = cut_dot(up_rows, gated)
    near_out = scatter_start(part_out, width)
    scaled = gated_grad * gate_gain
    row_sums = sum_tensor(jnp.sum(scaled * mixed, axis=-1))
    mixed_grad = gate_inverse * scaled - mixed * gate_inverse**3 * (row_sums / INNER)[:, :, None]
    grad_gate_gain = jnp.sum(gated_grad * mixed * gate_inverse, axis=(0, 1))
    mixer_grad = mixed_grad * gate_act
    z_grad = (mixed_grad * mixer * silu_grad(gate_input)).astype(BF).reshape(rows, local_inner)
    part_z = cut_dot(normed, z_grad)

    pulled = [scan_state(mixer_grad, rv, growth, k) for k in range(seqs)]
    dy = mixer_grad
    dx_bare, dw, dr = scan_within_back(dy, act_x, wv, rv, cum, cum_t, delta)
    dx_bare, near_out = tie(dx_bare, near_out)
    far_out = scatter_high(part_out, width, near_out)
    near_z = scatter_start(part_z, width)
    leaving = jnp.stack(chain(pulled, spread, True), axis=0)
    leaving, (far_out, near_z) = tie(leaving, (far_out, near_z))
    far_z = scatter_high(part_z, width, near_z)
    grad_out = scatter_end(part_out, width, near_out, far_out)
    dx, dw, dr, bare_dot, fade_dot, plain_dot, skip_dot = scan_state_back(
        dy, act_x, plain, dx_bare, wv, delta, fading, growth, entering, leaving, skip_lanes, dw, dr
    )
    cum_grad = plain_dot - delta * bare_dot - fading * fade_dot
    end_grad = jnp.sum(fading * fade_dot, axis=1) + totals * jnp.sum(
        (leaving * entering).reshape(seqs, local_heads, HEAD_DIM, STATE), axis=(2, 3)
    )
    step_grad = (
        einsum("tm,sth->smh", past, cum_grad) + end_grad[:, None, :]
    )
    delta_grad = bare_dot + fade_decay * fade_dot + rates * step_grad
    grad_rates = jnp.sum(delta * step_grad, axis=(0, 1))
    grad_skip = jnp.sum(skip_dot.reshape(seqs, local_heads, HEAD_DIM), axis=(0, 2))
    grad_log_rates = grad_rates * rates
    raw_grad = delta_grad * jax.nn.sigmoid(raw + delta_bias)
    grad_delta_bias = jnp.sum(raw_grad, axis=(0, 1))

    slope_x = dx.reshape(seqs, tokens, local_inner) * silu_grad(conv_x)
    slope_s = jnp.concatenate([dw, dr], axis=-1) * silu_grad(conv_s)
    follow = from_behind(
        jnp.concatenate([slope_x[:, :rim], slope_s[:, :rim]], axis=2), "ctx", -1
    )
    back_x, grad_conv_kernel, grad_conv_bias = conv_backward(
        slope_x, follow[:, :, :local_inner], ext_x, conv_kernel, tokens
    )
    back_s, grad_state_kernel, grad_state_bias = conv_backward(
        slope_s, follow[:, :, local_inner:], ext_s, state_kernel, tokens
    )
    x_grad = back_x.astype(BF).reshape(rows, local_inner)
    state_rows = back_s.reshape(rows, 2 * STATE)
    raw_rows = raw_grad.reshape(rows, local_heads)

    def normed_columns(start):
        def cut(weight):
            return lax.dynamic_slice_in_dim(weight, start, own_width, 0)

        product = dot(x_grad, cut(wx), (1, 1))
        return (
            product
            + dot(z_grad, cut(wz), (1, 1))
            + dot(state_rows, cut(ws).astype(F32), (1, 1), True)
            + dot(raw_rows, cut(wd).astype(F32), (1, 1), True)
        )

    x_grad, (branch_away, far_z, grad_out) = tie(x_grad, (branch_away, far_z, grad_out))
    layer_output = own_input + (branch + branch_away).reshape(seqs, tokens, own_width)
    grad_z = scatter_end(part_z, width, near_z, far_z)
    pieces_x = 3 if local_inner % (3 * LANES) == 0 else 1
    piece = local_inner // pieces_x
    parts_x = [
        cut_dot(normed, x_grad[:, k * piece : (k + 1) * piece]) for k in range(pieces_x)
    ]
    near_x = []
    for part in parts_x:
        near_x.append(scatter_start(part, width))

    starts = [(1 - rank) * own_width, rank * own_width]
    if n_t != 2:
        starts = [k * own_width for k in range(n_t)]
    columns = [normed_columns(start) for start in starts]
    if n_t == 2:
        normed_grad = columns[1] + swap(columns[0])
    else:
        normed_grad = lax.psum_scatter(
            jnp.concatenate(columns, axis=1), "tensor", scatter_dimension=1, tiled=True
        )
    normed_grad = normed_grad.reshape(seqs, tokens, own_width)
    own_gain = lax.dynamic_slice_in_dim(norm_gain, rank * own_width, own_width, 0)
    grad_norm_gain = jnp.zeros((D,), F32)
    in_sums = 0.0
    for start, part in zip(starts, columns):
        inputs = lax.dynamic_slice_in_dim(layer_input, start, own_width, 2).astype(F32)
        gain = lax.dynamic_slice_in_dim(norm_gain, start, own_width, 0)
        product = part.reshape(seqs, tokens, own_width) * inputs
        in_sums = in_sums + jnp.sum(product * gain, axis=-1)
        grad_norm_gain = lax.dynamic_update_slice_in_dim(
            grad_norm_gain, jnp.sum(product * inverse, axis=(0, 1)), start, 0
        )
    scaled_in = normed_grad * own_gain

    normed_float = normed.astype(F32)
    grad_state_part = dot(normed_float, state_rows, (0, 0), True)
    grad_delta_part = dot(normed_float, raw_rows, (0, 0), True)

    def widen(local_values, full_length):
        return lax.dynamic_update_slice_in_dim(
            jnp.zeros((full_length,), F32), local_values, rank * local_values.shape[0], 0
        )

    conv_wide = lax.dynamic_update_slice_in_dim(
        jnp.zeros((CONV, INNER), F32), grad_conv_kernel, rank * local_inner, 1
    ).reshape(-1)
    joined = jnp.concatenate(
        [
            conv_wide,
            widen(grad_conv_bias, INNER),
            widen(grad_gate_gain, INNER),
            grad_state_kernel.reshape(-1),
            grad_state_bias,
            widen(grad_delta_bias, HEADS),
            widen(grad_log_rates, HEADS),
            widen(grad_skip, HEADS),
            grad_norm_gain,
        ]
    )
    pack_group = n_t * pack_own
    packed_part = jnp.pad(joined, (0, groups * pack_group - joined.shape[0]))
    pack_cols = cdiv(pack_group, proj_rows)
    packed_part = jnp.pad(
        packed_part.reshape(groups, pack_group), ((0, 0), (0, pack_cols * proj_rows - pack_group))
    ).reshape(width, pack_cols)
    extra_pad = cdiv(local_heads + pack_cols, LANES) * LANES - local_heads - pack_cols
    tail_part = jnp.concatenate(
        [
            grad_state_part,
            grad_delta_part,
            packed_part,
            jnp.zeros((width, extra_pad), F32),
        ],
        axis=1,
    )
    far_x = []
    for k, part in enumerate(parts_x):
        if k:
            near_x[k], far_x[k - 1] = tie(near_x[k], far_x[k - 1])
        far_x.append(scatter_high(part, width, near_x[k]))
    grad_x = jnp.concatenate(
        [
            scatter_end(part, width, near, far)
            for part, near, far in zip(parts_x, near_x, far_x)
        ],
        axis=1,
    )

    grad_x, in_sums = tie(grad_x, in_sums)
    in_mean = sum_tensor(in_sums)[:, :, None] / width
    input_grad = cotangent + inverse * scaled_in - own_input * inverse**3 * in_mean

    def part_tail(start, rows):
        return lax.dynamic_slice_in_dim(tail_part, start, rows, 0)

    near_tail = scatter_start(part_tail, width)
    far_tail = scatter_high(part_tail, width, near_tail)
    tail = scatter_end(part_tail, width, near_tail, far_tail)
    at = 2 * STATE
    grad_delta = tail[:, at : at + local_heads]
    state_group = tail[:, :at]
    packed_group = tail[:, at + local_heads : at + local_heads + pack_cols]
    packed_group = packed_group.reshape(-1)[:pack_group]
    if n_t == 2:
        away = swap(
            (
                lax.dynamic_slice_in_dim(
                    state_group, (1 - rank) * state_rows_own, state_rows_own, 0
                ),
                lax.dynamic_slice_in_dim(packed_group, (1 - rank) * pack_own, pack_own, 0),
            )
        )
        grad_state = (
            lax.dynamic_slice_in_dim(state_group, rank * state_rows_own, state_rows_own, 0)
            + away[0]
        )
        grad_packed = (
            lax.dynamic_slice_in_dim(packed_group, rank * pack_own, pack_own, 0) + away[1]
        )
    else:
        grad_state = lax.psum_scatter(state_group, "tensor", scatter_dimension=0, tiled=True)
        grad_packed = lax.psum_scatter(packed_group, "tensor", scatter_dimension=0, tiled=True)
    grad_state = grad_state.reshape(state_rows_own, 2, STATE)
    grad_in = jnp.stack([grad_z, grad_x], axis=1)

    new_in, next_moment_in, next_square_in = adam_update(
        in_proj, moment_in, square_in, grad_in, MATRIX_RATE
    )
    new_delta, next_moment_delta, next_square_delta = adam_update(
        delta_proj, moment_delta, square_delta, grad_delta, MATRIX_RATE
    )
    new_out, next_moment_out, next_square_out = adam_update(
        out_proj, moment_out, square_out, grad_out, MATRIX_RATE
    )
    new_state, next_moment_state, next_square_state = adam_update(
        state_proj, moment_state, square_state, grad_state, MATRIX_RATE
    )
    new_packed, next_moment_packed, next_square_packed = adam_update(
        packed_params, moment_packed, square_packed, grad_packed, PACKED_RATE
    )
    return (
        layer_output,
        input_grad,
        grad_in,
        grad_delta,
        grad_out,
        grad_state,
        grad_packed,
        new_in,
        new_delta,
        new_out,
        new_state,
        new_packed,
        next_moment_in,
        next_moment_delta,
        next_moment_out,
        next_moment_state,
        next_moment_packed,
        next_square_in,
        next_square_delta,
        next_square_out,
        next_square_state,
        next_square_packed,
    )


def solution(mesh):
    matrix = P(("dp", "ctx"), "tensor")
    projection = P(("dp", "ctx"), None, "tensor")
    state = P(("dp", "ctx", "tensor"), None, None)
    flat = P(("dp", "ctx", "tensor"))
    tokens = P("dp", "ctx", "tensor")
    weights = (projection, matrix, matrix, state, flat)

    return jax.shard_map(
        on_device,
        mesh=mesh,
        in_specs=(P("dp", "ctx", None), tokens) + weights * 3,
        out_specs=(tokens, tokens) + weights * 4,
        check_vma=False,
    )
```

```python
import functools

import jax
import jax.numpy as jnp
from jax import lax
from jax.experimental import pallas as pl
from jax.experimental.pallas import tpu as pltpu
from jax.sharding import PartitionSpec as P


D = 1536
HEADS = 48
HEAD_DIM = 64
STATE = 128
CONV = 4
STEP = 3
INNER = 3072
LANES = 128

NORM_EPS = 1e-05
BETA_ONE = 0.9
BETA_TWO = 0.999
ADAM_EPS = 1e-08
DECAY_RATE = 0.1
MATRIX_RATE = 0.01
PACKED_RATE = 0.1
HIGH = lax.Precision.HIGHEST
MESH = pl.DeviceIdType.MESH
BF = jnp.bfloat16
F32 = jnp.float32


def cdiv(a, b):
    return -(-a // b)


def gather_kernel(sizes, in_ref, out_ref, local_sem, send_sem, recv_sem):
    n_dp, n_ctx, n_t = sizes
    d, c, t = lax.axis_index("dp"), lax.axis_index("ctx"), lax.axis_index("tensor")
    peers = []
    for k in range(1, n_ctx):
        peers.append((d, lax.rem(c + k, n_ctx), t))
    for k in range(1, n_t):
        peers.append((d, c, lax.rem(t + k, n_t)))
    for k in range(1, n_dp):
        peers.append((lax.rem(d + k, n_dp), c, t))
    barrier = pltpu.get_barrier_semaphore()
    for peer in peers:
        pl.semaphore_signal(barrier, inc=1, device_id=peer, device_id_type=MESH)
    pl.semaphore_wait(barrier, len(peers))
    own = pltpu.make_async_copy(in_ref, out_ref.at[d, c, t], local_sem)
    own.start()
    own.wait()
    number = 0

    def stage(copies):
        for copy in copies:
            copy.start()
        for copy in copies:
            copy.wait()

    copies = []
    for k in range(1, n_ctx):
        view = out_ref.at[d, c, t]
        copies.append(
            pltpu.make_async_remote_copy(
                src_ref=view,
                dst_ref=view,
                send_sem=send_sem.at[number],
                recv_sem=recv_sem.at[number],
                device_id=(d, lax.rem(c + k, n_ctx), t),
                device_id_type=MESH,
            )
        )
        number += 1
    stage(copies)
    copies = []
    for k in range(1, n_t):
        view = out_ref.at[d, :, t]
        copies.append(
            pltpu.make_async_remote_copy(
                src_ref=view,
                dst_ref=view,
                send_sem=send_sem.at[number],
                recv_sem=recv_sem.at[number],
                device_id=(d, c, lax.rem(t + k, n_t)),
                device_id_type=MESH,
            )
        )
        number += 1
    stage(copies)
    copies = []
    for k in range(1, n_dp):
        view = out_ref.at[d]
        copies.append(
            pltpu.make_async_remote_copy(
                src_ref=view,
                dst_ref=view,
                send_sem=send_sem.at[number],
                recv_sem=recv_sem.at[number],
                device_id=(lax.rem(d + k, n_dp), c, t),
                device_id_type=MESH,
            )
        )
        number += 1
    stage(copies)


def gather_small(block, sizes):
    count = sum(sizes) - 3
    return pl.pallas_call(
        functools.partial(gather_kernel, sizes),
        out_shape=jax.ShapeDtypeStruct(sizes + block.shape, block.dtype),
        in_specs=[pl.BlockSpec(memory_space=pltpu.VMEM)],
        out_specs=pl.BlockSpec(memory_space=pltpu.VMEM),
        scratch_shapes=[
            pltpu.SemaphoreType.DMA(()),
            pltpu.SemaphoreType.DMA((count,)),
            pltpu.SemaphoreType.DMA((count,)),
        ],
        compiler_params=pltpu.CompilerParams(collective_id=0, has_side_effects=True),
        name="gather_small",
    )(block)


PAIR = LANES // HEAD_DIM


def step_width(inner):
    return 3 * LANES if inner % (3 * LANES) == 0 else LANES


def matmul(left, right, contract):
    return lax.dot_general(
        left, right, ((contract[:1], contract[1:]), ((), ())), preferred_element_type=F32
    )


def split(value):
    high = value.astype(BF)
    return high, (value - high.astype(F32)).astype(BF)


def dot_exact_right(left, right, contract):
    high, low = split(left)
    return matmul(high, right, contract) + matmul(low, right, contract)


def dot_exact_left(left, right, contract):
    high, low = split(right)
    return matmul(left, high, contract) + matmul(left, low, contract)


def dot_terms(left, right, contract):
    left_high, left_low = split(left)
    right_high, right_low = split(right)
    return (
        matmul(left_high, right_high, contract)
        + matmul(left_high, right_low, contract)
        + matmul(left_low, right_high, contract)
    )


def picker(heads, first, width, each):
    row = lax.broadcasted_iota(jnp.int32, (heads, width), 0)
    lane = lax.broadcasted_iota(jnp.int32, (heads, width), 1)
    return jnp.where(row == first + lane // each, 1.0, 0.0).astype(BF)


def spread_exact(values, first, width, each):
    pick = picker(values.shape[1], first, width, each)
    high = values.astype(BF)
    rest = values - high.astype(F32)
    middle = rest.astype(BF)
    low = (rest - middle.astype(F32)).astype(BF)
    return matmul(high, pick, (1, 0)) + (matmul(middle, pick, (1, 0)) + matmul(low, pick, (1, 0)))


def place_heads(values, first, heads):
    width = values.shape[1]
    lane = lax.broadcasted_iota(jnp.int32, (width, heads), 0)
    column = lax.broadcasted_iota(jnp.int32, (width, heads), 1)
    pick = jnp.where(column == first + lane // HEAD_DIM, 1.0, 0.0).astype(BF)
    return dot_exact_right(values, pick, (1, 0))


def twice(value, wide):
    count = wide // LANES
    return value if count <= 1 else jnp.concatenate([value] * count, axis=1)


def state_kernel(v_ref, u_ref, scale_ref, out_ref):
    width = v_ref.shape[2]
    first = pl.program_id(0) * (width // HEAD_DIM)
    scaled = v_ref[0].astype(F32) * spread_exact(scale_ref[0], first, width, HEAD_DIM)
    out_ref[...] = dot_exact_right(scaled, u_ref[0], (0, 0))


def within_kernel(x_ref, w_ref, r_ref, cum_ref, cum_t_ref, delta_t_ref, out_ref, score_ref, down_ref):
    step = pl.program_id(1)
    tokens, width = x_ref.shape[1:]
    edge = min(tokens, LANES)
    count = width // HEAD_DIM
    first = step * count

    @pl.when(step == 0)
    def _():
        score_ref[...] = matmul(r_ref[0], w_ref[0], (1, 1))

    down_ref[...] = spread_exact(cum_ref[0], first, count * LANES, LANES)
    lanes = lax.broadcasted_iota(jnp.int32, (edge, LANES), 1)
    for top in range(0, tokens, edge):
        wide = top + edge
        rows_at = top + lax.broadcasted_iota(jnp.int32, (edge, wide), 0)
        causal = rows_at >= lax.broadcasted_iota(jnp.int32, (edge, wide), 1)
        score = score_ref[top:wide, :wide]
        for tile in range(width // LANES):
            channels = slice(tile * LANES, (tile + 1) * LANES)
            x = x_ref[0, :wide, channels]
            result = None
            for k in range(PAIR):
                at = tile * PAIR + k
                down = twice(down_ref[top:wide, at * LANES : (at + 1) * LANES], wide)
                across = cum_t_ref[0, pl.ds(first + at, 1), :][:, :wide]
                scale = delta_t_ref[0, pl.ds(first + at, 1), :][:, :wide]
                decays = jnp.exp(jnp.where(causal, down - across, -1e30))
                part = dot_exact_right(decays * (score * scale), x, (1, 0))
                result = part if k == 0 else jnp.where(lanes < k * HEAD_DIM, result, part)
            out_ref[0, top:wide, channels] = result


def gate_kernel(
    within_ref, x_ref, z_ref, r_ref, growth_ref, enter_ref, skip_ref, plain_ref, mixed_ref, sum_ref
):
    step = pl.program_id(1)
    width = x_ref.shape[2]
    first = step * (width // HEAD_DIM)
    carried = dot_exact_left(r_ref[0], enter_ref[0], (1, 1))
    plain = within_ref[0] + carried * spread_exact(growth_ref[0], first, width, HEAD_DIM)
    plain_ref[0] = plain
    gate = z_ref[0].astype(F32)
    mixed = (plain + skip_ref[...] * x_ref[0].astype(F32)) * (gate * jax.nn.sigmoid(gate))
    mixed_ref[0] = mixed

    @pl.when(step == 0)
    def _():
        sum_ref[...] = jnp.zeros_like(sum_ref)

    sum_ref[0] += jnp.sum(mixed * mixed, axis=1, keepdims=True)


def within_back_kernel(
    dy_ref, x_ref, w_ref, r_ref, cum_ref, cum_t_ref, delta_ref, bare_ref, dw_ref, dr_ref,
    score_ref, total_ref, down_ref, scale_ref,
):
    step = pl.program_id(1)
    tokens, width = x_ref.shape[1:]
    edge = min(tokens, LANES)
    count = width // HEAD_DIM
    first = step * count

    @pl.when(step == 0)
    def _():
        score_ref[...] = matmul(w_ref[0], r_ref[0], (1, 1))
        total_ref[...] = jnp.zeros_like(total_ref)

    down_ref[...] = spread_exact(cum_ref[0], first, count * LANES, LANES)
    scale_ref[...] = spread_exact(delta_ref[0], first, count * LANES, LANES)
    for top in range(0, tokens, edge):
        wide = tokens - top
        rows_at = lax.broadcasted_iota(jnp.int32, (edge, wide), 0)
        causal = rows_at <= lax.broadcasted_iota(jnp.int32, (edge, wide), 1)
        lanes = lax.broadcasted_iota(jnp.int32, (wide, LANES), 1)
        near = lax.broadcasted_iota(jnp.int32, (edge, LANES), 1)
        score = score_ref[top : top + edge, top:]
        added = None
        for tile in range(width // LANES):
            channels = slice(tile * LANES, (tile + 1) * LANES)
            x = x_ref[0, top : top + edge, channels]
            dy_high, dy_low = split(dy_ref[0, top:, channels])
            zero = jnp.zeros_like(dy_high)
            result = None
            for k in range(PAIR):
                at = tile * PAIR + k
                down = twice(down_ref[top : top + edge, at * LANES : (at + 1) * LANES], wide)
                scale = twice(scale_ref[top : top + edge, at * LANES : (at + 1) * LANES], wide)
                across = cum_t_ref[0, pl.ds(first + at, 1), :][:, top:]
                decays = jnp.exp(jnp.where(causal, across - down, -1e30))
                high, low = split(decays * score)
                part = matmul(high, dy_high, (1, 0)) + matmul(high, dy_low, (1, 0))
                part = part + matmul(low, dy_high, (1, 0))
                result = part if k == 0 else jnp.where(near < k * HEAD_DIM, result, part)
                mine = (lanes >= k * HEAD_DIM) & (lanes < (k + 1) * HEAD_DIM)
                pairs = matmul(x, jnp.where(mine, dy_high, zero), (1, 1))
                pairs = pairs + matmul(x, jnp.where(mine, dy_low, zero), (1, 1))
                term = pairs * decays * scale
                added = term if added is None else added + term
            bare_ref[0, top : top + edge, channels] = result
        total_ref[top : top + edge, top:] += added

    @pl.when(step == pl.num_programs(1) - 1)
    def _():
        high, low = split(total_ref[...])
        dw_ref[0] = matmul(high, r_ref[0], (1, 0)) + matmul(low, r_ref[0], (1, 0))
        dr_ref[0] = matmul(high, w_ref[0], (0, 0)) + matmul(low, w_ref[0], (0, 0))


def state_back_kernel(
    dy_ref, x_ref, plain_ref, bare_ref, w_ref, delta_ref, fading_ref, growth_ref, enter_ref,
    leave_ref, skip_ref, dw_in_ref, dr_in_ref, dx_ref, dw_ref, dr_ref, bare_dot_ref, fade_dot_ref,
    plain_dot_ref, skip_dot_ref,
):
    step = pl.program_id(1)
    width = x_ref.shape[2]
    first = step * (width // HEAD_DIM)
    heads = delta_ref.shape[2]

    @pl.when(step == 0)
    def _():
        dw_ref[...] = dw_in_ref[...]
        dr_ref[...] = dr_in_ref[...]
        bare_dot_ref[...] = jnp.zeros_like(bare_dot_ref)
        fade_dot_ref[...] = jnp.zeros_like(fade_dot_ref)
        plain_dot_ref[...] = jnp.zeros_like(plain_dot_ref)

    x = x_ref[0].astype(F32)
    dy = dy_ref[0]
    bare = bare_ref[0]
    fading = spread_exact(fading_ref[0], first, width, HEAD_DIM)
    reach = dot_exact_left(w_ref[0], leave_ref[0], (1, 1))
    dx_ref[0] = (
        spread_exact(delta_ref[0], first, width, HEAD_DIM) * bare
        + fading * reach
        + skip_ref[...] * dy
    )
    growth = spread_exact(growth_ref[0], first, width, HEAD_DIM)
    dr_ref[0] += dot_terms(dy * growth, enter_ref[0], (1, 0))
    dw_ref[0] += dot_terms(x * fading, leave_ref[0], (1, 0))
    bare_dot_ref[0] += place_heads(x * bare, first, heads)
    fade_dot_ref[0] += place_heads(x * reach, first, heads)
    plain_dot_ref[0] += place_heads(dy * plain_ref[0], first, heads)
    skip_dot_ref[0] = jnp.sum(dy * x, axis=0, keepdims=True)


def scan_specs(tokens, inner, heads):
    width = step_width(inner)
    tile = pl.BlockSpec((1, tokens, width), lambda s, j: (s, 0, j))
    state = pl.BlockSpec((1, tokens, STATE), lambda s, j: (s, 0, 0))
    per_head = pl.BlockSpec((1, tokens, heads), lambda s, j: (s, 0, 0))
    per_head_t = pl.BlockSpec((1, heads, tokens), lambda s, j: (s, 0, 0))
    carry = pl.BlockSpec((1, width, STATE), lambda s, j: (s, j, 0))
    lane = pl.BlockSpec((1, width), lambda s, j: (0, j))
    one = pl.BlockSpec((1, tokens, 1), lambda s, j: (s, 0, 0))
    lane_sum = pl.BlockSpec((1, 1, width), lambda s, j: (s, 0, j))
    return tile, state, per_head, per_head_t, carry, lane, one, lane_sum


def shaped(*shape):
    return jax.ShapeDtypeStruct(shape, F32)


def scan_call(kernel, grid, in_specs, out_specs, out_shape, scratch, flops, moved):
    return pl.pallas_call(
        kernel,
        grid=grid,
        in_specs=in_specs,
        out_specs=out_specs,
        out_shape=out_shape,
        scratch_shapes=scratch,
        cost_estimate=pl.CostEstimate(flops=flops, bytes_accessed=moved, transcendentals=0),
    )


def scan_state(v, u, scale, s):
    _, tokens, inner = v.shape
    heads = scale.shape[2]
    width = step_width(inner)
    return scan_call(
        state_kernel, (inner // width,),
        [
            pl.BlockSpec((1, tokens, width), lambda j: (s, 0, j)),
            pl.BlockSpec((1, tokens, STATE), lambda j: (s, 0, 0)),
            pl.BlockSpec((1, tokens, heads), lambda j: (s, 0, 0)),
        ],
        pl.BlockSpec((width, STATE), lambda j: (j, 0)), shaped(inner, STATE),
        [], 4 * tokens * inner * STATE, 8 * tokens * inner,
    )(v, u, scale)


def scan_within(x, w, r, cum, cum_t, delta_t):
    seqs, tokens, inner = x.shape
    width = step_width(inner)
    tile, state, per_head, per_head_t, _, _, _, _ = scan_specs(tokens, inner, cum.shape[2])
    size = seqs * tokens * inner
    return scan_call(
        within_kernel, (seqs, inner // width),
        [tile, state, state, per_head, per_head_t, per_head_t], tile, shaped(seqs, tokens, inner),
        [pltpu.VMEM((tokens, tokens), F32), pltpu.VMEM((tokens, PAIR * width), F32)],
        16 * size * tokens, 6 * size,
    )(x, w, r, cum, cum_t, delta_t)


def scan_gate(within, x, z, r, growth, enter, skip):
    seqs, tokens, inner = x.shape
    tile, state, per_head, _, carry, lane, one, _ = scan_specs(tokens, inner, growth.shape[2])
    size = seqs * tokens * inner
    return scan_call(
        gate_kernel, (seqs, inner // step_width(inner)),
        [tile, tile, tile, state, per_head, carry, lane], [tile, tile, one],
        [shaped(seqs, tokens, inner), shaped(seqs, tokens, inner), shaped(seqs, tokens, 1)],
        [], 8 * size * STATE, 16 * size,
    )(within, x, z, r, growth, enter, skip)


def scan_within_back(dy, x, w, r, cum, cum_t, delta):
    seqs, tokens, inner = x.shape
    width = step_width(inner)
    tile, state, per_head, per_head_t, _, _, _, _ = scan_specs(tokens, inner, cum.shape[2])
    size = seqs * tokens * inner
    square = pltpu.VMEM((tokens, tokens), F32)
    wide = pltpu.VMEM((tokens, PAIR * width), F32)
    return scan_call(
        within_back_kernel, (seqs, inner // width),
        [tile, tile, state, state, per_head, per_head_t, per_head], [tile, state, state],
        [shaped(seqs, tokens, inner), shaped(seqs, tokens, STATE), shaped(seqs, tokens, STATE)],
        [square, square, wide, wide], 32 * size * tokens, 10 * size,
    )(dy, x, w, r, cum, cum_t, delta)


def scan_state_back(dy, x, plain, bare, w, delta, fading, growth, enter, leave, skip, dw, dr):
    seqs, tokens, inner = x.shape
    heads = delta.shape[2]
    tile, state, per_head, _, carry, lane, _, lane_sum = scan_specs(tokens, inner, heads)
    size = seqs * tokens * inner
    sums = shaped(seqs, tokens, heads)
    return scan_call(
        state_back_kernel, (seqs, inner // step_width(inner)),
        [tile] * 4 + [state] + [per_head] * 3 + [carry, carry, lane, state, state],
        [tile, state, state, per_head, per_head, per_head, lane_sum],
        [shaped(seqs, tokens, inner), shaped(seqs, tokens, STATE), shaped(seqs, tokens, STATE)]
        + [sums] * 3 + [shaped(seqs, 1, inner)],
        [], 24 * size * STATE, 22 * size,
    )(dy, x, plain, bare, w, delta, fading, growth, enter, leave, skip, dw, dr)


def from_behind(value, axis, steps):
    count = lax.axis_size(axis)
    initial, last = (max(0, -steps), min(count, count - steps))
    return lax.ppermute(value, axis, [(source, source + steps) for source in range(initial, last)])


def swap(value):
    return lax.ppermute(value, "tensor", [(0, 1), (1, 0)])


def sum_tensor(value):
    if lax.axis_size("tensor") == 2:
        return value + swap(value)
    return lax.psum(value, "tensor")


def scatter_tensor(make, width, rank):
    if lax.axis_size("tensor") == 2:
        away = swap(make((1 - rank) * width))
        return make(rank * width), away
    whole = jnp.concatenate([make(k * width) for k in range(lax.axis_size("tensor"))], axis=-1)
    return lax.psum_scatter(whole, "tensor", scatter_dimension=whole.ndim - 1, tiled=True), 0.0


def over_dp(value, flip):
    return lax.ppermute(value, "dp", [(k, k ^ flip) for k in range(lax.axis_size("dp"))])


def row_blocks(width):
    d = lax.axis_index("dp")
    return lax.rem(d, 2), d // 2, width // lax.axis_size("dp")


def staged():
    return lax.axis_size("dp") == 4


def cut_dot(left, right):
    def part(start, rows):
        return dot(lax.dynamic_slice_in_dim(left, start, rows, 1), right, (0, 0))

    return part


def scatter_start(part, width):
    if not staged():
        return ()
    low, high, rows = row_blocks(width)
    first = part((2 * (1 - high) + 1 - low) * rows, rows)
    second = part((2 * high + 1 - low) * rows, rows)
    return over_dp(first, 1), over_dp(second, 1)


def scale_of(value):
    top = jnp.maximum(jnp.max(jnp.abs(value), axis=0, keepdims=True), 1e-37)
    return jnp.clip(jnp.floor(14.0 - jnp.log2(top)), -112.0, 100.0)


def narrowed(value, exponent):
    return (value * jnp.exp2(exponent)).astype(jnp.float16)


def with_exponent(scaled, exponent):
    note = jnp.broadcast_to(exponent.astype(jnp.float16), (16, scaled.shape[1]))
    return jnp.concatenate([scaled, note], axis=0)


def widened(packed):
    rows = packed.shape[0] - 16
    return packed[:rows].astype(F32) * jnp.exp2(-packed[rows : rows + 1].astype(F32))


def scatter_high(part, width, near):
    if not staged():
        return ()
    low, high, rows = row_blocks(width)
    value = part((2 * (1 - high) + low) * rows, rows) + near[0]
    exponent = scale_of(value)
    return over_dp(with_exponent(narrowed(value, exponent), exponent), 2)


def scatter_ctx(part, width, near, far):
    if not staged():
        return (
            lax.psum_scatter(part(0, width), ("dp", "ctx"), scatter_dimension=0, tiled=True),
            (),
        )
    low, high, rows = row_blocks(width)
    n_ctx, c = lax.axis_size("ctx"), lax.axis_index("ctx")
    held = part((2 * high + low) * rows, rows) + near[1] + widened(far)
    block = rows // n_ctx
    exponent = scale_of(held)
    scaled = narrowed(held, exponent)
    sent = []
    for k in range(1, n_ctx):
        give = lax.dynamic_slice_in_dim(scaled, lax.rem(c + k, n_ctx) * block, block, 0)
        give = with_exponent(give, exponent)
        sent.append(lax.ppermute(give, "ctx", [(m, (m + k) % n_ctx) for m in range(n_ctx)]))
    return lax.dynamic_slice_in_dim(held, c * block, block, 0), sent


def scatter_sum(total, sent):
    for packed in sent:
        total = total + widened(packed)
    return total


def scatter_end(part, width, near, far):
    return scatter_sum(*scatter_ctx(part, width, near, far))


def tie(first, second):
    return lax.optimization_barrier((first, second))


def chain(own, totals, backward):
    count = lax.axis_size("ctx")
    if count == 1:
        return [jnp.zeros_like(part) for part in own], own[0]
    entering = [None] * len(own)
    leaving = list(own)
    mark = own[0]
    for hop in range(count - 1):
        pair = (count - 1 - hop, count - 2 - hop) if backward else (hop, hop + 1)
        received = []
        for k, part in enumerate(leaving):
            if k:
                part, received[k - 1] = tie(part, received[k - 1])
            received.append(lax.ppermute(part, "ctx", [pair]))
        if hop == 1:
            mark = received[0]
        entering = received if hop == 0 else [e + r for e, r in zip(entering, received)]
        leaving = [t * r + o for t, r, o in zip(totals, received, own)]
    return entering, mark


def segment_lengths():
    return [CONV * INNER, INNER, INNER, 2 * CONV * STATE, 2 * STATE, HEADS, HEADS, HEADS, D]


def unpack(flat):
    pieces = []
    offset = 0
    for length in segment_lengths():
        pieces.append(flat[offset : offset + length])
        offset += length
    return pieces


def silu_grad(value):
    sigma = jax.nn.sigmoid(value)
    return sigma * (1.0 + value * (1.0 - sigma))


def conv_forward(extended, kernel, offset_bias, length):
    total = jnp.zeros(extended[:, :length].shape, F32) + offset_bias
    for tap_index in range(CONV):
        total = total + kernel[tap_index] * extended[:, tap_index : tap_index + length]
    return total


def conv_backward(slope, follow, extended, kernel, length):
    padded = jnp.concatenate([slope, follow], axis=1)
    grad_input = jnp.zeros(slope.shape, F32)
    kernel_grads = []
    for tap_index in range(CONV):
        begin = CONV - 1 - tap_index
        grad_input = grad_input + kernel[tap_index] * padded[:, begin : begin + length]
        kernel_grads.append(
            jnp.sum(slope * extended[:, tap_index : tap_index + length], axis=(0, 1))
        )
    return (grad_input, jnp.stack(kernel_grads), jnp.sum(slope, axis=(0, 1)))


def dot(left, right, contract, exact=False):
    return lax.dot_general(
        left,
        right,
        ((contract[:1], contract[1:]), ((), ())),
        precision=HIGH if exact else None,
        preferred_element_type=F32,
    )


def adam_update(weight, moment, second, gradient, rate):
    moment = BETA_ONE * moment + (1.0 - BETA_ONE) * gradient
    second = BETA_TWO * second + (1.0 - BETA_TWO) * gradient * gradient
    moment_hat = moment / (1.0 - BETA_ONE**STEP)
    second_hat = second / (1.0 - BETA_TWO**STEP)
    weight = weight - rate * (moment_hat / (jnp.sqrt(second_hat) + ADAM_EPS) + DECAY_RATE * weight)
    return (weight, moment, second)


def einsum(spec, *parts):
    return jnp.einsum(spec, *parts, precision=HIGH, preferred_element_type=F32)


def on_device(
    layer_input,
    cotangent,
    in_proj,
    delta_proj,
    out_proj,
    state_proj,
    packed_params,
    moment_in,
    moment_delta,
    moment_out,
    moment_state,
    moment_packed,
    square_in,
    square_delta,
    square_out,
    square_state,
    square_packed,
):
    sizes = (lax.axis_size("dp"), lax.axis_size("ctx"), lax.axis_size("tensor"))
    n_dp, n_ctx, n_t = sizes
    groups = n_dp * n_ctx
    rank = lax.axis_index("tensor")
    seqs, tokens, width = layer_input.shape
    rows = seqs * tokens
    local_inner = in_proj.shape[2]
    local_heads = delta_proj.shape[1]
    own_width = width // n_t
    rim = CONV - 1

    state_rows_own = state_proj.shape[0]
    pack_own = packed_params.shape[0]
    state_piece = jnp.concatenate(
        [state_proj[:, 0].astype(BF), state_proj[:, 1].astype(BF)], axis=0
    )
    state_pad = cdiv(2 * state_rows_own, 16) * 16
    delta_pad = cdiv(local_heads, 16) * 16
    pack_rows = cdiv(pack_own, LANES)
    pack_pad = cdiv(pack_rows, 16) * 16
    proj_rows = delta_proj.shape[0]
    block = jnp.concatenate(
        [
            jnp.pad(state_piece, ((0, state_pad - 2 * state_rows_own), (0, 0))),
            jnp.pad(
                delta_proj.astype(BF).T, ((0, delta_pad - local_heads), (0, LANES - proj_rows))
            ),
            jnp.pad(
                jnp.pad(packed_params.astype(BF), (0, pack_rows * LANES - pack_own)).reshape(
                    pack_rows, LANES
                ),
                ((0, pack_pad - pack_rows), (0, 0)),
            ),
        ],
        axis=0,
    )
    small = gather_small(block, sizes)
    wx = lax.all_gather(in_proj[:, 1].astype(BF), ("dp", "ctx"), axis=0, tiled=True)
    wz = lax.all_gather(in_proj[:, 0].astype(BF), ("dp", "ctx"), axis=0, tiled=True)
    small, late_cotangent = tie(small, cotangent)
    up_own = late_cotangent.astype(BF)
    if n_t == 2:
        up_away = swap(up_own)
        first = rank == 0
        up_full = jnp.concatenate(
            [jnp.where(first, up_own, up_away), jnp.where(first, up_away, up_own)], axis=2
        )
    else:
        up_full = lax.all_gather(up_own, "tensor", axis=2, tiled=True)
    up_rows = up_full.reshape(rows, width)

    state_slots = small[..., : 2 * state_rows_own, :].reshape(-1, 2, state_rows_own, STATE)
    ws = jnp.concatenate(
        [state_slots[:, 0].reshape(width, STATE), state_slots[:, 1].reshape(width, STATE)], axis=1
    )
    delta_slots = lax.dynamic_index_in_dim(small, rank, 2, False)
    delta_slots = delta_slots[..., state_pad : state_pad + local_heads, :proj_rows]
    wd = delta_slots.reshape(groups, local_heads, proj_rows).transpose(0, 2, 1)
    wd = wd.reshape(width, local_heads)
    pack_slots = small[..., state_pad + delta_pad : state_pad + delta_pad + pack_rows, :]
    packed = pack_slots.reshape(groups * n_t, pack_rows * LANES)[:, :pack_own].reshape(-1)
    pieces = unpack(packed.astype(F32))
    conv_kernel = lax.dynamic_slice_in_dim(
        pieces[0].reshape(CONV, INNER), rank * local_inner, local_inner, 1
    )
    conv_bias = lax.dynamic_slice_in_dim(pieces[1], rank * local_inner, local_inner, 0)
    gate_gain = lax.dynamic_slice_in_dim(pieces[2], rank * local_inner, local_inner, 0)
    state_kernel = pieces[3].reshape(CONV, 2 * STATE)
    state_bias = pieces[4]
    delta_bias = lax.dynamic_slice_in_dim(pieces[5], rank * local_heads, local_heads, 0)
    log_rates = lax.dynamic_slice_in_dim(pieces[6], rank * local_heads, local_heads, 0)
    skip_gain = lax.dynamic_slice_in_dim(pieces[7], rank * local_heads, local_heads, 0)
    norm_gain = pieces[8]
    rates = -jnp.exp(log_rates)

    input_float = layer_input.astype(F32)
    inverse = lax.rsqrt(jnp.mean(input_float * input_float, axis=-1, keepdims=True) + NORM_EPS)
    normed = (input_float * inverse * norm_gain).astype(BF).reshape(rows, width)
    sproj = dot(normed, ws, (1, 0)).astype(BF).reshape(seqs, tokens, 2 * STATE)
    raw = dot(normed, wd, (1, 0)).reshape(seqs, tokens, local_heads)
    xproj = dot(normed, wx, (1, 0)).astype(BF).reshape(seqs, tokens, local_inner)
    tails = from_behind(
        jnp.concatenate([xproj[:, tokens - rim :], sproj[:, tokens - rim :]], axis=2), "ctx", 1
    )
    ext_x = jnp.concatenate([tails[:, :, :local_inner], xproj], axis=1).astype(F32)
    ext_s = jnp.concatenate([tails[:, :, local_inner:], sproj], axis=1).astype(F32)
    conv_x = conv_forward(ext_x, conv_kernel, conv_bias, tokens)
    conv_s = conv_forward(ext_s, state_kernel, state_bias, tokens)
    act_x = jax.nn.silu(conv_x).astype(BF)
    act_s = jax.nn.silu(conv_s).astype(BF)
    delta = jax.nn.softplus(raw + delta_bias)
    wv = act_s[:, :, :STATE]
    rv = act_s[:, :, STATE:]
    past = (jnp.arange(tokens)[:, None] >= jnp.arange(tokens)[None, :]).astype(F32)
    cum = einsum("tm,smh->sth", past, delta * rates)
    totals = jnp.exp(cum[:, -1])
    fade_decay = jnp.exp(cum[:, -1:] - cum)
    fading = fade_decay * delta
    growth = jnp.exp(cum)
    spread = [
        jnp.broadcast_to(
            jnp.repeat(totals[k], HEAD_DIM)[:, None], (local_inner, STATE)
        )
        for k in range(seqs)
    ]
    cum_t = jnp.swapaxes(cum, 1, 2)
    skip_lanes = jnp.repeat(skip_gain, HEAD_DIM)[None, :]
    own_state = [scan_state(act_x, wv, fading, k) for k in range(seqs)]
    within = scan_within(act_x, wv, rv, cum, cum_t, jnp.swapaxes(delta, 1, 2))
    own_state, normed_late = tie(own_state, normed)
    zproj = dot(normed_late, wz, (1, 0)).astype(BF).reshape(seqs, tokens, local_inner)
    entering, mark = chain(own_state, spread, False)
    out_half = tie(out_proj.astype(BF), mark)[0]
    wo = lax.all_gather(out_half, ("dp", "ctx"), axis=0, tiled=True)
    entering = jnp.stack(entering, axis=0)

    plain, mixed, square_sums = scan_gate(within, act_x, zproj, rv, growth, entering, skip_lanes)
    gate_input = zproj.astype(F32)
    gate_act = jax.nn.silu(gate_input)
    mixer = plain + skip_lanes * act_x.astype(F32)
    square_sums = sum_tensor(square_sums[:, :, 0])
    gate_inverse = lax.rsqrt(square_sums / INNER + NORM_EPS)[:, :, None]
    gated = (mixed * gate_inverse * gate_gain).astype(BF).reshape(rows, local_inner)

    def out_columns(start):
        return dot(gated, lax.dynamic_slice_in_dim(wo, start, own_width, 0), (1, 1))

    branch, branch_away = scatter_tensor(out_columns, own_width, rank)
    own_input = lax.dynamic_slice_in_dim(layer_input, rank * own_width, own_width, 2).astype(F32)

    gated_grad = dot(up_rows, wo, (1, 0)).reshape(seqs, tokens, local_inner)
    part_out = cut_dot(up_rows, gated)
    near_out = scatter_start(part_out, width)
    scaled = gated_grad * gate_gain
    row_sums = sum_tensor(jnp.sum(scaled * mixed, axis=-1))
    mixed_grad = gate_inverse * scaled - mixed * gate_inverse**3 * (row_sums / INNER)[:, :, None]
    grad_gate_gain = jnp.sum(gated_grad * mixed * gate_inverse, axis=(0, 1))
    mixer_grad = mixed_grad * gate_act
    z_grad = (mixed_grad * mixer * silu_grad(gate_input)).astype(BF).reshape(rows, local_inner)
    part_z = cut_dot(normed, z_grad)

    pulled = [scan_state(mixer_grad, rv, growth, k) for k in range(seqs)]
    dy = mixer_grad
    dx_bare, dw, dr = scan_within_back(dy, act_x, wv, rv, cum, cum_t, delta)
    dx_bare, near_out = tie(dx_bare, near_out)
    far_out = scatter_high(part_out, width, near_out)
    near_z = scatter_start(part_z, width)
    leaving = jnp.stack(chain(pulled, spread, True)[0], axis=0)
    dx, dw, dr, bare_dot, fade_dot, plain_dot, skip_dot = scan_state_back(
        dy, act_x, plain, dx_bare, wv, delta, fading, growth, entering, leaving, skip_lanes, dw, dr
    )
    dx, (far_out, near_z) = tie(dx, (far_out, near_z))
    far_z = scatter_high(part_z, width, near_z)
    grad_out = scatter_end(part_out, width, near_out, far_out)
    cum_grad = plain_dot - delta * bare_dot - fading * fade_dot
    end_grad = jnp.sum(fading * fade_dot, axis=1) + totals * jnp.sum(
        (leaving * entering).reshape(seqs, local_heads, HEAD_DIM, STATE), axis=(2, 3)
    )
    step_grad = (
        einsum("tm,sth->smh", past, cum_grad) + end_grad[:, None, :]
    )
    delta_grad = bare_dot + fade_decay * fade_dot + rates * step_grad
    grad_rates = jnp.sum(delta * step_grad, axis=(0, 1))
    grad_skip = jnp.sum(skip_dot.reshape(seqs, local_heads, HEAD_DIM), axis=(0, 2))
    grad_log_rates = grad_rates * rates
    raw_grad = delta_grad * jax.nn.sigmoid(raw + delta_bias)
    grad_delta_bias = jnp.sum(raw_grad, axis=(0, 1))

    slope_x = dx.reshape(seqs, tokens, local_inner) * silu_grad(conv_x)
    slope_s = jnp.concatenate([dw, dr], axis=-1) * silu_grad(conv_s)
    follow = from_behind(
        jnp.concatenate([slope_x[:, :rim], slope_s[:, :rim]], axis=2), "ctx", -1
    )
    back_x, grad_conv_kernel, grad_conv_bias = conv_backward(
        slope_x, follow[:, :, :local_inner], ext_x, conv_kernel, tokens
    )
    back_s, grad_state_kernel, grad_state_bias = conv_backward(
        slope_s, follow[:, :, local_inner:], ext_s, state_kernel, tokens
    )
    x_grad = back_x.astype(BF).reshape(rows, local_inner)
    state_rows = back_s.reshape(rows, 2 * STATE)
    raw_rows = raw_grad.reshape(rows, local_heads)

    def normed_columns(start):
        def cut(weight):
            return lax.dynamic_slice_in_dim(weight, start, own_width, 0)

        product = dot(x_grad, cut(wx), (1, 1))
        product_z = dot(z_grad, cut(wz), (1, 1))
        return (
            product
            + product_z
            + dot(state_rows, cut(ws).astype(F32), (1, 1), True)
            + dot(raw_rows, cut(wd).astype(F32), (1, 1), True)
        )

    x_grad, (branch_away, far_z, grad_out) = tie(x_grad, (branch_away, far_z, grad_out))
    layer_output = own_input + (branch + branch_away).reshape(seqs, tokens, own_width)
    held_z, sent_z = scatter_ctx(part_z, width, near_z, far_z)
    pieces_x = 2 if local_inner % (2 * LANES) == 0 else 1
    piece = local_inner // pieces_x
    parts_x = [
        cut_dot(normed, x_grad[:, k * piece : (k + 1) * piece]) for k in range(pieces_x)
    ]
    near_x = []
    for part in parts_x:
        near_x.append(scatter_start(part, width))

    starts = [(1 - rank) * own_width, rank * own_width]
    if n_t != 2:
        starts = [k * own_width for k in range(n_t)]
    columns = [normed_columns(start) for start in starts]
    if n_t == 2:
        normed_grad = columns[1] + swap(columns[0])
    else:
        normed_grad = lax.psum_scatter(
            jnp.concatenate(columns, axis=1), "tensor", scatter_dimension=1, tiled=True
        )
    normed_grad = normed_grad.reshape(seqs, tokens, own_width)
    own_gain = lax.dynamic_slice_in_dim(norm_gain, rank * own_width, own_width, 0)
    grad_norm_gain = jnp.zeros((D,), F32)
    in_sums = 0.0
    for start, part in zip(starts, columns):
        inputs = lax.dynamic_slice_in_dim(layer_input, start, own_width, 2).astype(F32)
        gain = lax.dynamic_slice_in_dim(norm_gain, start, own_width, 0)
        product = part.reshape(seqs, tokens, own_width) * inputs
        in_sums = in_sums + jnp.sum(product * gain, axis=-1)
        grad_norm_gain = lax.dynamic_update_slice_in_dim(
            grad_norm_gain, jnp.sum(product * inverse, axis=(0, 1)), start, 0
        )
    scaled_in = normed_grad * own_gain

    normed_float = normed.astype(F32)
    grad_state_part = dot(normed_float, state_rows, (0, 0), True)
    grad_delta_part = dot(normed_float, raw_rows, (0, 0), True)

    def widen(local_values, full_length):
        return lax.dynamic_update_slice_in_dim(
            jnp.zeros((full_length,), F32), local_values, rank * local_values.shape[0], 0
        )

    conv_wide = lax.dynamic_update_slice_in_dim(
        jnp.zeros((CONV, INNER), F32), grad_conv_kernel, rank * local_inner, 1
    ).reshape(-1)
    joined = jnp.concatenate(
        [
            conv_wide,
            widen(grad_conv_bias, INNER),
            widen(grad_gate_gain, INNER),
            grad_state_kernel.reshape(-1),
            grad_state_bias,
            widen(grad_delta_bias, HEADS),
            widen(grad_log_rates, HEADS),
            widen(grad_skip, HEADS),
            grad_norm_gain,
        ]
    )
    pack_group = n_t * pack_own
    packed_part = jnp.pad(joined, (0, groups * pack_group - joined.shape[0]))
    pack_cols = cdiv(pack_group, proj_rows)
    packed_part = jnp.pad(
        packed_part.reshape(groups, pack_group), ((0, 0), (0, pack_cols * proj_rows - pack_group))
    ).reshape(width, pack_cols)
    extra_pad = cdiv(local_heads + pack_cols, LANES) * LANES - local_heads - pack_cols
    tail_part = jnp.concatenate(
        [
            grad_state_part,
            grad_delta_part,
            packed_part,
            jnp.zeros((width, extra_pad), F32),
        ],
        axis=1,
    )
    far_x = []
    for k, part in enumerate(parts_x):
        if k:
            near_x[k], far_x[k - 1] = tie(near_x[k], far_x[k - 1])
        far_x.append(scatter_high(part, width, near_x[k]))
    blocks_x = []
    for k, part in enumerate(parts_x):
        blocks_x.append(scatter_ctx(part, width, near_x[k], far_x[k]))
    grad_x = jnp.concatenate([scatter_sum(*block) for block in blocks_x], axis=1)

    grad_x, (in_sums, sent_z) = tie(grad_x, (in_sums, sent_z))
    grad_z = scatter_sum(held_z, sent_z)
    in_mean = sum_tensor(in_sums)[:, :, None] / width
    input_grad = cotangent + inverse * scaled_in - own_input * inverse**3 * in_mean

    def part_tail(start, rows):
        return lax.dynamic_slice_in_dim(tail_part, start, rows, 0)

    near_tail = scatter_start(part_tail, width)
    far_tail = scatter_high(part_tail, width, near_tail)
    tail = scatter_end(part_tail, width, near_tail, far_tail)
    at = 2 * STATE
    grad_delta = tail[:, at : at + local_heads]
    state_group = tail[:, :at]
    packed_group = tail[:, at + local_heads : at + local_heads + pack_cols]
    packed_group = packed_group.reshape(-1)[:pack_group]
    if n_t == 2:
        away = swap(
            (
                lax.dynamic_slice_in_dim(
                    state_group, (1 - rank) * state_rows_own, state_rows_own, 0
                ),
                lax.dynamic_slice_in_dim(packed_group, (1 - rank) * pack_own, pack_own, 0),
            )
        )
        grad_state = (
            lax.dynamic_slice_in_dim(state_group, rank * state_rows_own, state_rows_own, 0)
            + away[0]
        )
        grad_packed = (
            lax.dynamic_slice_in_dim(packed_group, rank * pack_own, pack_own, 0) + away[1]
        )
    else:
        grad_state = lax.psum_scatter(state_group, "tensor", scatter_dimension=0, tiled=True)
        grad_packed = lax.psum_scatter(packed_group, "tensor", scatter_dimension=0, tiled=True)
    grad_state = grad_state.reshape(state_rows_own, 2, STATE)
    grad_in = jnp.stack([grad_z, grad_x], axis=1)

    new_in, next_moment_in, next_square_in = adam_update(
        in_proj, moment_in, square_in, grad_in, MATRIX_RATE
    )
    new_delta, next_moment_delta, next_square_delta = adam_update(
        delta_proj, moment_delta, square_delta, grad_delta, MATRIX_RATE
    )
    new_out, next_moment_out, next_square_out = adam_update(
        out_proj, moment_out, square_out, grad_out, MATRIX_RATE
    )
    new_state, next_moment_state, next_square_state = adam_update(
        state_proj, moment_state, square_state, grad_state, MATRIX_RATE
    )
    new_packed, next_moment_packed, next_square_packed = adam_update(
        packed_params, moment_packed, square_packed, grad_packed, PACKED_RATE
    )
    return (
        layer_output,
        input_grad,
        grad_in,
        grad_delta,
        grad_out,
        grad_state,
        grad_packed,
        new_in,
        new_delta,
        new_out,
        new_state,
        new_packed,
        next_moment_in,
        next_moment_delta,
        next_moment_out,
        next_moment_state,
        next_moment_packed,
        next_square_in,
        next_square_delta,
        next_square_out,
        next_square_state,
        next_square_packed,
    )


def solution(mesh):
    matrix = P(("dp", "ctx"), "tensor")
    projection = P(("dp", "ctx"), None, "tensor")
    state = P(("dp", "ctx", "tensor"), None, None)
    flat = P(("dp", "ctx", "tensor"))
    tokens = P("dp", "ctx", "tensor")
    weights = (projection, matrix, matrix, state, flat)

    return jax.shard_map(
        on_device,
        mesh=mesh,
        in_specs=(P("dp", "ctx", None), tokens) + weights * 3,
        out_specs=(tokens, tokens) + weights * 4,
        check_vma=False,
    )
```

```python
import functools

import jax
import jax.numpy as jnp
from jax import lax
from jax.experimental import pallas as pl
from jax.experimental.pallas import tpu as pltpu
from jax.sharding import PartitionSpec as P


D = 1536
HEADS = 48
HEAD_DIM = 64
STATE = 128
CONV = 4
STEP = 3
INNER = 3072
LANES = 128

NORM_EPS = 1e-05
BETA_ONE = 0.9
BETA_TWO = 0.999
ADAM_EPS = 1e-08
DECAY_RATE = 0.1
MATRIX_RATE = 0.01
PACKED_RATE = 0.1
HIGH = lax.Precision.HIGHEST
MESH = pl.DeviceIdType.MESH
BF = jnp.bfloat16
F32 = jnp.float32


def cdiv(a, b):
    return -(-a // b)


def gather_kernel(sizes, in_ref, out_ref, local_sem, send_sem, recv_sem):
    n_dp, n_ctx, n_t = sizes
    d, c, t = lax.axis_index("dp"), lax.axis_index("ctx"), lax.axis_index("tensor")
    peers = []
    for k in range(1, n_ctx):
        peers.append((d, lax.rem(c + k, n_ctx), t))
    for k in range(1, n_t):
        peers.append((d, c, lax.rem(t + k, n_t)))
    for k in range(1, n_dp):
        peers.append((lax.rem(d + k, n_dp), c, t))
    barrier = pltpu.get_barrier_semaphore()
    for peer in peers:
        pl.semaphore_signal(barrier, inc=1, device_id=peer, device_id_type=MESH)
    pl.semaphore_wait(barrier, len(peers))
    own = pltpu.make_async_copy(in_ref, out_ref.at[d, c, t], local_sem)
    own.start()
    own.wait()
    number = 0

    def stage(copies):
        for copy in copies:
            copy.start()
        for copy in copies:
            copy.wait()

    copies = []
    for k in range(1, n_ctx):
        view = out_ref.at[d, c, t]
        copies.append(
            pltpu.make_async_remote_copy(
                src_ref=view,
                dst_ref=view,
                send_sem=send_sem.at[number],
                recv_sem=recv_sem.at[number],
                device_id=(d, lax.rem(c + k, n_ctx), t),
                device_id_type=MESH,
            )
        )
        number += 1
    stage(copies)
    copies = []
    for k in range(1, n_t):
        view = out_ref.at[d, :, t]
        copies.append(
            pltpu.make_async_remote_copy(
                src_ref=view,
                dst_ref=view,
                send_sem=send_sem.at[number],
                recv_sem=recv_sem.at[number],
                device_id=(d, c, lax.rem(t + k, n_t)),
                device_id_type=MESH,
            )
        )
        number += 1
    stage(copies)
    copies = []
    for k in range(1, n_dp):
        view = out_ref.at[d]
        copies.append(
            pltpu.make_async_remote_copy(
                src_ref=view,
                dst_ref=view,
                send_sem=send_sem.at[number],
                recv_sem=recv_sem.at[number],
                device_id=(lax.rem(d + k, n_dp), c, t),
                device_id_type=MESH,
            )
        )
        number += 1
    stage(copies)


def gather_small(block, sizes):
    count = sum(sizes) - 3
    return pl.pallas_call(
        functools.partial(gather_kernel, sizes),
        out_shape=jax.ShapeDtypeStruct(sizes + block.shape, block.dtype),
        in_specs=[pl.BlockSpec(memory_space=pltpu.VMEM)],
        out_specs=pl.BlockSpec(memory_space=pltpu.VMEM),
        scratch_shapes=[
            pltpu.SemaphoreType.DMA(()),
            pltpu.SemaphoreType.DMA((count,)),
            pltpu.SemaphoreType.DMA((count,)),
        ],
        compiler_params=pltpu.CompilerParams(collective_id=0, has_side_effects=True),
        name="gather_small",
    )(block)


PAIR = LANES // HEAD_DIM


def step_width(inner):
    return 3 * LANES if inner % (3 * LANES) == 0 else LANES


def matmul(left, right, contract):
    return lax.dot_general(
        left, right, ((contract[:1], contract[1:]), ((), ())), preferred_element_type=F32
    )


def split(value):
    high = value.astype(BF)
    return high, (value - high.astype(F32)).astype(BF)


def dot_exact_right(left, right, contract):
    high, low = split(left)
    return matmul(high, right, contract) + matmul(low, right, contract)


def dot_exact_left(left, right, contract):
    high, low = split(right)
    return matmul(left, high, contract) + matmul(left, low, contract)


def dot_terms(left, right, contract):
    left_high, left_low = split(left)
    right_high, right_low = split(right)
    return (
        matmul(left_high, right_high, contract)
        + matmul(left_high, right_low, contract)
        + matmul(left_low, right_high, contract)
    )


def picker(heads, first, width, each):
    row = lax.broadcasted_iota(jnp.int32, (heads, width), 0)
    lane = lax.broadcasted_iota(jnp.int32, (heads, width), 1)
    return jnp.where(row == first + lane // each, 1.0, 0.0).astype(BF)


def spread_exact(values, first, width, each):
    pick = picker(values.shape[1], first, width, each)
    high = values.astype(BF)
    rest = values - high.astype(F32)
    middle = rest.astype(BF)
    low = (rest - middle.astype(F32)).astype(BF)
    return matmul(high, pick, (1, 0)) + (matmul(middle, pick, (1, 0)) + matmul(low, pick, (1, 0)))


def place_heads(values, first, heads):
    width = values.shape[1]
    lane = lax.broadcasted_iota(jnp.int32, (width, heads), 0)
    column = lax.broadcasted_iota(jnp.int32, (width, heads), 1)
    pick = jnp.where(column == first + lane // HEAD_DIM, 1.0, 0.0).astype(BF)
    return dot_exact_right(values, pick, (1, 0))


def twice(value, wide):
    count = wide // LANES
    return value if count <= 1 else jnp.concatenate([value] * count, axis=1)


def state_kernel(v_ref, u_ref, scale_ref, out_ref):
    width = v_ref.shape[2]
    first = pl.program_id(0) * (width // HEAD_DIM)
    scaled = v_ref[0].astype(F32) * spread_exact(scale_ref[0], first, width, HEAD_DIM)
    out_ref[...] = dot_exact_right(scaled, u_ref[0], (0, 0))


def within_kernel(x_ref, w_ref, r_ref, cum_ref, cum_t_ref, delta_t_ref, out_ref, score_ref, down_ref):
    step = pl.program_id(1)
    tokens, width = x_ref.shape[1:]
    edge = min(tokens, LANES)
    count = width // HEAD_DIM
    first = step * count

    @pl.when(step == 0)
    def _():
        score_ref[...] = matmul(r_ref[0], w_ref[0], (1, 1))

    down_ref[...] = spread_exact(cum_ref[0], first, count * LANES, LANES)
    lanes = lax.broadcasted_iota(jnp.int32, (edge, LANES), 1)
    for top in range(0, tokens, edge):
        wide = top + edge
        rows_at = top + lax.broadcasted_iota(jnp.int32, (edge, wide), 0)
        causal = rows_at >= lax.broadcasted_iota(jnp.int32, (edge, wide), 1)
        score = score_ref[top:wide, :wide]
        for tile in range(width // LANES):
            channels = slice(tile * LANES, (tile + 1) * LANES)
            x = x_ref[0, :wide, channels]
            result = None
            for k in range(PAIR):
                at = tile * PAIR + k
                down = twice(down_ref[top:wide, at * LANES : (at + 1) * LANES], wide)
                across = cum_t_ref[0, pl.ds(first + at, 1), :][:, :wide]
                scale = delta_t_ref[0, pl.ds(first + at, 1), :][:, :wide]
                decays = jnp.exp(jnp.where(causal, down - across, -1e30))
                part = dot_exact_right(decays * (score * scale), x, (1, 0))
                result = part if k == 0 else jnp.where(lanes < k * HEAD_DIM, result, part)
            out_ref[0, top:wide, channels] = result


def gate_kernel(
    within_ref, x_ref, z_ref, r_ref, growth_ref, enter_ref, skip_ref, plain_ref, mixed_ref, sum_ref
):
    step = pl.program_id(1)
    width = x_ref.shape[2]
    first = step * (width // HEAD_DIM)
    carried = dot_exact_left(r_ref[0], enter_ref[0], (1, 1))
    plain = within_ref[0] + carried * spread_exact(growth_ref[0], first, width, HEAD_DIM)
    plain_ref[0] = plain
    gate = z_ref[0].astype(F32)
    mixed = (plain + skip_ref[...] * x_ref[0].astype(F32)) * (gate * jax.nn.sigmoid(gate))
    mixed_ref[0] = mixed

    @pl.when(step == 0)
    def _():
        sum_ref[...] = jnp.zeros_like(sum_ref)

    sum_ref[0] += jnp.sum(mixed * mixed, axis=1, keepdims=True)


def within_back_kernel(
    dy_ref, x_ref, w_ref, r_ref, cum_ref, cum_t_ref, delta_ref, bare_ref, dw_ref, dr_ref,
    score_ref, total_ref, down_ref, scale_ref,
):
    step = pl.program_id(1)
    tokens, width = x_ref.shape[1:]
    edge = min(tokens, LANES)
    count = width // HEAD_DIM
    first = step * count

    @pl.when(step == 0)
    def _():
        score_ref[...] = matmul(w_ref[0], r_ref[0], (1, 1))
        total_ref[...] = jnp.zeros_like(total_ref)

    down_ref[...] = spread_exact(cum_ref[0], first, count * LANES, LANES)
    scale_ref[...] = spread_exact(delta_ref[0], first, count * LANES, LANES)
    for top in range(0, tokens, edge):
        wide = tokens - top
        rows_at = lax.broadcasted_iota(jnp.int32, (edge, wide), 0)
        causal = rows_at <= lax.broadcasted_iota(jnp.int32, (edge, wide), 1)
        lanes = lax.broadcasted_iota(jnp.int32, (wide, LANES), 1)
        near = lax.broadcasted_iota(jnp.int32, (edge, LANES), 1)
        score = score_ref[top : top + edge, top:]
        added = None
        for tile in range(width // LANES):
            channels = slice(tile * LANES, (tile + 1) * LANES)
            x = x_ref[0, top : top + edge, channels]
            dy_high, dy_low = split(dy_ref[0, top:, channels])
            zero = jnp.zeros_like(dy_high)
            result = None
            for k in range(PAIR):
                at = tile * PAIR + k
                down = twice(down_ref[top : top + edge, at * LANES : (at + 1) * LANES], wide)
                scale = twice(scale_ref[top : top + edge, at * LANES : (at + 1) * LANES], wide)
                across = cum_t_ref[0, pl.ds(first + at, 1), :][:, top:]
                decays = jnp.exp(jnp.where(causal, across - down, -1e30))
                high, low = split(decays * score)
                part = matmul(high, dy_high, (1, 0)) + matmul(high, dy_low, (1, 0))
                part = part + matmul(low, dy_high, (1, 0))
                result = part if k == 0 else jnp.where(near < k * HEAD_DIM, result, part)
                mine = (lanes >= k * HEAD_DIM) & (lanes < (k + 1) * HEAD_DIM)
                pairs = matmul(x, jnp.where(mine, dy_high, zero), (1, 1))
                pairs = pairs + matmul(x, jnp.where(mine, dy_low, zero), (1, 1))
                term = pairs * decays * scale
                added = term if added is None else added + term
            bare_ref[0, top : top + edge, channels] = result
        total_ref[top : top + edge, top:] += added

    @pl.when(step == pl.num_programs(1) - 1)
    def _():
        high, low = split(total_ref[...])
        dw_ref[0] = matmul(high, r_ref[0], (1, 0)) + matmul(low, r_ref[0], (1, 0))
        dr_ref[0] = matmul(high, w_ref[0], (0, 0)) + matmul(low, w_ref[0], (0, 0))


def state_back_kernel(
    dy_ref, x_ref, plain_ref, bare_ref, w_ref, delta_ref, fading_ref, growth_ref, enter_ref,
    leave_ref, skip_ref, dw_in_ref, dr_in_ref, dx_ref, dw_ref, dr_ref, bare_dot_ref, fade_dot_ref,
    plain_dot_ref, skip_dot_ref,
):
    step = pl.program_id(1)
    width = x_ref.shape[2]
    first = step * (width // HEAD_DIM)
    heads = delta_ref.shape[2]

    @pl.when(step == 0)
    def _():
        dw_ref[...] = dw_in_ref[...]
        dr_ref[...] = dr_in_ref[...]
        bare_dot_ref[...] = jnp.zeros_like(bare_dot_ref)
        fade_dot_ref[...] = jnp.zeros_like(fade_dot_ref)
        plain_dot_ref[...] = jnp.zeros_like(plain_dot_ref)

    x = x_ref[0].astype(F32)
    dy = dy_ref[0]
    bare = bare_ref[0]
    fading = spread_exact(fading_ref[0], first, width, HEAD_DIM)
    reach = dot_exact_left(w_ref[0], leave_ref[0], (1, 1))
    dx_ref[0] = (
        spread_exact(delta_ref[0], first, width, HEAD_DIM) * bare
        + fading * reach
        + skip_ref[...] * dy
    )
    growth = spread_exact(growth_ref[0], first, width, HEAD_DIM)
    dr_ref[0] += dot_terms(dy * growth, enter_ref[0], (1, 0))
    dw_ref[0] += dot_terms(x * fading, leave_ref[0], (1, 0))
    bare_dot_ref[0] += place_heads(x * bare, first, heads)
    fade_dot_ref[0] += place_heads(x * reach, first, heads)
    plain_dot_ref[0] += place_heads(dy * plain_ref[0], first, heads)
    skip_dot_ref[0] = jnp.sum(dy * x, axis=0, keepdims=True)


def scan_specs(tokens, inner, heads):
    width = step_width(inner)
    tile = pl.BlockSpec((1, tokens, width), lambda s, j: (s, 0, j))
    state = pl.BlockSpec((1, tokens, STATE), lambda s, j: (s, 0, 0))
    per_head = pl.BlockSpec((1, tokens, heads), lambda s, j: (s, 0, 0))
    per_head_t = pl.BlockSpec((1, heads, tokens), lambda s, j: (s, 0, 0))
    carry = pl.BlockSpec((1, width, STATE), lambda s, j: (s, j, 0))
    lane = pl.BlockSpec((1, width), lambda s, j: (0, j))
    one = pl.BlockSpec((1, tokens, 1), lambda s, j: (s, 0, 0))
    lane_sum = pl.BlockSpec((1, 1, width), lambda s, j: (s, 0, j))
    return tile, state, per_head, per_head_t, carry, lane, one, lane_sum


def shaped(*shape):
    return jax.ShapeDtypeStruct(shape, F32)


def scan_call(kernel, grid, in_specs, out_specs, out_shape, scratch, flops, moved):
    return pl.pallas_call(
        kernel,
        grid=grid,
        in_specs=in_specs,
        out_specs=out_specs,
        out_shape=out_shape,
        scratch_shapes=scratch,
        cost_estimate=pl.CostEstimate(flops=flops, bytes_accessed=moved, transcendentals=0),
    )


def scan_state(v, u, scale, s):
    _, tokens, inner = v.shape
    heads = scale.shape[2]
    width = step_width(inner)
    return scan_call(
        state_kernel, (inner // width,),
        [
            pl.BlockSpec((1, tokens, width), lambda j: (s, 0, j)),
            pl.BlockSpec((1, tokens, STATE), lambda j: (s, 0, 0)),
            pl.BlockSpec((1, tokens, heads), lambda j: (s, 0, 0)),
        ],
        pl.BlockSpec((width, STATE), lambda j: (j, 0)), shaped(inner, STATE),
        [], 4 * tokens * inner * STATE, 8 * tokens * inner,
    )(v, u, scale)


def scan_states(v, u, scale):
    states = [scan_state(v, u, scale, 0)]
    return states + [scan_state(v, u, scale, k) for k in range(1, v.shape[0])]


def scan_within(x, w, r, cum, cum_t, delta_t):
    seqs, tokens, inner = x.shape
    width = step_width(inner)
    tile, state, per_head, per_head_t, _, _, _, _ = scan_specs(tokens, inner, cum.shape[2])
    size = seqs * tokens * inner
    return scan_call(
        within_kernel, (seqs, inner // width),
        [tile, state, state, per_head, per_head_t, per_head_t], tile, shaped(seqs, tokens, inner),
        [pltpu.VMEM((tokens, tokens), F32), pltpu.VMEM((tokens, PAIR * width), F32)],
        16 * size * tokens, 6 * size,
    )(x, w, r, cum, cum_t, delta_t)


def scan_gate(within, x, z, r, growth, enter, skip):
    seqs, tokens, inner = x.shape
    tile, state, per_head, _, carry, lane, one, _ = scan_specs(tokens, inner, growth.shape[2])
    size = seqs * tokens * inner
    return scan_call(
        gate_kernel, (seqs, inner // step_width(inner)),
        [tile, tile, tile, state, per_head, carry, lane], [tile, tile, one],
        [shaped(seqs, tokens, inner), shaped(seqs, tokens, inner), shaped(seqs, tokens, 1)],
        [], 8 * size * STATE, 16 * size,
    )(within, x, z, r, growth, enter, skip)


def scan_within_back(dy, x, w, r, cum, cum_t, delta):
    seqs, tokens, inner = x.shape
    width = step_width(inner)
    tile, state, per_head, per_head_t, _, _, _, _ = scan_specs(tokens, inner, cum.shape[2])
    size = seqs * tokens * inner
    square = pltpu.VMEM((tokens, tokens), F32)
    wide = pltpu.VMEM((tokens, PAIR * width), F32)
    return scan_call(
        within_back_kernel, (seqs, inner // width),
        [tile, tile, state, state, per_head, per_head_t, per_head], [tile, state, state],
        [shaped(seqs, tokens, inner), shaped(seqs, tokens, STATE), shaped(seqs, tokens, STATE)],
        [square, square, wide, wide], 32 * size * tokens, 10 * size,
    )(dy, x, w, r, cum, cum_t, delta)


def scan_state_back(dy, x, plain, bare, w, delta, fading, growth, enter, leave, skip, dw, dr):
    seqs, tokens, inner = x.shape
    heads = delta.shape[2]
    tile, state, per_head, _, carry, lane, _, lane_sum = scan_specs(tokens, inner, heads)
    size = seqs * tokens * inner
    sums = shaped(seqs, tokens, heads)
    return scan_call(
        state_back_kernel, (seqs, inner // step_width(inner)),
        [tile] * 4 + [state] + [per_head] * 3 + [carry, carry, lane, state, state],
        [tile, state, state, per_head, per_head, per_head, lane_sum],
        [shaped(seqs, tokens, inner), shaped(seqs, tokens, STATE), shaped(seqs, tokens, STATE)]
        + [sums] * 3 + [shaped(seqs, 1, inner)],
        [], 24 * size * STATE, 22 * size,
    )(dy, x, plain, bare, w, delta, fading, growth, enter, leave, skip, dw, dr)


def from_behind(value, axis, steps):
    count = lax.axis_size(axis)
    initial, last = (max(0, -steps), min(count, count - steps))
    return lax.ppermute(value, axis, [(source, source + steps) for source in range(initial, last)])


def swap(value):
    return lax.ppermute(value, "tensor", [(0, 1), (1, 0)])


def sum_tensor(value):
    if lax.axis_size("tensor") == 2:
        return value + swap(value)
    return lax.psum(value, "tensor")


def scatter_tensor(make, width, rank):
    if lax.axis_size("tensor") == 2:
        away = swap(make((1 - rank) * width))
        return make(rank * width), away
    whole = jnp.concatenate([make(k * width) for k in range(lax.axis_size("tensor"))], axis=-1)
    return lax.psum_scatter(whole, "tensor", scatter_dimension=whole.ndim - 1, tiled=True), 0.0


def over_dp(value, flip):
    return lax.ppermute(value, "dp", [(k, k ^ flip) for k in range(lax.axis_size("dp"))])


def row_blocks(width):
    d = lax.axis_index("dp")
    return lax.rem(d, 2), d // 2, width // lax.axis_size("dp")


def staged():
    return lax.axis_size("dp") == 4


def cut_dot(left, right):
    def part(start, rows):
        return dot(lax.dynamic_slice_in_dim(left, start, rows, 1), right, (0, 0))

    return part


def scatter_start(part, width):
    if not staged():
        return ()
    low, high, rows = row_blocks(width)
    first = part((2 * (1 - high) + 1 - low) * rows, rows)
    second = part((2 * high + 1 - low) * rows, rows)
    return over_dp(first, 1), over_dp(second, 1)


def scale_of(value):
    top = jnp.maximum(jnp.max(jnp.abs(value), axis=0, keepdims=True), 1e-37)
    return jnp.clip(jnp.floor(14.0 - jnp.log2(top)), -112.0, 100.0)


def narrowed(value, exponent):
    return (value * jnp.exp2(exponent)).astype(jnp.float16)


def with_exponent(scaled, exponent):
    note = jnp.broadcast_to(exponent.astype(jnp.float16), (16, scaled.shape[1]))
    return jnp.concatenate([scaled, note], axis=0)


def widened(packed):
    rows = packed.shape[0] - 16
    return packed[:rows].astype(F32) * jnp.exp2(-packed[rows : rows + 1].astype(F32))


def scatter_high(part, width, near):
    if not staged():
        return ()
    low, high, rows = row_blocks(width)
    value = part((2 * (1 - high) + low) * rows, rows) + near[0]
    exponent = scale_of(value)
    return over_dp(with_exponent(narrowed(value, exponent), exponent), 2)


def scatter_ctx(part, width, near, far):
    if not staged():
        return (
            lax.psum_scatter(part(0, width), ("dp", "ctx"), scatter_dimension=0, tiled=True),
            (),
        )
    low, high, rows = row_blocks(width)
    n_ctx, c = lax.axis_size("ctx"), lax.axis_index("ctx")
    held = part((2 * high + low) * rows, rows) + near[1] + widened(far)
    block = rows // n_ctx
    exponent = scale_of(held)
    scaled = narrowed(held, exponent)
    sent = []
    for k in range(1, n_ctx):
        give = lax.dynamic_slice_in_dim(scaled, lax.rem(c + k, n_ctx) * block, block, 0)
        give = with_exponent(give, exponent)
        sent.append(lax.ppermute(give, "ctx", [(m, (m + k) % n_ctx) for m in range(n_ctx)]))
    return lax.dynamic_slice_in_dim(held, c * block, block, 0), sent


def scatter_sum(total, sent):
    for packed in sent:
        total = total + widened(packed)
    return total


def scatter_end(part, width, near, far):
    return scatter_sum(*scatter_ctx(part, width, near, far))


def tie(first, second):
    return lax.optimization_barrier((first, second))


def chain(own, totals, backward):
    count = lax.axis_size("ctx")
    if count == 1:
        return [jnp.zeros_like(part) for part in own], own[0]
    entering = [None] * len(own)
    leaving = list(own)
    mark = own[0]
    for hop in range(count - 1):
        pair = (count - 1 - hop, count - 2 - hop) if backward else (hop, hop + 1)
        received = []
        for k, part in enumerate(leaving):
            if k:
                part, received[k - 1] = tie(part, received[k - 1])
            received.append(lax.ppermute(part, "ctx", [pair]))
        if hop == count - 2:
            mark = received[0]
        entering = received if hop == 0 else [e + r for e, r in zip(entering, received)]
        leaving = [t * r + o for t, r, o in zip(totals, received, own)]
    return entering, mark


def segment_lengths():
    return [CONV * INNER, INNER, INNER, 2 * CONV * STATE, 2 * STATE, HEADS, HEADS, HEADS, D]


def unpack(flat):
    pieces = []
    offset = 0
    for length in segment_lengths():
        pieces.append(flat[offset : offset + length])
        offset += length
    return pieces


def silu_grad(value):
    sigma = jax.nn.sigmoid(value)
    return sigma * (1.0 + value * (1.0 - sigma))


def conv_forward(extended, kernel, offset_bias, length):
    total = jnp.zeros(extended[:, :length].shape, F32) + offset_bias
    for tap_index in range(CONV):
        total = total + kernel[tap_index] * extended[:, tap_index : tap_index + length]
    return total


def conv_backward(slope, follow, extended, kernel, length):
    padded = jnp.concatenate([slope, follow], axis=1)
    grad_input = jnp.zeros(slope.shape, F32)
    kernel_grads = []
    for tap_index in range(CONV):
        begin = CONV - 1 - tap_index
        grad_input = grad_input + kernel[tap_index] * padded[:, begin : begin + length]
        kernel_grads.append(
            jnp.sum(slope * extended[:, tap_index : tap_index + length], axis=(0, 1))
        )
    return (grad_input, jnp.stack(kernel_grads), jnp.sum(slope, axis=(0, 1)))


def dot(left, right, contract, exact=False):
    return lax.dot_general(
        left,
        right,
        ((contract[:1], contract[1:]), ((), ())),
        precision=HIGH if exact else None,
        preferred_element_type=F32,
    )


def adam_update(weight, moment, second, gradient, rate):
    moment = BETA_ONE * moment + (1.0 - BETA_ONE) * gradient
    second = BETA_TWO * second + (1.0 - BETA_TWO) * gradient * gradient
    moment_hat = moment / (1.0 - BETA_ONE**STEP)
    second_hat = second / (1.0 - BETA_TWO**STEP)
    weight = weight - rate * (moment_hat / (jnp.sqrt(second_hat) + ADAM_EPS) + DECAY_RATE * weight)
    return (weight, moment, second)


def einsum(spec, *parts):
    return jnp.einsum(spec, *parts, precision=HIGH, preferred_element_type=F32)


def on_device(
    layer_input,
    cotangent,
    in_proj,
    delta_proj,
    out_proj,
    state_proj,
    packed_params,
    moment_in,
    moment_delta,
    moment_out,
    moment_state,
    moment_packed,
    square_in,
    square_delta,
    square_out,
    square_state,
    square_packed,
):
    sizes = (lax.axis_size("dp"), lax.axis_size("ctx"), lax.axis_size("tensor"))
    n_dp, n_ctx, n_t = sizes
    groups = n_dp * n_ctx
    rank = lax.axis_index("tensor")
    seqs, tokens, width = layer_input.shape
    rows = seqs * tokens
    local_inner = in_proj.shape[2]
    local_heads = delta_proj.shape[1]
    own_width = width // n_t
    rim = CONV - 1

    state_rows_own = state_proj.shape[0]
    pack_own = packed_params.shape[0]
    state_piece = jnp.concatenate(
        [state_proj[:, 0].astype(BF), state_proj[:, 1].astype(BF)], axis=0
    )
    state_pad = cdiv(2 * state_rows_own, 16) * 16
    delta_pad = cdiv(local_heads, 16) * 16
    pack_rows = cdiv(pack_own, LANES)
    pack_pad = cdiv(pack_rows, 16) * 16
    proj_rows = delta_proj.shape[0]
    block = jnp.concatenate(
        [
            jnp.pad(state_piece, ((0, state_pad - 2 * state_rows_own), (0, 0))),
            jnp.pad(
                delta_proj.astype(BF).T, ((0, delta_pad - local_heads), (0, LANES - proj_rows))
            ),
            jnp.pad(
                jnp.pad(packed_params.astype(BF), (0, pack_rows * LANES - pack_own)).reshape(
                    pack_rows, LANES
                ),
                ((0, pack_pad - pack_rows), (0, 0)),
            ),
        ],
        axis=0,
    )
    small = gather_small(block, sizes)
    wx = lax.all_gather(in_proj[:, 1].astype(BF), ("dp", "ctx"), axis=0, tiled=True)
    wz = lax.all_gather(in_proj[:, 0].astype(BF), ("dp", "ctx"), axis=0, tiled=True)
    small, late_cotangent = tie(small, cotangent)
    up_own = late_cotangent.astype(BF)
    if n_t == 2:
        up_away = swap(up_own)
        first = rank == 0
        up_full = jnp.concatenate(
            [jnp.where(first, up_own, up_away), jnp.where(first, up_away, up_own)], axis=2
        )
    else:
        up_full = lax.all_gather(up_own, "tensor", axis=2, tiled=True)
    up_rows = up_full.reshape(rows, width)

    state_slots = small[..., : 2 * state_rows_own, :].reshape(-1, 2, state_rows_own, STATE)
    ws = jnp.concatenate(
        [state_slots[:, 0].reshape(width, STATE), state_slots[:, 1].reshape(width, STATE)], axis=1
    )
    delta_slots = lax.dynamic_index_in_dim(small, rank, 2, False)
    delta_slots = delta_slots[..., state_pad : state_pad + local_heads, :proj_rows]
    wd = delta_slots.reshape(groups, local_heads, proj_rows).transpose(0, 2, 1)
    wd = wd.reshape(width, local_heads)
    pack_slots = small[..., state_pad + delta_pad : state_pad + delta_pad + pack_rows, :]
    packed = pack_slots.reshape(groups * n_t, pack_rows * LANES)[:, :pack_own].reshape(-1)
    pieces = unpack(packed.astype(F32))
    conv_kernel = lax.dynamic_slice_in_dim(
        pieces[0].reshape(CONV, INNER), rank * local_inner, local_inner, 1
    )
    conv_bias = lax.dynamic_slice_in_dim(pieces[1], rank * local_inner, local_inner, 0)
    gate_gain = lax.dynamic_slice_in_dim(pieces[2], rank * local_inner, local_inner, 0)
    state_kernel = pieces[3].reshape(CONV, 2 * STATE)
    state_bias = pieces[4]
    delta_bias = lax.dynamic_slice_in_dim(pieces[5], rank * local_heads, local_heads, 0)
    log_rates = lax.dynamic_slice_in_dim(pieces[6], rank * local_heads, local_heads, 0)
    skip_gain = lax.dynamic_slice_in_dim(pieces[7], rank * local_heads, local_heads, 0)
    norm_gain = pieces[8]
    rates = -jnp.exp(log_rates)

    input_float = layer_input.astype(F32)
    inverse = lax.rsqrt(jnp.mean(input_float * input_float, axis=-1, keepdims=True) + NORM_EPS)
    normed = (input_float * inverse * norm_gain).astype(BF).reshape(rows, width)
    sproj = dot(normed, ws, (1, 0)).astype(BF).reshape(seqs, tokens, 2 * STATE)
    raw = dot(normed, wd, (1, 0)).reshape(seqs, tokens, local_heads)
    xproj = dot(normed, wx, (1, 0)).astype(BF).reshape(seqs, tokens, local_inner)
    tails = from_behind(
        jnp.concatenate([xproj[:, tokens - rim :], sproj[:, tokens - rim :]], axis=2), "ctx", 1
    )
    ext_x = jnp.concatenate([tails[:, :, :local_inner], xproj], axis=1).astype(F32)
    ext_s = jnp.concatenate([tails[:, :, local_inner:], sproj], axis=1).astype(F32)
    conv_x = conv_forward(ext_x, conv_kernel, conv_bias, tokens)
    conv_s = conv_forward(ext_s, state_kernel, state_bias, tokens)
    act_x = jax.nn.silu(conv_x).astype(BF)
    act_s = jax.nn.silu(conv_s).astype(BF)
    delta = jax.nn.softplus(raw + delta_bias)
    wv = act_s[:, :, :STATE]
    rv = act_s[:, :, STATE:]
    past = (jnp.arange(tokens)[:, None] >= jnp.arange(tokens)[None, :]).astype(F32)
    cum = einsum("tm,smh->sth", past, delta * rates)
    totals = jnp.exp(cum[:, -1])
    fade_decay = jnp.exp(cum[:, -1:] - cum)
    fading = fade_decay * delta
    growth = jnp.exp(cum)
    spread = [
        jnp.broadcast_to(
            jnp.repeat(totals[k], HEAD_DIM)[:, None], (local_inner, STATE)
        )
        for k in range(seqs)
    ]
    cum_t = jnp.swapaxes(cum, 1, 2)
    skip_lanes = jnp.repeat(skip_gain, HEAD_DIM)[None, :]
    own_state = scan_states(act_x, wv, fading)
    within = scan_within(act_x, wv, rv, cum, cum_t, jnp.swapaxes(delta, 1, 2))
    own_state[1:], normed_late = tie(own_state[1:], normed)
    zproj = dot(normed_late, wz, (1, 0)).astype(BF).reshape(seqs, tokens, local_inner)
    entering, mark = chain(own_state, spread, False)
    out_half = tie(out_proj.astype(BF), mark)[0]
    wo = lax.all_gather(out_half, ("dp", "ctx"), axis=0, tiled=True)
    entering = jnp.stack(entering, axis=0)

    plain, mixed, square_sums = scan_gate(within, act_x, zproj, rv, growth, entering, skip_lanes)
    gate_input = zproj.astype(F32)
    gate_act = jax.nn.silu(gate_input)
    mixer = plain + skip_lanes * act_x.astype(F32)
    square_sums = sum_tensor(square_sums[:, :, 0])
    gate_inverse = lax.rsqrt(square_sums / INNER + NORM_EPS)[:, :, None]
    gated = (mixed * gate_inverse * gate_gain).astype(BF).reshape(rows, local_inner)

    def out_columns(start):
        return dot(gated, lax.dynamic_slice_in_dim(wo, start, own_width, 0), (1, 1))

    branch, branch_away = scatter_tensor(out_columns, own_width, rank)
    own_input = lax.dynamic_slice_in_dim(layer_input, rank * own_width, own_width, 2).astype(F32)

    gated_grad = dot(up_rows, wo, (1, 0)).reshape(seqs, tokens, local_inner)
    part_out = cut_dot(up_rows, gated)
    near_out = scatter_start(part_out, width)
    scaled = gated_grad * gate_gain
    row_sums = sum_tensor(jnp.sum(scaled * mixed, axis=-1))
    mixed_grad = gate_inverse * scaled - mixed * gate_inverse**3 * (row_sums / INNER)[:, :, None]
    grad_gate_gain = jnp.sum(gated_grad * mixed * gate_inverse, axis=(0, 1))
    mixer_grad = mixed_grad * gate_act
    z_grad = (mixed_grad * mixer * silu_grad(gate_input)).astype(BF).reshape(rows, local_inner)
    part_z = cut_dot(normed, z_grad)

    pulled = scan_states(mixer_grad, rv, growth)
    dy = mixer_grad
    dx_bare, dw, dr = scan_within_back(dy, act_x, wv, rv, cum, cum_t, delta)
    dx_bare, near_out = tie(dx_bare, near_out)
    far_out = scatter_high(part_out, width, near_out)
    near_z = scatter_start(part_z, width)
    leaving = jnp.stack(chain(pulled, spread, True)[0], axis=0)
    dx, dw, dr, bare_dot, fade_dot, plain_dot, skip_dot = scan_state_back(
        dy, act_x, plain, dx_bare, wv, delta, fading, growth, entering, leaving, skip_lanes, dw, dr
    )
    dx, (far_out, near_z, branch) = tie(dx, (far_out, near_z, branch))
    far_z = scatter_high(part_z, width, near_z)
    grad_out = scatter_end(part_out, width, near_out, far_out)
    cum_grad = plain_dot - delta * bare_dot - fading * fade_dot
    end_grad = jnp.sum(fading * fade_dot, axis=1) + totals * jnp.sum(
        (leaving * entering).reshape(seqs, local_heads, HEAD_DIM, STATE), axis=(2, 3)
    )
    step_grad = (
        einsum("tm,sth->smh", past, cum_grad) + end_grad[:, None, :]
    )
    delta_grad = bare_dot + fade_decay * fade_dot + rates * step_grad
    grad_rates = jnp.sum(delta * step_grad, axis=(0, 1))
    grad_skip = jnp.sum(skip_dot.reshape(seqs, local_heads, HEAD_DIM), axis=(0, 2))
    grad_log_rates = grad_rates * rates
    raw_grad = delta_grad * jax.nn.sigmoid(raw + delta_bias)
    grad_delta_bias = jnp.sum(raw_grad, axis=(0, 1))

    slope_x = dx.reshape(seqs, tokens, local_inner) * silu_grad(conv_x)
    slope_s = jnp.concatenate([dw, dr], axis=-1) * silu_grad(conv_s)
    follow = from_behind(
        jnp.concatenate([slope_x[:, :rim], slope_s[:, :rim]], axis=2), "ctx", -1
    )
    back_x, grad_conv_kernel, grad_conv_bias = conv_backward(
        slope_x, follow[:, :, :local_inner], ext_x, conv_kernel, tokens
    )
    back_s, grad_state_kernel, grad_state_bias = conv_backward(
        slope_s, follow[:, :, local_inner:], ext_s, state_kernel, tokens
    )
    x_grad = back_x.astype(BF).reshape(rows, local_inner)
    state_rows = back_s.reshape(rows, 2 * STATE)
    raw_rows = raw_grad.reshape(rows, local_heads)

    def normed_columns(start):
        def cut(weight):
            return lax.dynamic_slice_in_dim(weight, start, own_width, 0)

        product = dot(x_grad, cut(wx), (1, 1))
        product_z = dot(z_grad, cut(wz), (1, 1))
        return (
            product
            + product_z
            + dot(state_rows, cut(ws).astype(F32), (1, 1), True)
            + dot(raw_rows, cut(wd).astype(F32), (1, 1), True)
        )

    x_grad, (branch_away, far_z, grad_out) = tie(x_grad, (branch_away, far_z, grad_out))
    layer_output = own_input + (branch + branch_away).reshape(seqs, tokens, own_width)
    held_z, sent_z = scatter_ctx(part_z, width, near_z, far_z)
    pieces_x = 2 if local_inner % (2 * LANES) == 0 else 1
    piece = local_inner // pieces_x
    parts_x = [
        cut_dot(normed, x_grad[:, k * piece : (k + 1) * piece]) for k in range(pieces_x)
    ]
    near_x = []
    for part in parts_x:
        near_x.append(scatter_start(part, width))

    starts = [(1 - rank) * own_width, rank * own_width]
    if n_t != 2:
        starts = [k * own_width for k in range(n_t)]
    columns = [normed_columns(start) for start in starts]
    if n_t == 2:
        normed_grad, normed_away = columns[1], swap(columns[0])
    else:
        normed_grad = lax.psum_scatter(
            jnp.concatenate(columns, axis=1), "tensor", scatter_dimension=1, tiled=True
        )
        normed_away = jnp.zeros((1,), F32)
    own_gain = lax.dynamic_slice_in_dim(norm_gain, rank * own_width, own_width, 0)
    grad_norm_gain = jnp.zeros((D,), F32)
    in_sums = 0.0
    for start, part in zip(starts, columns):
        inputs = lax.dynamic_slice_in_dim(layer_input, start, own_width, 2).astype(F32)
        gain = lax.dynamic_slice_in_dim(norm_gain, start, own_width, 0)
        product = part.reshape(seqs, tokens, own_width) * inputs
        in_sums = in_sums + jnp.sum(product * gain, axis=-1)
        grad_norm_gain = lax.dynamic_update_slice_in_dim(
            grad_norm_gain, jnp.sum(product * inverse, axis=(0, 1)), start, 0
        )

    normed_float = normed.astype(F32)
    grad_state_part = dot(normed_float, state_rows, (0, 0), True)
    grad_delta_part = dot(normed_float, raw_rows, (0, 0), True)

    def widen(local_values, full_length):
        return lax.dynamic_update_slice_in_dim(
            jnp.zeros((full_length,), F32), local_values, rank * local_values.shape[0], 0
        )

    conv_wide = lax.dynamic_update_slice_in_dim(
        jnp.zeros((CONV, INNER), F32), grad_conv_kernel, rank * local_inner, 1
    ).reshape(-1)
    joined = jnp.concatenate(
        [
            conv_wide,
            widen(grad_conv_bias, INNER),
            widen(grad_gate_gain, INNER),
            grad_state_kernel.reshape(-1),
            grad_state_bias,
            widen(grad_delta_bias, HEADS),
            widen(grad_log_rates, HEADS),
            widen(grad_skip, HEADS),
            grad_norm_gain,
        ]
    )
    pack_group = n_t * pack_own
    packed_part = jnp.pad(joined, (0, groups * pack_group - joined.shape[0]))
    pack_cols = cdiv(pack_group, proj_rows)
    packed_part = jnp.pad(
        packed_part.reshape(groups, pack_group), ((0, 0), (0, pack_cols * proj_rows - pack_group))
    ).reshape(width, pack_cols)
    extra_pad = cdiv(local_heads + pack_cols, LANES) * LANES - local_heads - pack_cols
    tail_part = jnp.concatenate(
        [
            grad_state_part,
            grad_delta_part,
            packed_part,
            jnp.zeros((width, extra_pad), F32),
        ],
        axis=1,
    )
    far_x = []
    for k, part in enumerate(parts_x):
        if k:
            near_x[k], far_x[k - 1] = tie(near_x[k], far_x[k - 1])
        far_x.append(scatter_high(part, width, near_x[k]))
    blocks_x = []
    for k, part in enumerate(parts_x):
        blocks_x.append(scatter_ctx(part, width, near_x[k], far_x[k]))
    grad_x = jnp.concatenate([scatter_sum(*block) for block in blocks_x], axis=1)

    grad_x, (in_sums, sent_z, normed_away) = tie(grad_x, (in_sums, sent_z, normed_away))
    scaled_in = (normed_grad + normed_away).reshape(seqs, tokens, own_width) * own_gain
    grad_z = scatter_sum(held_z, sent_z)
    in_mean = sum_tensor(in_sums)[:, :, None] / width
    input_grad = cotangent + inverse * scaled_in - own_input * inverse**3 * in_mean

    def part_tail(start, rows):
        return lax.dynamic_slice_in_dim(tail_part, start, rows, 0)

    near_tail = scatter_start(part_tail, width)
    far_tail = scatter_high(part_tail, width, near_tail)
    tail = scatter_end(part_tail, width, near_tail, far_tail)
    at = 2 * STATE
    grad_delta = tail[:, at : at + local_heads]
    state_group = tail[:, :at]
    packed_group = tail[:, at + local_heads : at + local_heads + pack_cols]
    packed_group = packed_group.reshape(-1)[:pack_group]
    if n_t == 2:
        away = swap(
            (
                lax.dynamic_slice_in_dim(
                    state_group, (1 - rank) * state_rows_own, state_rows_own, 0
                ),
                lax.dynamic_slice_in_dim(packed_group, (1 - rank) * pack_own, pack_own, 0),
            )
        )
        grad_state = (
            lax.dynamic_slice_in_dim(state_group, rank * state_rows_own, state_rows_own, 0)
            + away[0]
        )
        grad_packed = (
            lax.dynamic_slice_in_dim(packed_group, rank * pack_own, pack_own, 0) + away[1]
        )
    else:
        grad_state = lax.psum_scatter(state_group, "tensor", scatter_dimension=0, tiled=True)
        grad_packed = lax.psum_scatter(packed_group, "tensor", scatter_dimension=0, tiled=True)
    grad_state = grad_state.reshape(state_rows_own, 2, STATE)
    grad_in = jnp.stack([grad_z, grad_x], axis=1)

    new_in, next_moment_in, next_square_in = adam_update(
        in_proj, moment_in, square_in, grad_in, MATRIX_RATE
    )
    new_delta, next_moment_delta, next_square_delta = adam_update(
        delta_proj, moment_delta, square_delta, grad_delta, MATRIX_RATE
    )
    new_out, next_moment_out, next_square_out = adam_update(
        out_proj, moment_out, square_out, grad_out, MATRIX_RATE
    )
    new_state, next_moment_state, next_square_state = adam_update(
        state_proj, moment_state, square_state, grad_state, MATRIX_RATE
    )
    new_packed, next_moment_packed, next_square_packed = adam_update(
        packed_params, moment_packed, square_packed, grad_packed, PACKED_RATE
    )
    return (
        layer_output,
        input_grad,
        grad_in,
        grad_delta,
        grad_out,
        grad_state,
        grad_packed,
        new_in,
        new_delta,
        new_out,
        new_state,
        new_packed,
        next_moment_in,
        next_moment_delta,
        next_moment_out,
        next_moment_state,
        next_moment_packed,
        next_square_in,
        next_square_delta,
        next_square_out,
        next_square_state,
        next_square_packed,
    )


def solution(mesh):
    matrix = P(("dp", "ctx"), "tensor")
    projection = P(("dp", "ctx"), None, "tensor")
    state = P(("dp", "ctx", "tensor"), None, None)
    flat = P(("dp", "ctx", "tensor"))
    tokens = P("dp", "ctx", "tensor")
    weights = (projection, matrix, matrix, state, flat)

    return jax.shard_map(
        on_device,
        mesh=mesh,
        in_specs=(P("dp", "ctx", None), tokens) + weights * 3,
        out_specs=(tokens, tokens) + weights * 4,
        check_vma=False,
    )
```
